8 devices in a mesh: cp: 8 (over z, y, x, core).
Axes of the slice: x: 2, y: 2, z: 1, core: 2. Of those that a mesh axis runs over, the one named last changes fastest.
Arguments:
- x_in: bfloat16 [8192, 640], P('cp')
- norm_gains: float32 [2, 4, 640], replicated
- qk_gains: float32 [2, 2, 256], replicated
- w_q: bfloat16 [2, 640, 4, 256], replicated
- w_k: bfloat16 [2, 640, 1, 256], replicated
- w_v: bfloat16 [2, 640, 1, 256], replicated
- w_o: bfloat16 [2, 4, 256, 640], replicated
- w_gate: bfloat16 [2, 640, 2048], replicated
- w_up: bfloat16 [2, 640, 2048], replicated
- w_down: bfloat16 [2, 2048, 640], replicated
Outputs:
- output 1: bfloat16 [8192, 640], P('cp')
- output 2: bfloat16 [8192, 1, 256], P('cp')
- output 3: bfloat16 [8192, 1, 256], P('cp')
- output 4: bfloat16 [1024, 1, 256], replicated
- output 5: bfloat16 [1024, 1, 256], replicated
All inputs are finite; a program needn't handle non-finite values.
Results may differ from the reference program's by a relative error of at most 0.016197.
Values are sent between devices in bfloat16 or wider.
A program may use at most 1 GiB of HBM per device.

```python
import jax
import jax.numpy as jnp
from jax import lax

D = 640
HEADS = 4
KV_HEADS = 1
HEAD = 256
FF = 2048
WINDOW = 1024
TOKENS_DEV = 1024
SEQ = 8192

GROUP = HEADS // KV_HEADS
QBLK = min(SEQ, 64)
EPS = 1e-6
LOCAL_BASE = 10000.0
GLOBAL_BASE = 1000000.0
GLOBAL_SCALE = 8.0


def setup_inputs(seed: int = 0) -> dict:
    rng_keys = jax.random.split(jax.random.key(seed), 13)
    positions = jnp.arange(SEQ)
    sprinkle = jax.random.randint(rng_keys[0], (SEQ,), 0, 32) == 0
    amplitude = jnp.where(positions < TOKENS_DEV, 3.0, jnp.where(sprinkle, 2.0, 0.6))
    direction = jax.random.normal(rng_keys[1], (D,), jnp.float32)
    x_in = jax.random.normal(rng_keys[2], (SEQ, D), jnp.float32) + amplitude[:, None] * direction[None, :]
    shared = jax.random.normal(rng_keys[3], (2, D, KV_HEADS, 1, HEAD), jnp.float32)
    w_q = (shared + 0.6 * jax.random.normal(rng_keys[4], (2, D, KV_HEADS, GROUP, HEAD), jnp.float32)) * D ** -0.5
    w_k = (shared[:, :, :, 0, :] + 0.6 * jax.random.normal(rng_keys[5], (2, D, KV_HEADS, HEAD), jnp.float32)) * D ** -0.5
    w_v = jax.random.normal(rng_keys[6], (2, D, KV_HEADS, HEAD), jnp.float32) * D ** -0.5
    w_o = jax.random.normal(rng_keys[7], (2, HEADS, HEAD, D), jnp.float32) * (HEADS * HEAD) ** -0.5
    w_gate = jax.random.normal(rng_keys[8], (2, D, FF), jnp.float32) * D ** -0.5
    w_up = jax.random.normal(rng_keys[9], (2, D, FF), jnp.float32) * D ** -0.5
    w_down = jax.random.normal(rng_keys[10], (2, FF, D), jnp.float32) * FF ** -0.5
    norm_gains = 0.3 * jax.random.normal(rng_keys[11], (2, 4, D), jnp.float32)
    qk_gains = 0.3 * jax.random.normal(rng_keys[12], (2, 2, HEAD), jnp.float32)
    return {
        'x_in': x_in.astype(jnp.bfloat16),
        'norm_gains': norm_gains,
        'qk_gains': qk_gains,
        'w_q': w_q.reshape(2, D, HEADS, HEAD).astype(jnp.bfloat16),
        'w_k': w_k.astype(jnp.bfloat16),
        'w_v': w_v.astype(jnp.bfloat16),
        'w_o': w_o.astype(jnp.bfloat16),
        'w_gate': w_gate.astype(jnp.bfloat16),
        'w_up': w_up.astype(jnp.bfloat16),
        'w_down': w_down.astype(jnp.bfloat16),
    }


def gain_norm(x_val, gain_vec):
    x_f32 = x_val.astype(jnp.float32)
    mean_sq = jnp.mean(x_f32 * x_f32, axis=-1, keepdims=True)
    return x_f32 * lax.rsqrt(mean_sq + EPS) * (1.0 + gain_vec)


def rope_tables(positions, rope_base, pos_scale):
    inv_freq = rope_base ** (-jnp.arange(HEAD // 2, dtype=jnp.float32) * 2.0 / HEAD)
    angles = (positions.astype(jnp.float32) / pos_scale)[:, None] * inv_freq[None, :]
    return jnp.cos(angles), jnp.sin(angles)


def rotate(x_val, cos_tab, sin_tab):
    half_dim = x_val.shape[-1] // 2
    lower_half = x_val[..., :half_dim]
    upper_half = x_val[..., half_dim:]
    return jnp.concatenate([lower_half * cos_tab - upper_half * sin_tab, upper_half * cos_tab + lower_half * sin_tab], axis=-1)


def attend_block(q_blk, k_blk, v_blk, q_pos, k_pos, is_local):
    scores = jnp.einsum('qkgd,skd->kgqs', q_blk, k_blk) * HEAD ** -0.5
    offsets = q_pos[:, None] - k_pos[None, :]
    visible = offsets >= 0
    if is_local:
        visible = visible & (offsets < WINDOW) & (k_pos >= 0)[None, :]
    scores = jnp.where(visible, scores, -jnp.inf)
    probs = jax.nn.softmax(scores, axis=-1)
    return jnp.einsum('kgqs,skd->qkgd', probs, v_blk)


def decoder_layer(x_in, layer_gains, qk_gain, w_q, w_k, w_v, w_o, w_gate, w_up, w_down, is_local):
    positions = jnp.arange(SEQ)
    normed = gain_norm(x_in, layer_gains[0]).astype(jnp.bfloat16)
    q_proj = jnp.dot(normed, w_q.reshape(D, HEADS * HEAD), preferred_element_type=jnp.float32).astype(jnp.bfloat16).reshape(SEQ, KV_HEADS, GROUP, HEAD)
    k_proj = jnp.dot(normed, w_k.reshape(D, KV_HEADS * HEAD), preferred_element_type=jnp.float32).astype(jnp.bfloat16).reshape(SEQ, KV_HEADS, HEAD)
    v_proj = jnp.dot(normed, w_v.reshape(D, KV_HEADS * HEAD), preferred_element_type=jnp.float32).astype(jnp.bfloat16).reshape(SEQ, KV_HEADS, HEAD)
    rope_base = LOCAL_BASE if is_local else GLOBAL_BASE
    pos_scale = 1.0 if is_local else GLOBAL_SCALE
    cos_tab, sin_tab = rope_tables(positions, rope_base, pos_scale)
    q_rot = rotate(gain_norm(q_proj, qk_gain[0]), cos_tab[:, None, None, :], sin_tab[:, None, None, :]).astype(jnp.bfloat16)
    k_rot = rotate(gain_norm(k_proj, qk_gain[1]), cos_tab[:, None, :], sin_tab[:, None, :]).astype(jnp.bfloat16)
    q_f32 = q_rot.astype(jnp.float32)
    k_f32 = k_rot.astype(jnp.float32)
    v_f32 = v_proj.astype(jnp.float32)
    if is_local:
        zero_pad = jnp.zeros((WINDOW, KV_HEADS, HEAD), jnp.float32)
        k_pad = jnp.concatenate([zero_pad, k_f32], axis=0)
        v_pad = jnp.concatenate([zero_pad, v_f32], axis=0)

        def attend_rows(blk_index):
            row_start = blk_index * QBLK
            q_blk = lax.dynamic_slice_in_dim(q_f32, row_start, QBLK)
            k_blk = lax.dynamic_slice_in_dim(k_pad, row_start, WINDOW + QBLK)
            v_blk = lax.dynamic_slice_in_dim(v_pad, row_start, WINDOW + QBLK)
            k_pos = row_start - WINDOW + jnp.arange(WINDOW + QBLK)
            return attend_block(q_blk, k_blk, v_blk, row_start + jnp.arange(QBLK), k_pos, True)
    else:
        def attend_rows(blk_index):
            row_start = blk_index * QBLK
            q_blk = lax.dynamic_slice_in_dim(q_f32, row_start, QBLK)
            return attend_block(q_blk, k_f32, v_f32, row_start + jnp.arange(QBLK), positions, False)
    attn_out = lax.map(attend_rows, jnp.arange(SEQ // QBLK)).reshape(SEQ, HEADS * HEAD).astype(jnp.bfloat16)
    o_proj = jnp.dot(attn_out, w_o.reshape(HEADS * HEAD, D), preferred_element_type=jnp.float32).astype(jnp.bfloat16)
    resid_mid = (x_in.astype(jnp.float32) + gain_norm(o_proj, layer_gains[1])).astype(jnp.bfloat16)
    ff_in = gain_norm(resid_mid, layer_gains[2]).astype(jnp.bfloat16)
    gate_act = jnp.dot(ff_in, w_gate, preferred_element_type=jnp.float32)
    up_proj = jnp.dot(ff_in, w_up, preferred_element_type=jnp.float32)
    hidden = (jax.nn.gelu(gate_act, approximate=True) * up_proj).astype(jnp.bfloat16)
    mlp_out = jnp.dot(hidden, w_down, preferred_element_type=jnp.float32).astype(jnp.bfloat16)
    x_out = (resid_mid.astype(jnp.float32) + gain_norm(mlp_out, layer_gains[3])).astype(jnp.bfloat16)
    return x_out, k_rot, v_proj


def reference(x_in, norm_gains, qk_gains, w_q, w_k, w_v, w_o, w_gate, w_up, w_down):
    mid_out, k_loc, v_loc = decoder_layer(x_in, norm_gains[0], qk_gains[0], w_q[0], w_k[0], w_v[0], w_o[0], w_gate[0], w_up[0], w_down[0], True)
    x_out, k_glob, v_glob = decoder_layer(mid_out, norm_gains[1], qk_gains[1], w_q[1], w_k[1], w_v[1], w_o[1], w_gate[1], w_up[1], w_down[1], False)
    return (x_out, k_glob, v_glob, k_loc[SEQ - WINDOW:], v_loc[SEQ - WINDOW:])
```

```python
import functools

import numpy as np
import jax
import jax.numpy as jnp
from jax import lax
from jax.experimental import pallas as pl
from jax.experimental.pallas import tpu as pltpu
from jax.sharding import PartitionSpec as P

WINDOW = 1024
EPS = 1e-6
BASES = (10000.0, 1000000.0)
SCALES = (1.0, 8.0)
HEAD = 256
TOK = 1024
D = 640
FF = 2048
TILE = 256
LO = 32
LOG2E = 1.4426950408889634
COEF = LOG2E / 16.0
TOP = 36.0
LIMIT = 56.0
NEG = -1e30
F32 = jnp.float32
BF16 = jnp.bfloat16
VLIM = 58 << 20


def rope_const(layer, seq_len):
    base, scale = BASES[layer], SCALES[layer]
    freq = base ** (-np.arange(HEAD // 2, dtype=np.float64) * 2.0 / HEAD)
    hi = (np.arange(seq_len // LO) * LO / scale)[:, None] * freq[None, :]
    lo = (np.arange(LO) / scale)[:, None] * freq[None, :]
    hi_tab = np.concatenate([np.cos(hi), np.sin(hi)], axis=1).astype(np.float32)
    lo_tab = np.concatenate([np.cos(lo), np.sin(lo)], axis=1).astype(np.float32)
    return hi_tab, lo_tab


def rms(x, gain):
    return x * lax.rsqrt(jnp.mean(x * x, axis=-1, keepdims=True) + EPS) * gain


def cos_sin(hi_ref, lo_ref, row0, rows):
    n_hi = rows // LO
    hi = hi_ref[pl.ds(pl.multiple_of(row0 // LO, 8), n_hi), :]
    lo = lo_ref[...]
    ch, sh = hi[:, None, 0:128], hi[:, None, 128:256]
    cl, sl = lo[None, :, 0:128], lo[None, :, 128:256]
    cos = (ch * cl - sh * sl).reshape(rows, 128)
    sin = (sh * cl + ch * sl).reshape(rows, 128)
    return cos, sin


def rotate(x, cos, sin):
    a, b = x[:, 0:128], x[:, 128:256]
    return jnp.concatenate([a * cos - b * sin, b * cos + a * sin], axis=1).astype(BF16)


def head_rope(proj, gain, cos, sin):
    return rotate(rms(proj.astype(BF16).astype(F32), gain), cos, sin)


def dot(a, b):
    return jnp.dot(a, b, preferred_element_type=F32)


def dot_t(a, b):
    return lax.dot_general(a, b, (((1,), (1,)), ((), ())), preferred_element_type=F32)


def qkv_tile(normed, gq, gk, wq, wk, wv, cos, sin, q_ref, kv_ref, k_ref, v_ref):
    k = head_rope(dot(normed, wk[...]), gk, cos, sin)
    v = dot(normed, wv[...]).astype(BF16)
    kv_ref[:, 0:HEAD] = k
    kv_ref[:, HEAD:2 * HEAD] = v
    k_ref[...] = k
    v_ref[...] = v
    for h in range(4):
        q_ref[h] = head_rope(dot(normed, wq[:, h * HEAD:(h + 1) * HEAD]), gq, cos, sin)


def proj_kernel(x_ref, ng_ref, qg_ref, hi_ref, lo_ref, wq_ref, wk_ref, wv_ref, q_ref, kv_ref, k_ref, v_ref):
    i = pl.program_id(0)
    row0 = lax.axis_index('cp') * TOK + i * TILE
    cos, sin = cos_sin(hi_ref, lo_ref, row0, TILE)
    normed = rms(x_ref[...].astype(F32), 1.0 + ng_ref[0:1, :]).astype(BF16)
    qkv_tile(normed, 1.0 + qg_ref[0:1, :], 1.0 + qg_ref[1:2, :], wq_ref, wk_ref, wv_ref, cos, sin, q_ref, kv_ref, k_ref, v_ref)


def whole(shape):
    zeros = (0,) * len(shape)
    return pl.BlockSpec(shape, lambda *_: zeros, pipeline_mode=pl.Buffered(1))


def layer_of(layer, shape):
    idx = (layer,) + (0,) * len(shape)
    return pl.BlockSpec((None,) + shape, lambda *_: idx, pipeline_mode=pl.Buffered(1))


def rows_spec(cols):
    return pl.BlockSpec((TILE, cols), lambda i: (i, 0))


Q_SPEC = pl.BlockSpec((4, TILE, HEAD), lambda i: (0, i, 0))
Q_SHAPE = jax.ShapeDtypeStruct((4, TOK, HEAD), BF16)
KV_SHAPE = jax.ShapeDtypeStruct((TOK, 2 * HEAD), BF16)
K_SHAPE = jax.ShapeDtypeStruct((TOK, HEAD), BF16)
X_SHAPE = jax.ShapeDtypeStruct((TOK, D), BF16)


def project(layer, x, ng, qg, hi, lo, wq, wk, wv):
    return pl.pallas_call(
        proj_kernel,
        grid=(TOK // TILE,),
        in_specs=[rows_spec(D), layer_of(layer, (4, D)), layer_of(layer, (2, HEAD)), whole(hi.shape), whole(lo.shape),
                  layer_of(layer, (D, 4 * HEAD)), layer_of(layer, (D, HEAD)), layer_of(layer, (D, HEAD))],
        out_specs=[Q_SPEC, rows_spec(2 * HEAD), rows_spec(HEAD), rows_spec(HEAD)],
        out_shape=[Q_SHAPE, KV_SHAPE, K_SHAPE, K_SHAPE],
        name=f"project{layer}",
        compiler_params=pltpu.CompilerParams(vmem_limit_bytes=VLIM),
        cost_estimate=pl.CostEstimate(flops=2 * TOK * D * 1536, bytes_accessed=8 << 20, transcendentals=0),
    )(x, ng, qg, hi, lo, wq, wk, wv)


def finish_tile(x, attn, ng, wo, wg, wu, wd):
    o = dot(attn, wo).astype(BF16).astype(F32)
    h1 = (x.astype(F32) + rms(o, 1.0 + ng[1:2, :])).astype(BF16)
    b = rms(h1.astype(F32), 1.0 + ng[2:3, :]).astype(BF16)
    acc = None
    step = 512
    for f in range(0, FF, step):
        g = dot(b, wg[:, f:f + step])
        u = dot(b, wu[:, f:f + step])
        m = (jax.nn.gelu(g, approximate=True) * u).astype(BF16)
        part = dot(m, wd[f:f + step, :])
        acc = part if acc is None else acc + part
    o2 = acc.astype(BF16).astype(F32)
    return (h1.astype(F32) + rms(o2, 1.0 + ng[3:4, :])).astype(BF16)


def local_tile(q_ref, halo_ref, own_ref, win_ref, sigma, fast):
    i = pl.program_id(0)
    first = lax.axis_index('cp') == 0

    @pl.when(i == 0)
    def _():
        win_ref[0:WINDOW, :] = halo_ref[...]
        win_ref[WINDOW:WINDOW + TOK, :] = own_ref[...]

    n_key = WINDOW + TILE
    start = pl.multiple_of(i * TILE, TILE)
    ks = win_ref[pl.ds(start, n_key), 0:HEAD]
    vs = win_ref[pl.ds(start, n_key), HEAD:2 * HEAD]
    col = lax.broadcasted_iota(jnp.int32, (1, n_key), 1)
    hidden = jnp.logical_and(first, col + start < WINDOW)
    r = lax.broadcasted_iota(jnp.int32, (TILE, TILE), 0)
    c = lax.broadcasted_iota(jnp.int32, (TILE, TILE), 1)
    outs = []
    for h in range(4):
        s = dot_t(q_ref[h], ks)
        if fast:
            t = s * COEF + jnp.where(hidden, NEG, -sigma)
        else:
            t = s * COEF + jnp.where(hidden, NEG, 0.0)
        t = jnp.concatenate([jnp.where(c > r, t[:, 0:TILE], NEG), t[:, TILE:WINDOW], jnp.where(c <= r, t[:, WINDOW:], NEG)], axis=1)
        if not fast:
            t = t - jnp.max(t, axis=1, keepdims=True)
        p = jnp.exp2(t)
        total = jnp.sum(p, axis=1, keepdims=True)
        outs.append((dot(p.astype(BF16), vs) / total).astype(BF16))
    return jnp.concatenate(outs, axis=1)


def mid_kernel(fast, sig_ref, q_ref, halo_ref, own_ref, x_ref, ng_ref, ng2_ref, qg_ref, hi_ref, lo_ref,
               wo_hbm, wg_hbm, wu_hbm, wd_hbm, wq_hbm, wk_hbm, wv_hbm,
               mid_ref, q2_ref, kv_ref, k_ref, v_ref,
               win_ref, wo, wg, wu, wd, wq, wk, wv, sems):
    i = pl.program_id(0)
    pairs = [(wo_hbm.at[0], wo), (wg_hbm.at[0], wg), (wu_hbm.at[0], wu), (wd_hbm.at[0], wd),
             (wq_hbm.at[1], wq), (wk_hbm.at[1], wk), (wv_hbm.at[1], wv)]
    copies = [pltpu.make_async_copy(s, d, sems.at[n]) for n, (s, d) in enumerate(pairs)]

    @pl.when(i == 0)
    def _():
        for cp in copies:
            cp.start()

    attn = local_tile(q_ref, halo_ref, own_ref, win_ref, sig_ref[0], fast)

    @pl.when(i == 0)
    def _():
        for cp in copies:
            cp.wait()

    mid = finish_tile(x_ref[...], attn, ng_ref, wo[...], wg, wu, wd)
    mid_ref[...] = mid
    row0 = lax.axis_index('cp') * TOK + i * TILE
    cos, sin = cos_sin(hi_ref, lo_ref, row0, TILE)
    normed = rms(mid.astype(F32), 1.0 + ng2_ref[0:1, :]).astype(BF16)
    qkv_tile(normed, 1.0 + qg_ref[0:1, :], 1.0 + qg_ref[1:2, :], wq, wk, wv, cos, sin, q2_ref, kv_ref, k_ref, v_ref)


ANY = pl.BlockSpec(memory_space=pl.ANY)
SMEM = pl.BlockSpec(memory_space=pltpu.SMEM)
FIN_SCRATCH = [pltpu.VMEM((4 * HEAD, D), BF16), pltpu.VMEM((D, FF), BF16), pltpu.VMEM((D, FF), BF16), pltpu.VMEM((FF, D), BF16)]


def middle(fast, sig, q, halo, own, x, ng, qg, hi, lo, wo, wg, wu, wd, wq, wk, wv):
    return pl.pallas_call(
        functools.partial(mid_kernel, fast),
        grid=(TOK // TILE,),
        in_specs=[SMEM, Q_SPEC, whole((TOK, 2 * HEAD)), whole((TOK, 2 * HEAD)), rows_spec(D), layer_of(0, (4, D)), layer_of(1, (4, D)),
                  layer_of(1, (2, HEAD)), whole(hi.shape), whole(lo.shape)] + [ANY] * 7,
        out_specs=[rows_spec(D), Q_SPEC, rows_spec(2 * HEAD), rows_spec(HEAD), rows_spec(HEAD)],
        out_shape=[X_SHAPE, Q_SHAPE, KV_SHAPE, K_SHAPE, K_SHAPE],
        scratch_shapes=[pltpu.VMEM((WINDOW + TOK, 2 * HEAD), BF16)] + FIN_SCRATCH +
                       [pltpu.VMEM((D, 4 * HEAD), BF16), pltpu.VMEM((D, HEAD), BF16), pltpu.VMEM((D, HEAD), BF16), pltpu.SemaphoreType.DMA((7,))],
        name="middle",
        compiler_params=pltpu.CompilerParams(vmem_limit_bytes=VLIM),
        cost_estimate=pl.CostEstimate(flops=18 * 10**9, bytes_accessed=20 << 20, transcendentals=0),
    )(sig, q, halo, own, x, ng, ng, qg, hi, lo, wo, wg, wu, wd, wq, wk, wv)


def finish_kernel(attn_ref, x_ref, ng_ref, wo_hbm, wg_hbm, wu_hbm, wd_hbm, out_ref, wo, wg, wu, wd, sems):
    i = pl.program_id(0)
    pairs = [(wo_hbm.at[1], wo), (wg_hbm.at[1], wg), (wu_hbm.at[1], wu), (wd_hbm.at[1], wd)]
    copies = [pltpu.make_async_copy(s, d, sems.at[n]) for n, (s, d) in enumerate(pairs)]

    @pl.when(i == 0)
    def _():
        for cp in copies:
            cp.start()
        for cp in copies:
            cp.wait()

    attn = jnp.concatenate([attn_ref[h] for h in range(4)], axis=1)
    out_ref[...] = finish_tile(x_ref[...], attn, ng_ref, wo[...], wg, wu, wd)


def finish(attn, x, ng, wo, wg, wu, wd):
    return pl.pallas_call(
        finish_kernel,
        grid=(TOK // TILE,),
        in_specs=[Q_SPEC, rows_spec(D), layer_of(1, (4, D))] + [ANY] * 4,
        out_specs=rows_spec(D),
        out_shape=X_SHAPE,
        scratch_shapes=FIN_SCRATCH + [pltpu.SemaphoreType.DMA((4,))],
        name="finish",
        compiler_params=pltpu.CompilerParams(vmem_limit_bytes=VLIM),
        cost_estimate=pl.CostEstimate(flops=10 * 10**9, bytes_accessed=12 << 20, transcendentals=0),
    )(attn, x, ng, wo, wg, wu, wd)


def flash_kernel(fast, sig_ref, q_ref, kv_ref, o_ref, acc, l, m):
    me = lax.axis_index('cp')
    i = pl.program_id(0)
    sigma = sig_ref[1]

    def update(ks, vs, width, masked, first):
        if masked:
            r = lax.broadcasted_iota(jnp.int32, (TILE, width), 0) + i * TILE
            vis = lax.broadcasted_iota(jnp.int32, (TILE, width), 1) <= r
        for h in range(4):
            sl = slice(h * TILE, (h + 1) * TILE)
            s = dot_t(q_ref[h], ks)
            if fast:
                t = s * COEF - sigma
                if masked:
                    t = jnp.where(vis, t, NEG)
                p = jnp.exp2(t)
            else:
                t = s * COEF
                if masked:
                    t = jnp.where(vis, t, NEG)
                top = jnp.broadcast_to(jnp.max(t, axis=1, keepdims=True), (TILE, 128))
                new = top if first else jnp.maximum(m[sl], top)
                if not first:
                    decay = jnp.exp2(m[sl] - new)
                    l[sl] = l[sl] * decay
                    acc[sl] = acc[sl] * decay[:, 0:1]
                m[sl] = new
                p = jnp.exp2(t - new[:, 0:1])
            lp = p[:, 0:128]
            for j in range(1, width // 128):
                lp = lp + p[:, j * 128:(j + 1) * 128]
            o = dot(p.astype(BF16), vs)
            if first:
                l[sl] = lp
                acc[sl] = o
            else:
                l[sl] += lp
                acc[sl] += o

    base = pl.multiple_of(me * TOK, TOK)
    update(kv_ref[pl.ds(base, TOK), 0:HEAD], kv_ref[pl.ds(base, TOK), HEAD:2 * HEAD], TOK, True, True)

    def body(j, carry):
        b = pl.multiple_of(j * TOK, TOK)
        update(kv_ref[pl.ds(b, TOK), 0:HEAD], kv_ref[pl.ds(b, TOK), HEAD:2 * HEAD], TOK, False, False)
        return carry

    lax.fori_loop(0, me, body, 0)
    total = jnp.sum(l[...], axis=1, keepdims=True)
    o_ref[...] = (acc[...] / total).astype(BF16).reshape(4, TILE, HEAD)


def flash(fast, sig, q, kv_all):
    return pl.pallas_call(
        functools.partial(flash_kernel, fast),
        grid=(TOK // TILE,),
        in_specs=[SMEM, Q_SPEC, whole(kv_all.shape)],
        out_specs=Q_SPEC,
        out_shape=Q_SHAPE,
        scratch_shapes=[pltpu.VMEM((4 * TILE, HEAD), F32), pltpu.VMEM((4 * TILE, 128), F32), pltpu.VMEM((4 * TILE, 128), F32)],
        name="flash",
        compiler_params=pltpu.CompilerParams(vmem_limit_bytes=VLIM),
        cost_estimate=pl.CostEstimate(flops=32 * 10**9, bytes_accessed=12 << 20, transcendentals=0),
    )(sig, q, kv_all)


def score_bound(qk_gain):
    g = jnp.abs(1.0 + qk_gain)
    pair = jnp.maximum(g[:, 0:HEAD // 2], g[:, HEAD // 2:])
    return 16.0 * 1.02 * jnp.max(pair[0] * pair[1])


def solution(mesh):
    n_dev = mesh.shape['cp']
    rope = [rope_const(layer, TOK * n_dev) for layer in range(2)]
    rounds = [[(7, 5)], [(7, 3), (5, 1)], [(7, 6), (5, 4), (3, 2), (1, 0)]]

    def spread(kv):
        me = lax.axis_index('cp')
        got = kv
        for pairs in rounds:
            new = lax.ppermute(got, 'cp', perm=pairs)
            takes = functools.reduce(jnp.logical_or, [me == r for _, r in pairs])
            got = jnp.where(takes, new, got)
        return got

    def shard_body(x, ng, qg, w_q, w_k, w_v, w_o, w_gate, w_up, w_down):
        wq = w_q.reshape(2, D, 4 * HEAD)
        wk = w_k.reshape(2, D, HEAD)
        wv = w_v.reshape(2, D, HEAD)
        wo = w_o.reshape(2, 4 * HEAD, D)
        bounds = [score_bound(qg[layer]) for layer in range(2)]
        safe = jnp.maximum(bounds[0], bounds[1]) <= LIMIT
        sig = jnp.stack([jnp.maximum(b - TOP, 0.0) * LOG2E for b in bounds])

        def run(fast):
            q, kv, _, _ = project(0, x, ng, qg, *rope[0], wq, wk, wv)
            halo = lax.ppermute(kv, 'cp', perm=[(s, s + 1) for s in range(n_dev - 1)])
            mid, q5, kv5, k5, v5 = middle(fast, sig, q, halo, kv, x, ng, qg, *rope[1], wo, w_gate, w_up, w_down, wq, wk, wv)
            kv_all = lax.all_gather(kv5, 'cp', axis=0, tiled=True)
            last = spread(kv)
            attn = flash(fast, sig, q5, kv_all)
            out = finish(attn, mid, ng, wo, w_gate, w_up, w_down)
            return out, k5, v5, last[:, 0:HEAD], last[:, HEAD:]

        out, k5, v5, kl, vl = lax.cond(safe, lambda: run(True), lambda: run(False))
        return out, k5[:, None, :], v5[:, None, :], kl[:, None, :], vl[:, None, :]

    return jax.shard_map(shard_body, mesh=mesh, in_specs=(P('cp'), P(), P(), P(), P(), P(), P(), P(), P(), P()),
                         out_specs=(P('cp'), P('cp'), P('cp'), P(), P()), check_vma=False)
```

```python
import functools

import numpy as np
import jax
import jax.numpy as jnp
from jax import lax
from jax.experimental import pallas as pl
from jax.experimental.pallas import tpu as pltpu
from jax.sharding import PartitionSpec as P

WINDOW = 1024
EPS = 1e-6
BASES = (10000.0, 1000000.0)
SCALES = (1.0, 8.0)
HEAD = 256
TOK = 1024
D = 640
FF = 2048
TILE = 256
LO = 32
LOG2E = 1.4426950408889634
COEF = LOG2E / 16.0
TOP = 36.0
LIMIT = 56.0
NEG = -1e30
F32 = jnp.float32
BF16 = jnp.bfloat16
VLIM = 58 << 20


def rope_const(layer, seq_len):
    base, scale = BASES[layer], SCALES[layer]
    freq = base ** (-np.arange(HEAD // 2, dtype=np.float64) * 2.0 / HEAD)
    hi = (np.arange(seq_len // LO) * LO / scale)[:, None] * freq[None, :]
    lo = (np.arange(LO) / scale)[:, None] * freq[None, :]
    hi_tab = np.concatenate([np.cos(hi), np.sin(hi)], axis=1).astype(np.float32)
    lo_tab = np.concatenate([np.cos(lo), np.sin(lo)], axis=1).astype(np.float32)
    return hi_tab, lo_tab


def rms(x, gain):
    return x * lax.rsqrt(jnp.mean(x * x, axis=-1, keepdims=True) + EPS) * gain


def cos_sin(hi_ref, lo_ref, row0, rows):
    n_hi = rows // LO
    hi = hi_ref[pl.ds(pl.multiple_of(row0 // LO, 8), n_hi), :]
    lo = lo_ref[...]
    ch, sh = hi[:, None, 0:128], hi[:, None, 128:256]
    cl, sl = lo[None, :, 0:128], lo[None, :, 128:256]
    cos = (ch * cl - sh * sl).reshape(rows, 128)
    sin = (sh * cl + ch * sl).reshape(rows, 128)
    return cos, sin


def rotate(x, cos, sin):
    a, b = x[:, 0:128], x[:, 128:256]
    return jnp.concatenate([a * cos - b * sin, b * cos + a * sin], axis=1).astype(BF16)


def head_rope(proj, gain, cos, sin):
    return rotate(rms(proj.astype(BF16).astype(F32), gain), cos, sin)


def dot(a, b):
    return jnp.dot(a, b, preferred_element_type=F32)


def dot_t(a, b):
    return lax.dot_general(a, b, (((1,), (1,)), ((), ())), preferred_element_type=F32)


def qkv_tile(normed, gq, gk, wq, wk, wv, cos, sin, q_ref, kv_ref, k_ref, v_ref):
    k = head_rope(dot(normed, wk[...]), gk, cos, sin)
    v = dot(normed, wv[...]).astype(BF16)
    kv_ref[:, 0:HEAD] = k
    kv_ref[:, HEAD:2 * HEAD] = v
    k_ref[...] = k
    v_ref[...] = v
    for h in range(4):
        q_ref[h] = head_rope(dot(normed, wq[:, h * HEAD:(h + 1) * HEAD]), gq, cos, sin)


def proj_kernel(x_ref, ng_ref, qg_ref, hi_ref, lo_ref, wq_ref, wk_ref, wv_ref, q_ref, kv_ref, k_ref, v_ref):
    i = pl.program_id(0)
    row0 = lax.axis_index('cp') * TOK + i * TILE
    cos, sin = cos_sin(hi_ref, lo_ref, row0, TILE)
    normed = rms(x_ref[...].astype(F32), 1.0 + ng_ref[0:1, :]).astype(BF16)
    qkv_tile(normed, 1.0 + qg_ref[0:1, :], 1.0 + qg_ref[1:2, :], wq_ref, wk_ref, wv_ref, cos, sin, q_ref, kv_ref, k_ref, v_ref)


def whole(shape):
    zeros = (0,) * len(shape)
    return pl.BlockSpec(shape, lambda *_: zeros, pipeline_mode=pl.Buffered(1))


def layer_of(layer, shape):
    idx = (layer,) + (0,) * len(shape)
    return pl.BlockSpec((None,) + shape, lambda *_: idx, pipeline_mode=pl.Buffered(1))


def rows_spec(cols):
    return pl.BlockSpec((TILE, cols), lambda i: (i, 0))


Q_SPEC = pl.BlockSpec((4, TILE, HEAD), lambda i: (0, i, 0))
Q_SHAPE = jax.ShapeDtypeStruct((4, TOK, HEAD), BF16)
KV_SHAPE = jax.ShapeDtypeStruct((TOK, 2 * HEAD), BF16)
K_SHAPE = jax.ShapeDtypeStruct((TOK, HEAD), BF16)
X_SHAPE = jax.ShapeDtypeStruct((TOK, D), BF16)


def project(layer, x, ng, qg, hi, lo, wq, wk, wv):
    return pl.pallas_call(
        proj_kernel,
        grid=(TOK // TILE,),
        in_specs=[rows_spec(D), layer_of(layer, (4, D)), layer_of(layer, (2, HEAD)), whole(hi.shape), whole(lo.shape),
                  layer_of(layer, (D, 4 * HEAD)), layer_of(layer, (D, HEAD)), layer_of(layer, (D, HEAD))],
        out_specs=[Q_SPEC, rows_spec(2 * HEAD), rows_spec(HEAD), rows_spec(HEAD)],
        out_shape=[Q_SHAPE, KV_SHAPE, K_SHAPE, K_SHAPE],
        name=f"project{layer}",
        compiler_params=pltpu.CompilerParams(vmem_limit_bytes=VLIM),
        cost_estimate=pl.CostEstimate(flops=2 * TOK * D * 1536, bytes_accessed=8 << 20, transcendentals=0),
    )(x, ng, qg, hi, lo, wq, wk, wv)


def finish_tile(x, attn, ng, wo, wg, wu, wd):
    o = dot(attn, wo).astype(BF16).astype(F32)
    h1 = (x.astype(F32) + rms(o, 1.0 + ng[1:2, :])).astype(BF16)
    b = rms(h1.astype(F32), 1.0 + ng[2:3, :]).astype(BF16)
    acc = None
    step = 512
    for f in range(0, FF, step):
        g = dot(b, wg[:, f:f + step])
        u = dot(b, wu[:, f:f + step])
        m = (jax.nn.gelu(g, approximate=True) * u).astype(BF16)
        part = dot(m, wd[f:f + step, :])
        acc = part if acc is None else acc + part
    o2 = acc.astype(BF16).astype(F32)
    return (h1.astype(F32) + rms(o2, 1.0 + ng[3:4, :])).astype(BF16)


def local_tile(q_ref, halo_ref, own_ref, win_ref, sigma, fast):
    i = pl.program_id(0)
    first = lax.axis_index('cp') == 0

    @pl.when(i == 0)
    def _():
        win_ref[0:WINDOW, :] = halo_ref[...]
        win_ref[WINDOW:WINDOW + TOK, :] = own_ref[...]

    n_key = WINDOW + TILE
    start = pl.multiple_of(i * TILE, TILE)
    ks = win_ref[pl.ds(start, n_key), 0:HEAD]
    vs = win_ref[pl.ds(start, n_key), HEAD:2 * HEAD]
    col = lax.broadcasted_iota(jnp.int32, (1, n_key), 1)
    hidden = jnp.logical_and(first, col + start < WINDOW)
    r = lax.broadcasted_iota(jnp.int32, (TILE, TILE), 0)
    c = lax.broadcasted_iota(jnp.int32, (TILE, TILE), 1)
    outs = []
    for h in range(4):
        s = dot_t(q_ref[h], ks)
        if fast:
            t = s * COEF + jnp.where(hidden, NEG, -sigma)
        else:
            t = s * COEF + jnp.where(hidden, NEG, 0.0)
        t = jnp.concatenate([jnp.where(c > r, t[:, 0:TILE], NEG), t[:, TILE:WINDOW], jnp.where(c <= r, t[:, WINDOW:], NEG)], axis=1)
        if not fast:
            t = t - jnp.max(t, axis=1, keepdims=True)
        p = jnp.exp2(t)
        total = jnp.sum(p, axis=1, keepdims=True)
        outs.append((dot(p.astype(BF16), vs) / total).astype(BF16))
    return jnp.concatenate(outs, axis=1)


def mid_kernel(fast, sig_ref, q_ref, halo_ref, own_ref, x_ref, ng_ref, ng2_ref, qg_ref, hi_ref, lo_ref,
               wo_hbm, wg_hbm, wu_hbm, wd_hbm, wq_hbm, wk_hbm, wv_hbm,
               mid_ref, q2_ref, kv_ref, k_ref, v_ref,
               win_ref, wo, wg, wu, wd, wq, wk, wv, sems):
    i = pl.program_id(0)
    pairs = [(wo_hbm.at[0], wo), (wg_hbm.at[0], wg), (wu_hbm.at[0], wu), (wd_hbm.at[0], wd),
             (wq_hbm.at[1], wq), (wk_hbm.at[1], wk), (wv_hbm.at[1], wv)]
    copies = [pltpu.make_async_copy(s, d, sems.at[n]) for n, (s, d) in enumerate(pairs)]

    @pl.when(i == 0)
    def _():
        for cp in copies:
            cp.start()

    attn = local_tile(q_ref, halo_ref, own_ref, win_ref, sig_ref[0], fast)

    @pl.when(i == 0)
    def _():
        for cp in copies:
            cp.wait()

    mid = finish_tile(x_ref[...], attn, ng_ref, wo[...], wg, wu, wd)
    mid_ref[...] = mid
    row0 = lax.axis_index('cp') * TOK + i * TILE
    cos, sin = cos_sin(hi_ref, lo_ref, row0, TILE)
    normed = rms(mid.astype(F32), 1.0 + ng2_ref[0:1, :]).astype(BF16)
    qkv_tile(normed, 1.0 + qg_ref[0:1, :], 1.0 + qg_ref[1:2, :], wq, wk, wv, cos, sin, q2_ref, kv_ref, k_ref, v_ref)


ANY = pl.BlockSpec(memory_space=pl.ANY)
SMEM = pl.BlockSpec(memory_space=pltpu.SMEM)
FIN_SCRATCH = [pltpu.VMEM((4 * HEAD, D), BF16), pltpu.VMEM((D, FF), BF16), pltpu.VMEM((D, FF), BF16), pltpu.VMEM((FF, D), BF16)]


def middle(fast, sig, q, halo, own, x, ng, qg, hi, lo, wo, wg, wu, wd, wq, wk, wv):
    return pl.pallas_call(
        functools.partial(mid_kernel, fast),
        grid=(TOK // TILE,),
        in_specs=[SMEM, Q_SPEC, whole((TOK, 2 * HEAD)), whole((TOK, 2 * HEAD)), rows_spec(D), layer_of(0, (4, D)), layer_of(1, (4, D)),
                  layer_of(1, (2, HEAD)), whole(hi.shape), whole(lo.shape)] + [ANY] * 7,
        out_specs=[rows_spec(D), Q_SPEC, rows_spec(2 * HEAD), rows_spec(HEAD), rows_spec(HEAD)],
        out_shape=[X_SHAPE, Q_SHAPE, KV_SHAPE, K_SHAPE, K_SHAPE],
        scratch_shapes=[pltpu.VMEM((WINDOW + TOK, 2 * HEAD), BF16)] + FIN_SCRATCH +
                       [pltpu.VMEM((D, 4 * HEAD), BF16), pltpu.VMEM((D, HEAD), BF16), pltpu.VMEM((D, HEAD), BF16), pltpu.SemaphoreType.DMA((7,))],
        name="middle",
        compiler_params=pltpu.CompilerParams(vmem_limit_bytes=VLIM),
        cost_estimate=pl.CostEstimate(flops=18 * 10**9, bytes_accessed=20 << 20, transcendentals=0),
    )(sig, q, halo, own, x, ng, ng, qg, hi, lo, wo, wg, wu, wd, wq, wk, wv)


def finish_kernel(attn_ref, x_ref, ng_ref, wo_hbm, wg_hbm, wu_hbm, wd_hbm, out_ref, wo, wg, wu, wd, sems):
    i = pl.program_id(0)
    pairs = [(wo_hbm.at[1], wo), (wg_hbm.at[1], wg), (wu_hbm.at[1], wu), (wd_hbm.at[1], wd)]
    copies = [pltpu.make_async_copy(s, d, sems.at[n]) for n, (s, d) in enumerate(pairs)]

    @pl.when(i == 0)
    def _():
        for cp in copies:
            cp.start()
        for cp in copies:
            cp.wait()

    attn = jnp.concatenate([attn_ref[h] for h in range(4)], axis=1)
    out_ref[...] = finish_tile(x_ref[...], attn, ng_ref, wo[...], wg, wu, wd)


def finish(attn, x, ng, wo, wg, wu, wd):
    return pl.pallas_call(
        finish_kernel,
        grid=(TOK // TILE,),
        in_specs=[Q_SPEC, rows_spec(D), layer_of(1, (4, D))] + [ANY] * 4,
        out_specs=rows_spec(D),
        out_shape=X_SHAPE,
        scratch_shapes=FIN_SCRATCH + [pltpu.SemaphoreType.DMA((4,))],
        name="finish",
        compiler_params=pltpu.CompilerParams(vmem_limit_bytes=VLIM),
        cost_estimate=pl.CostEstimate(flops=10 * 10**9, bytes_accessed=12 << 20, transcendentals=0),
    )(attn, x, ng, wo, wg, wu, wd)


MESH = pl.DeviceIdType.MESH
HALF = TOK // 2
N_SLOT = 7


def flash_kernel(fast, sig_ref, q_ref, kv_ref, o_ref, buf, acc, l, m, first_sem, pass_sem, over_sem, recv):
    me = lax.axis_index('cp')
    core = me % 2
    chip = me // 2
    partner = me + 1 - 2 * core
    xnb = me + 2 - 4 * (chip % 2)
    ynb = me + 4 - 8 * (chip // 2)
    sigma = sig_ref[1]

    barrier = pltpu.get_barrier_semaphore()
    for other in (partner, xnb, ynb):
        pl.semaphore_signal(barrier, inc=1, device_id=(other,), device_id_type=MESH)
    pl.semaphore_wait(barrier, 3)

    def send(src, dst, ssem, rsem, dev):
        return pltpu.make_async_remote_copy(src_ref=src, dst_ref=dst, send_sem=ssem, recv_sem=rsem, device_id=(dev,), device_id_type=MESH)

    def half(ref, h):
        return ref.at[pl.ds(h * HALF, HALF)]

    to_partner = send(kv_ref, buf.at[0], first_sem.at[0], recv.at[0, 0], partner)
    own_a = [send(half(kv_ref, h), half(buf.at[1 + h], 0), first_sem.at[1 + 2 * h + n], recv.at[1 + h, 0], dev)
             for h in range(2) for n, dev in enumerate((xnb, ynb))]
    own_b = [send(half(kv_ref, h), half(buf.at[1 + 2 * h], 0), first_sem.at[1 + h], recv.at[1 + 2 * h, 0], ynb) for h in range(2)]
    own_c = [send(half(kv_ref, h), half(buf.at[1 + 2 * h], 1), first_sem.at[1 + h], recv.at[1 + 2 * h, 1], xnb) for h in range(2)]
    plan = [(core == 0, [to_partner]), (chip == 0, own_a), (chip == 1, own_b), (chip == 2, own_c)]
    for cond, copies in plan:
        @pl.when(cond)
        def _(copies=copies):
            for cp in copies:
                cp.start()

    def relay(s, start):
        far = chip == 3
        whole_pass = send(buf.at[s], buf.at[jnp.minimum(s + 1, N_SLOT - 1)], pass_sem.at[s], recv.at[jnp.minimum(s + 1, N_SLOT - 1), 0], partner)
        half_pass = send(half(buf.at[s], 0), half(buf.at[s], 1), pass_sem.at[s], recv.at[s, 1], partner)
        back = s // 2 + 3
        to_c = send(half(buf.at[s], 0), half(buf.at[back], 0), over_sem.at[s], recv.at[back, 0], xnb)
        to_d = send(half(buf.at[s], 0), half(buf.at[5], jnp.clip(s - 1, 0, 1)), over_sem.at[s], recv.at[5, jnp.clip(s - 1, 0, 1)],
                    jnp.where(chip == 1, ynb, xnb))
        near = jnp.logical_or(jnp.logical_and(chip == 1, core == 0), jnp.logical_and(chip == 2, core == 1))
        jobs = [(jnp.logical_and(far, s % 2 == 1), whole_pass),
                (jnp.logical_and(far, jnp.logical_or(s == 1, s == 3)), to_c),
                (jnp.logical_not(far), half_pass),
                (jnp.logical_and(near, s <= 2), to_d)]
        return jobs

    def attend(ks, vs, rows, width, masked, first):
        n = rows.size
        if masked:
            r = lax.broadcasted_iota(jnp.int32, (n, n), 0)
            vis = lax.broadcasted_iota(jnp.int32, (n, n), 1) <= r
        for h in range(4):
            s = dot_t(q_ref[h, rows, :], ks)
            t = s * COEF - sigma if fast else s * COEF
            if masked:
                tail = jnp.where(vis, t[:, width - n:], NEG)
                t = tail if width == n else jnp.concatenate([t[:, 0:width - n], tail], axis=1)
            if not fast:
                top = jnp.broadcast_to(jnp.max(t, axis=1, keepdims=True), (n, 128))
                fresh = top if first else jnp.maximum(m[h, rows, :], top)
                if not first:
                    decay = jnp.exp2(m[h, rows, :] - fresh)
                    l[h, rows, :] = l[h, rows, :] * decay
                    acc[h, rows, :] = acc[h, rows, :] * decay[:, 0:1]
                m[h, rows, :] = fresh
                t = t - fresh[:, 0:1]
            p = jnp.exp2(t)
            lp = p[:, 0:128]
            for j in range(1, width // 128):
                lp = lp + p[:, j * 128:(j + 1) * 128]
            o = dot(p.astype(BF16), vs)
            if first:
                l[h, rows, :] = lp
                acc[h, rows, :] = o
            else:
                l[h, rows, :] += lp
                acc[h, rows, :] += o

    for i in range(4):
        width = (i + 1) * TILE
        attend(kv_ref[0:width, 0:HEAD], kv_ref[0:width, HEAD:2 * HEAD], pl.ds(i * TILE, TILE), width, True, True)

    def slot(s):
        ks = buf[s, :, 0:HEAD]
        vs = buf[s, :, HEAD:2 * HEAD]

        def q_rows(i, carry):
            attend(ks, vs, pl.ds(pl.multiple_of(i * QROWS, QROWS), QROWS), TOK, False, False)
            return carry

        lax.fori_loop(0, TOK // QROWS, q_rows, 0)

    def arrive(s, h):
        send(half(buf.at[s], 0), half(buf.at[s], h), pass_sem.at[s], recv.at[s, h], partner).wait_recv()

    def step(s, carry):
        @pl.when(jnp.logical_and(s == 0, core == 1))
        def _():
            send(kv_ref, buf.at[0], pass_sem.at[0], recv.at[0, 0], partner).wait_recv()

        @pl.when(s >= 1)
        def _():
            @pl.when(chip == 3)
            def _():
                @pl.when(s % 2 == 1)
                def _():
                    arrive(s, 0)
                    arrive(s, 1)

                @pl.when(s % 2 == 0)
                def _():
                    send(buf.at[s], buf.at[s], pass_sem.at[s], recv.at[s, 0], partner).wait_recv()

            @pl.when(chip < 3)
            def _():
                arrive(s, 0)

            for cond, cp in relay(s, True):
                @pl.when(cond)
                def _(cp=cp):
                    cp.start()

            @pl.when(chip < 3)
            def _():
                arrive(s, 1)

        @pl.when(jnp.logical_or(s >= 1, core == 1))
        def _():
            slot(s)

        return carry

    lax.fori_loop(0, 2 * chip + 1, step, 0)

    for h in range(4):
        total = jnp.sum(l[h], axis=1, keepdims=True)
        o_ref[h] = (acc[h] / total).astype(BF16)

    for cond, copies in plan:
        @pl.when(cond)
        def _(copies=copies):
            for cp in copies:
                cp.wait_send()

    def drain(s, carry):
        for cond, cp in relay(s, False):
            @pl.when(cond)
            def _(cp=cp):
                cp.wait_send()
        return carry

    lax.fori_loop(1, 2 * chip + 1, drain, 0)


QROWS = 512


def flash(fast, sig, q, kv):
    vm = pl.BlockSpec(memory_space=pltpu.VMEM)
    return pl.pallas_call(
        functools.partial(flash_kernel, fast),
        in_specs=[SMEM, vm, vm],
        out_specs=vm,
        out_shape=Q_SHAPE,
        scratch_shapes=[pltpu.VMEM((N_SLOT, TOK, 2 * HEAD), BF16), pltpu.VMEM((4, TOK, HEAD), F32), pltpu.VMEM((4, TOK, 128), F32),
                        pltpu.VMEM((4, TOK, 128), F32), pltpu.SemaphoreType.DMA((5,)), pltpu.SemaphoreType.DMA((N_SLOT,)),
                        pltpu.SemaphoreType.DMA((N_SLOT,)), pltpu.SemaphoreType.DMA((N_SLOT, 2))],
        name="flash_fast" if fast else "flash_safe",
        compiler_params=pltpu.CompilerParams(vmem_limit_bytes=VLIM, collective_id=0 if fast else 1, has_side_effects=True),
        cost_estimate=pl.CostEstimate(flops=32 * 10**9, bytes_accessed=12 << 20, transcendentals=0),
    )(sig, q, kv)


def score_bound(qk_gain):
    g = jnp.abs(1.0 + qk_gain)
    pair = jnp.maximum(g[:, 0:HEAD // 2], g[:, HEAD // 2:])
    return 16.0 * 1.02 * jnp.max(pair[0] * pair[1])


def solution(mesh):
    n_dev = mesh.shape['cp']
    rope = [rope_const(layer, TOK * n_dev) for layer in range(2)]
    rounds = [[(7, 5)], [(7, 3), (5, 1)], [(7, 6), (5, 4), (3, 2), (1, 0)]]

    def hop(got, pairs):
        me = lax.axis_index('cp')
        new = lax.ppermute(got, 'cp', perm=pairs)
        takes = functools.reduce(jnp.logical_or, [me == r for _, r in pairs])
        return jnp.where(takes, new, got)

    def shard_body(x, ng, qg, w_q, w_k, w_v, w_o, w_gate, w_up, w_down):
        wq = w_q.reshape(2, D, 4 * HEAD)
        wk = w_k.reshape(2, D, HEAD)
        wv = w_v.reshape(2, D, HEAD)
        wo = w_o.reshape(2, 4 * HEAD, D)
        bounds = [score_bound(qg[layer]) for layer in range(2)]
        safe = jnp.maximum(bounds[0], bounds[1]) <= LIMIT
        sig = jnp.stack([jnp.maximum(b - TOP, 0.0) * LOG2E for b in bounds])

        def run(fast):
            q, kv, _, _ = project(0, x, ng, qg, *rope[0], wq, wk, wv)
            halo = lax.ppermute(kv, 'cp', perm=[(s, s + 1) for s in range(n_dev - 1)])
            mid, q5, kv5, k5, v5 = middle(fast, sig, q, halo, kv, x, ng, qg, *rope[1], wo, w_gate, w_up, w_down, wq, wk, wv)
            got = hop(kv, rounds[0])
            got, kv5 = lax.optimization_barrier((got, kv5))
            got = hop(got, rounds[1])
            attn = flash(fast, sig, q5, kv5)
            got, attn = lax.optimization_barrier((got, attn))
            last = hop(got, rounds[2])
            out = finish(attn, mid, ng, wo, w_gate, w_up, w_down)
            return out, k5, v5, last[:, 0:HEAD], last[:, HEAD:]

        out, k5, v5, kl, vl = lax.cond(safe, lambda: run(True), lambda: run(False))
        return out, k5[:, None, :], v5[:, None, :], kl[:, None, :], vl[:, None, :]

    return jax.shard_map(shard_body, mesh=mesh, in_specs=(P('cp'), P(), P(), P(), P(), P(), P(), P(), P(), P()),
                         out_specs=(P('cp'), P('cp'), P('cp'), P(), P()), check_vma=False)
```

```python
import functools

import numpy as np
import jax
import jax.numpy as jnp
from jax import lax
from jax.experimental import pallas as pl
from jax.experimental.pallas import tpu as pltpu
from jax.sharding import PartitionSpec as P

WINDOW = 1024
EPS = 1e-6
BASES = (10000.0, 1000000.0)
SCALES = (1.0, 8.0)
HEAD = 256
TOK = 1024
D = 640
FF = 2048
TILE = 256
LO = 32
LOG2E = 1.4426950408889634
COEF = LOG2E / 16.0
TOP = 36.0
LIMIT = 56.0
NEG = -1e30
F32 = jnp.float32
BF16 = jnp.bfloat16
VLIM = 58 << 20


def rope_const(layer, seq_len):
    base, scale = BASES[layer], SCALES[layer]
    freq = base ** (-np.arange(HEAD // 2, dtype=np.float64) * 2.0 / HEAD)
    hi = (np.arange(seq_len // LO) * LO / scale)[:, None] * freq[None, :]
    lo = (np.arange(LO) / scale)[:, None] * freq[None, :]
    hi_tab = np.concatenate([np.cos(hi), np.sin(hi)], axis=1).astype(np.float32)
    lo_tab = np.concatenate([np.cos(lo), np.sin(lo)], axis=1).astype(np.float32)
    return hi_tab, lo_tab


def rms(x, gain):
    return x * lax.rsqrt(jnp.mean(x * x, axis=-1, keepdims=True) + EPS) * gain


def cos_sin(hi_ref, lo_ref, row0, rows):
    n_hi = rows // LO
    hi = hi_ref[pl.ds(pl.multiple_of(row0 // LO, 8), n_hi), :]
    lo = lo_ref[...]
    ch, sh = hi[:, None, 0:128], hi[:, None, 128:256]
    cl, sl = lo[None, :, 0:128], lo[None, :, 128:256]
    cos = (ch * cl - sh * sl).reshape(rows, 128)
    sin = (sh * cl + ch * sl).reshape(rows, 128)
    return cos, sin


def rotate(x, cos, sin):
    a, b = x[:, 0:128], x[:, 128:256]
    return jnp.concatenate([a * cos - b * sin, b * cos + a * sin], axis=1).astype(BF16)


def head_rope(proj, gain, cos, sin):
    return rotate(rms(proj.astype(BF16).astype(F32), gain), cos, sin)


def dot(a, b):
    return jnp.dot(a, b, preferred_element_type=F32)


def dot_t(a, b):
    return lax.dot_general(a, b, (((1,), (1,)), ((), ())), preferred_element_type=F32)


MESH = pl.DeviceIdType.MESH
N_SLOT = 7
N_TILE = TOK // TILE
QROWS = 512
FROWS = 512
FSTEP = 512


def finish_rows(x, attn, ng, wo, wg, wu, wd):
    o = dot(attn, wo[...]).astype(BF16).astype(F32)
    h1 = (x.astype(F32) + rms(o, 1.0 + ng[1:2, :])).astype(BF16)
    b = rms(h1.astype(F32), 1.0 + ng[2:3, :]).astype(BF16)
    acc = None
    for f in range(0, FF, FSTEP):
        g = dot(b, wg[:, f:f + FSTEP])
        u = dot(b, wu[:, f:f + FSTEP])
        m = (jax.nn.gelu(g, approximate=True) * u).astype(BF16)
        part = dot(m, wd[f:f + FSTEP, :])
        acc = part if acc is None else acc + part
    o2 = acc.astype(BF16).astype(F32)
    return (h1.astype(F32) + rms(o2, 1.0 + ng[3:4, :])).astype(BF16)


def layers_kernel(fast, sig_ref, ng_ref, qg_ref, hi4_ref, lo4_ref, hi5_ref, lo5_ref, x_hbm, wq_hbm, wk_hbm, wv_hbm, wo_hbm, wg_hbm, wu_hbm, wd_hbm,
                  out_hbm, k_hbm, v_hbm, kl_hbm, vl_hbm,
                  x, mid, win, kv5, q, buf, acc, l, m, last, xo, wq, wk, wv, wo, wg, wu, wd,
                  load_sem, out_sem, halo_send, halo_recv, hop_send, hop_recv, pass_send, over_send, wide_recv, last_send, last_recv):
    me = lax.axis_index('cp')
    core = me % 2
    chip = me // 2
    partner = me + 1 - 2 * core
    xnb = me + 2 - 4 * (chip % 2)
    ynb = me + 4 - 8 * (chip // 2)
    top = 7
    is_last = me == top

    def load(src, dst, n):
        return pltpu.make_async_copy(src, dst, load_sem.at[n])

    early = [load(x_hbm, x, 0), load(wk_hbm.at[0], wk.at[0], 1), load(wv_hbm.at[0], wv.at[0], 2), load(wq_hbm.at[0], wq.at[0], 3)]
    ff4 = [load(wo_hbm.at[0], wo, 4), load(wg_hbm.at[0], wg, 5), load(wu_hbm.at[0], wu, 6), load(wd_hbm.at[0], wd, 7)]
    next_qkv = [load(wk_hbm.at[1], wk.at[1], 8), load(wv_hbm.at[1], wv.at[1], 9), load(wq_hbm.at[1], wq.at[1], 10)]
    ff5 = [load(wo_hbm.at[1], wo, 4), load(wg_hbm.at[1], wg, 5), load(wu_hbm.at[1], wu, 6), load(wd_hbm.at[1], wd, 7)]
    for cp in early:
        cp.start()

    if fast:
        barrier = pltpu.get_barrier_semaphore()
        for other in (partner, xnb, ynb, (me + 1) % 8, (me + 7) % 8):
            pl.semaphore_signal(barrier, inc=1, device_id=(other,), device_id_type=MESH)
    for cp in ff4 + next_qkv:
        cp.start()

    @pl.when(me == 0)
    def _():
        win[0:WINDOW, :] = jnp.zeros((WINDOW, 2 * HEAD), BF16)

    if fast:
        pl.semaphore_wait(barrier, 5)

    def send(src, dst, ssem, rsem, dev):
        return pltpu.make_async_remote_copy(src_ref=src, dst_ref=dst, send_sem=ssem, recv_sem=rsem, device_id=(dev,), device_id_type=MESH)

    def on(cond, copy, act):
        @pl.when(cond)
        def _():
            getattr(copy, act)()

    def rows_of(t, n=TILE):
        return pl.ds(pl.multiple_of(t * n, n), n)

    def halo_copy(t):
        return send(win.at[rows_of(t + N_TILE)], win.at[rows_of(t)], halo_send.at[t], halo_recv.at[t], (me + 1) % 8)

    g4q, g4k = 1.0 + qg_ref[0, 0:1, :], 1.0 + qg_ref[0, 1:2, :]
    g5q, g5k = 1.0 + qg_ref[1, 0:1, :], 1.0 + qg_ref[1, 1:2, :]
    for cp in early[:3]:
        cp.wait()

    def kv_tile(it, carry):
        t = N_TILE - 1 - it
        cos, sin = cos_sin(hi4_ref, lo4_ref, me * TOK + t * TILE, TILE)
        a = rms(x[rows_of(t), :].astype(F32), 1.0 + ng_ref[0, 0:1, :]).astype(BF16)
        win[rows_of(t + N_TILE), 0:HEAD] = head_rope(dot(a, wk[0]), g4k, cos, sin)
        win[rows_of(t + N_TILE), HEAD:2 * HEAD] = dot(a, wv[0]).astype(BF16)
        on(me < top, halo_copy(t), 'start')
        return carry

    lax.fori_loop(0, N_TILE, kv_tile, 0)
    own4 = win.at[pl.ds(WINDOW, TOK)]
    last_cps = [send(own4, last, last_send.at[n], last_recv, dev) for n, dev in enumerate((partner, xnb, ynb))]
    for cp in last_cps:
        on(is_last, cp, 'start')
    early[3].wait()
    for cp in ff4 + next_qkv:
        cp.wait()

    def hops(t):
        def hop(k, slot, rk, dev):
            return send(kv5.at[rows_of(t)], buf.at[slot, rows_of(t)], hop_send.at[k, t], hop_recv.at[rk, t], dev)
        return [(core == 0, hop(0, 0, 0, partner)),
                (chip == 0, hop(1, 1, 1, xnb)),
                (chip == 0, hop(2, 1, 1, ynb)),
                (chip == 1, hop(2, 1, 1, ynb)),
                (chip == 2, hop(1, 3, 2, xnb))]

    sig4, sig5 = sig_ref[0], sig_ref[1]
    n_key = WINDOW + TILE

    def layer_tile(it, carry):
        t = N_TILE - 1 - it
        rows = rows_of(t)
        cos, sin = cos_sin(hi4_ref, lo4_ref, me * TOK + t * TILE, TILE)
        a = rms(x[rows, :].astype(F32), 1.0 + ng_ref[0, 0:1, :]).astype(BF16)
        qs = [head_rope(dot(a, wq[0, :, h * HEAD:(h + 1) * HEAD]), g4q, cos, sin) for h in range(4)]

        on(me > 0, halo_copy(t), 'wait_recv')
        start = pl.multiple_of(t * TILE, TILE)
        ks = win[pl.ds(start, n_key), 0:HEAD]
        vs = win[pl.ds(start, n_key), HEAD:2 * HEAD]
        col = lax.broadcasted_iota(jnp.int32, (1, n_key), 1)
        hidden = jnp.logical_and(me == 0, col + start < WINDOW)
        bias = jnp.where(hidden, NEG, -sig4 if fast else 0.0)
        r = lax.broadcasted_iota(jnp.int32, (TILE, TILE), 0)
        c = lax.broadcasted_iota(jnp.int32, (TILE, TILE), 1)
        outs = []
        for h in range(4):
            s = dot_t(qs[h], ks) * COEF + bias
            s = jnp.concatenate([jnp.where(c > r, s[:, 0:TILE], NEG), s[:, TILE:WINDOW], jnp.where(c <= r, s[:, WINDOW:], NEG)], axis=1)
            if not fast:
                s = s - jnp.max(s, axis=1, keepdims=True)
            p = jnp.exp2(s)
            total = jnp.sum(p, axis=1, keepdims=True)
            outs.append((dot(p.astype(BF16), vs) / total).astype(BF16))
        h_mid = finish_rows(x[rows, :], jnp.concatenate(outs, axis=1), ng_ref[0], wo, wg, wu, wd)
        mid[rows, :] = h_mid
        cos, sin = cos_sin(hi5_ref, lo5_ref, me * TOK + t * TILE, TILE)
        a = rms(h_mid.astype(F32), 1.0 + ng_ref[1, 0:1, :]).astype(BF16)
        kv5[rows, 0:HEAD] = head_rope(dot(a, wk[1]), g5k, cos, sin)
        kv5[rows, HEAD:2 * HEAD] = dot(a, wv[1]).astype(BF16)
        for h in range(4):
            q[h, rows, :] = head_rope(dot(a, wq[1, :, h * HEAD:(h + 1) * HEAD]), g5q, cos, sin)
        for cond, cp in hops(t):
            on(cond, cp, 'start')
        return carry

    lax.fori_loop(0, N_TILE, layer_tile, 0)
    outs5 = [pltpu.make_async_copy(kv5.at[:, pl.ds(0, HEAD)], k_hbm, out_sem.at[0]), pltpu.make_async_copy(kv5.at[:, pl.ds(HEAD, HEAD)], v_hbm, out_sem.at[1])]
    for cp in outs5 + ff5:
        cp.start()

    def attend(ks, vs, rows, width, masked, first):
        n = rows.size
        if masked:
            r = lax.broadcasted_iota(jnp.int32, (n, n), 0)
            vis = lax.broadcasted_iota(jnp.int32, (n, n), 1) <= r
        for h in range(4):
            s = dot_t(q[h, rows, :], ks)
            t = s * COEF - sig5 if fast else s * COEF
            if masked:
                tail = jnp.where(vis, t[:, width - n:], NEG)
                t = tail if width == n else jnp.concatenate([t[:, 0:width - n], tail], axis=1)
            if not fast:
                mx = jnp.broadcast_to(jnp.max(t, axis=1, keepdims=True), (n, 128))
                fresh = mx if first else jnp.maximum(m[h, rows, :], mx)
                if not first:
                    decay = jnp.exp2(m[h, rows, :] - fresh)
                    l[h, rows, :] = l[h, rows, :] * decay
                    acc[h, rows, :] = acc[h, rows, :] * decay[:, 0:1]
                m[h, rows, :] = fresh
                t = t - fresh[:, 0:1]
            p = jnp.exp2(t)
            lp = p[:, 0:128]
            for j in range(1, width // 128):
                lp = lp + p[:, j * 128:(j + 1) * 128]
            o = dot(p.astype(BF16), vs)
            if first:
                l[h, rows, :] = lp
                acc[h, rows, :] = o
            else:
                l[h, rows, :] += lp
                acc[h, rows, :] += o

    for i in range(N_TILE):
        width = (i + 1) * TILE
        attend(kv5[0:width, 0:HEAD], kv5[0:width, HEAD:2 * HEAD], pl.ds(i * TILE, TILE), width, True, True)

    def slot(s):
        ks = buf[s, :, 0:HEAD]
        vs = buf[s, :, HEAD:2 * HEAD]

        def q_rows(i, carry):
            attend(ks, vs, rows_of(i, QROWS), TOK, False, False)
            return carry

        lax.fori_loop(0, TOK // QROWS, q_rows, 0)

    def wide(s, dst, ssem, dev):
        return send(buf.at[s], buf.at[dst], ssem, wide_recv.at[dst], dev)

    def relay(s):
        odd = s % 2 == 1
        return [(odd, wide(s, jnp.minimum(s + 1, N_SLOT - 1), pass_send.at[s], partner)),
                (jnp.logical_and(chip == 3, s == 1), wide(s, 3, over_send, xnb)),
                (jnp.logical_and(jnp.logical_and(chip == 1, core == 0), s == 1), wide(s, 5, over_send, ynb)),
                (jnp.logical_and(jnp.logical_and(chip == 2, core == 1), s == 1), wide(s, 5, over_send, xnb))]

    def chunks_in(cond, slot_no, rk):
        @pl.when(cond)
        def _():
            def one(t, carry):
                send(kv5.at[rows_of(t)], buf.at[slot_no, rows_of(t)], hop_send.at[0, t], hop_recv.at[rk, t], partner).wait_recv()
                return carry
            lax.fori_loop(0, N_TILE, one, 0)

    gives = jnp.logical_or(me == 3, jnp.logical_or(me == 5, me == 1))
    spread = [(gives, send(last, last, last_send.at[0], last_recv, partner)), (me == 3, send(last, last, last_send.at[1], last_recv, xnb))]

    def pass_last(cond):
        @pl.when(cond)
        def _():
            send(last, last, last_send.at[2], last_recv, partner).wait_recv()
            for c, cp in spread:
                on(c, cp, 'start')

    pass_last(jnp.logical_and(gives, me > 1))

    def step(s, carry):
        chunks_in(jnp.logical_and(s == 0, core == 1), 0, 0)
        chunks_in(s == 1, 1, 1)
        chunks_in(jnp.logical_and(s == 3, chip == 3), 3, 2)

        @pl.when(jnp.logical_or(jnp.logical_and(s > 0, s % 2 == 0), jnp.logical_or(s == 5, jnp.logical_and(s == 3, chip == 2))))
        def _():
            wide(s, s, pass_send.at[s], partner).wait_recv()

        for cond, cp in relay(s):
            on(cond, cp, 'start')

        @pl.when(jnp.logical_or(s >= 1, core == 1))
        def _():
            slot(s)

        return carry

    lax.fori_loop(0, 2 * chip + 1, step, 0)
    pass_last(me == 1)

    @pl.when(jnp.logical_and(jnp.logical_not(gives), jnp.logical_not(is_last)))
    def _():
        send(last, last, last_send.at[2], last_recv, partner).wait_recv()

    def put_last(src):
        return [pltpu.make_async_copy(src.at[:, pl.ds(0, HEAD)], kl_hbm, out_sem.at[2]), pltpu.make_async_copy(src.at[:, pl.ds(HEAD, HEAD)], vl_hbm, out_sem.at[3])]

    for cp in put_last(own4):
        on(is_last, cp, 'start')
    for cp in put_last(last):
        on(jnp.logical_not(is_last), cp, 'start')

    for cp in ff5:
        cp.wait()

    def out_copy(t):
        return pltpu.make_async_copy(xo.at[rows_of(t, FROWS)], out_hbm.at[rows_of(t, FROWS)], out_sem.at[4 + t])

    def finish_tile(t, carry):
        rows = rows_of(t, FROWS)
        attn = []
        for h in range(4):
            total = jnp.sum(l[h, rows, :], axis=1, keepdims=True)
            attn.append((acc[h, rows, :] / total).astype(BF16))
        xo[rows, :] = finish_rows(mid[rows, :], jnp.concatenate(attn, axis=1), ng_ref[1], wo, wg, wu, wd)
        out_copy(t).start()
        return carry

    lax.fori_loop(0, TOK // FROWS, finish_tile, 0)

    def drain_tile(t, carry):
        on(me < top, halo_copy(t), 'wait_send')
        for cond, cp in hops(t):
            on(cond, cp, 'wait_send')
        return carry

    lax.fori_loop(0, N_TILE, drain_tile, 0)

    def drain_step(s, carry):
        for cond, cp in relay(s):
            on(cond, cp, 'wait_send')
        return carry

    lax.fori_loop(1, 2 * chip + 1, drain_step, 0)
    for cp in last_cps:
        on(is_last, cp, 'wait_send')
    for cond, cp in spread:
        on(cond, cp, 'wait_send')
    for cp in outs5 + put_last(last):
        cp.wait()
    for t in range(TOK // FROWS):
        out_copy(t).wait()


def layers(fast, sig, ng, qg, rope, x, wq, wk, wv, wo, wg, wu, wd):
    vm = pl.BlockSpec(memory_space=pltpu.VMEM)
    anyw = pl.BlockSpec(memory_space=pl.ANY)
    dma = pltpu.SemaphoreType.DMA
    kshape = jax.ShapeDtypeStruct((TOK, HEAD), BF16)
    return pl.pallas_call(
        functools.partial(layers_kernel, fast),
        in_specs=[pl.BlockSpec(memory_space=pltpu.SMEM)] + [vm] * 6 + [anyw] * 8,
        out_specs=[anyw] * 5,
        out_shape=[jax.ShapeDtypeStruct((TOK, D), BF16), kshape, kshape, kshape, kshape],
        scratch_shapes=[
            pltpu.VMEM((TOK, D), BF16), pltpu.VMEM((TOK, D), BF16), pltpu.VMEM((WINDOW + TOK, 2 * HEAD), BF16), pltpu.VMEM((TOK, 2 * HEAD), BF16),
            pltpu.VMEM((4, TOK, HEAD), BF16), pltpu.VMEM((N_SLOT, TOK, 2 * HEAD), BF16), pltpu.VMEM((4, TOK, HEAD), F32), pltpu.VMEM((4, TOK, 128), F32),
            pltpu.VMEM((8, 128) if fast else (4, TOK, 128), F32), pltpu.VMEM((TOK, 2 * HEAD), BF16), pltpu.VMEM((TOK, D), BF16),
            pltpu.VMEM((2, D, 4 * HEAD), BF16), pltpu.VMEM((2, D, HEAD), BF16), pltpu.VMEM((2, D, HEAD), BF16),
            pltpu.VMEM((4 * HEAD, D), BF16), pltpu.VMEM((D, FF), BF16), pltpu.VMEM((D, FF), BF16), pltpu.VMEM((FF, D), BF16),
            dma((11,)), dma((4 + TOK // FROWS,)), dma((N_TILE,)), dma((N_TILE,)), dma((3, N_TILE)), dma((3, N_TILE)), dma((N_SLOT,)), dma, dma((N_SLOT,)),
            dma((3,)), dma],
        name="layers_fast" if fast else "layers_safe",
        compiler_params=pltpu.CompilerParams(vmem_limit_bytes=VLIM, collective_id=0 if fast else None, has_side_effects=True),
        cost_estimate=pl.CostEstimate(flops=60 * 10**9, bytes_accessed=30 << 20, transcendentals=0),
    )(sig, ng, qg, *rope[0], *rope[1], x, wq, wk, wv, wo, wg, wu, wd)


def score_bound(qk_gains):
    g = jnp.abs(1.0 + qk_gains)
    pair = jnp.maximum(g[:, :, 0:HEAD // 2], g[:, :, HEAD // 2:])
    return 16.0 * 1.02 * jnp.max(pair[:, 0] * pair[:, 1])


def solution(mesh):
    n_dev = mesh.shape['cp']
    rope = [rope_const(layer, TOK * n_dev) for layer in range(2)]

    def shard_body(x, ng, qg, w_q, w_k, w_v, w_o, w_gate, w_up, w_down):
        wq = w_q.reshape(2, D, 4 * HEAD)
        wk = w_k.reshape(2, D, HEAD)
        wv = w_v.reshape(2, D, HEAD)
        wo = w_o.reshape(2, 4 * HEAD, D)
        bound = score_bound(qg)
        safe = bound <= LIMIT
        sig = jnp.full((2,), jnp.maximum(bound - TOP, 0.0) * LOG2E)

        def run(fast):
            return tuple(layers(fast, sig, ng, qg, rope, x, wq, wk, wv, wo, w_gate, w_up, w_down))

        start = (jnp.logical_not(safe), run(True))
        _, (out, k5, v5, kl, vl) = lax.while_loop(lambda c: c[0], lambda c: (jnp.zeros((), jnp.bool_), run(False)), start)
        return out, k5[:, None, :], v5[:, None, :], kl[:, None, :], vl[:, None, :]

    return jax.shard_map(shard_body, mesh=mesh, in_specs=(P('cp'), P(), P(), P(), P(), P(), P(), P(), P(), P()),
                         out_specs=(P('cp'), P('cp'), P('cp'), P(), P()), check_vma=False)
```

```python
import functools

import numpy as np
import jax
import jax.numpy as jnp
from jax import lax
from jax.experimental import pallas as pl
from jax.experimental.pallas import tpu as pltpu
from jax.sharding import PartitionSpec as P

WINDOW = 1024
EPS = 1e-6
BASES = (10000.0, 1000000.0)
SCALES = (1.0, 8.0)
HEAD = 256
TOK = 1024
D = 640
FF = 2048
TILE = 256
LO = 32
LOG2E = 1.4426950408889634
COEF = LOG2E / 16.0
TOP = 36.0
LIMIT = 56.0
NEG = -1e30
F32 = jnp.float32
BF16 = jnp.bfloat16
VLIM = 58 << 20


def rope_const(layer, seq_len):
    base, scale = BASES[layer], SCALES[layer]
    freq = base ** (-np.arange(HEAD // 2, dtype=np.float64) * 2.0 / HEAD)
    hi = (np.arange(seq_len // LO) * LO / scale)[:, None] * freq[None, :]
    lo = (np.arange(LO) / scale)[:, None] * freq[None, :]
    hi_tab = np.concatenate([np.cos(hi), np.sin(hi)], axis=1).astype(np.float32)
    lo_tab = np.concatenate([np.cos(lo), np.sin(lo)], axis=1).astype(np.float32)
    return hi_tab, lo_tab


def rms(x, gain):
    return x * lax.rsqrt(jnp.mean(x * x, axis=-1, keepdims=True) + EPS) * gain


def cos_sin(hi_ref, lo_ref, row0, rows):
    n_hi = rows // LO
    hi = hi_ref[pl.ds(pl.multiple_of(row0 // LO, 8), n_hi), :]
    lo = lo_ref[...]
    ch, sh = hi[:, None, 0:128], hi[:, None, 128:256]
    cl, sl = lo[None, :, 0:128], lo[None, :, 128:256]
    cos = (ch * cl - sh * sl).reshape(rows, 128)
    sin = (sh * cl + ch * sl).reshape(rows, 128)
    return cos, sin


def rotate(x, cos, sin):
    a, b = x[:, 0:128], x[:, 128:256]
    return jnp.concatenate([a * cos - b * sin, b * cos + a * sin], axis=1).astype(BF16)


def head_rope(proj, gain, cos, sin):
    return rotate(rms(proj.astype(BF16).astype(F32), gain), cos, sin)


def dot(a, b):
    return jnp.dot(a, b, preferred_element_type=F32)


def dot_t(a, b):
    return lax.dot_general(a, b, (((1,), (1,)), ((), ())), preferred_element_type=F32)


MESH = pl.DeviceIdType.MESH
N_SLOT = 7
N_TILE = TOK // TILE
QROWS = 512
FROWS = 512
FSTEP = 2048


def finish_rows(x, attn, ng, wo, wg, wu, wd):
    o = dot(attn, wo[...]).astype(BF16).astype(F32)
    h1 = (x.astype(F32) + rms(o, 1.0 + ng[1:2, :])).astype(BF16)
    b = rms(h1.astype(F32), 1.0 + ng[2:3, :]).astype(BF16)
    acc = None
    for f in range(0, FF, FSTEP):
        g = dot(b, wg[:, f:f + FSTEP])
        u = dot(b, wu[:, f:f + FSTEP])
        m = (jax.nn.gelu(g, approximate=True) * u).astype(BF16)
        part = dot(m, wd[f:f + FSTEP, :])
        acc = part if acc is None else acc + part
    o2 = acc.astype(BF16).astype(F32)
    return (h1.astype(F32) + rms(o2, 1.0 + ng[3:4, :])).astype(BF16)


def layers_kernel(fast, ng_ref, qg_ref, hi4_ref, lo4_ref, hi5_ref, lo5_ref, x_hbm, wq_hbm, wk_hbm, wv_hbm, wo_hbm, wg_hbm, wu_hbm, wd_hbm,
                  out_hbm, k_hbm, v_hbm, kl_hbm, vl_hbm, bound_ref,
                  x, mid, win, kv5, q, buf, acc, l, m, last, xo, wq, wk, wv, wo, wg, wu, wd,
                  load_sem, out_sem, halo_send, halo_recv, hop_send, hop_recv, pass_send, over_send, wide_recv, last_send, last_recv):
    me = lax.axis_index('cp')
    core = me % 2
    chip = me // 2
    partner = me + 1 - 2 * core
    xnb = me + 2 - 4 * (chip % 2)
    ynb = me + 4 - 8 * (chip // 2)
    top = 7
    is_last = me == top

    def load(src, dst, n):
        return pltpu.make_async_copy(src, dst, load_sem.at[n])

    early = [load(x_hbm, x, 0), load(wk_hbm.at[0], wk.at[0], 1), load(wv_hbm.at[0], wv.at[0], 2), load(wq_hbm.at[0], wq.at[0], 3)]
    ff4 = [load(wo_hbm.at[0], wo, 4), load(wg_hbm.at[0], wg, 5), load(wu_hbm.at[0], wu, 6), load(wd_hbm.at[0], wd, 7)]
    next_qkv = [load(wk_hbm.at[1], wk.at[1], 8), load(wv_hbm.at[1], wv.at[1], 9), load(wq_hbm.at[1], wq.at[1], 10)]
    ff5 = [load(wo_hbm.at[1], wo, 4), load(wg_hbm.at[1], wg, 5), load(wu_hbm.at[1], wu, 6), load(wd_hbm.at[1], wd, 7)]
    for cp in early:
        cp.start()

    if fast:
        barrier = pltpu.get_barrier_semaphore()
        for other in (partner, xnb, ynb, (me + 1) % 8, (me + 7) % 8):
            pl.semaphore_signal(barrier, inc=1, device_id=(other,), device_id_type=MESH)
    for cp in ff4 + next_qkv:
        cp.start()

    @pl.when(me == 0)
    def _():
        win[0:WINDOW, :] = jnp.zeros((WINDOW, 2 * HEAD), BF16)

    if fast:
        pl.semaphore_wait(barrier, 5)

    def send(src, dst, ssem, rsem, dev):
        return pltpu.make_async_remote_copy(src_ref=src, dst_ref=dst, send_sem=ssem, recv_sem=rsem, device_id=(dev,), device_id_type=MESH)

    def on(cond, copy, act):
        @pl.when(cond)
        def _():
            getattr(copy, act)()

    def rows_of(t, n=TILE):
        return pl.ds(pl.multiple_of(t * n, n), n)

    def halo_copy(t):
        return send(win.at[rows_of(t + N_TILE)], win.at[rows_of(t)], halo_send.at[t], halo_recv.at[t], (me + 1) % 8)

    gains = jnp.abs(1.0 + qg_ref[...])
    pair = jnp.maximum(gains[:, :, 0:HEAD // 2], gains[:, :, HEAD // 2:])
    bound = 16.0 * 1.02 * jnp.max(pair[:, 0:1] * pair[:, 1:2])
    bound_ref[0] = bound
    sigma = jnp.maximum(bound - TOP, 0.0) * LOG2E
    g4q, g4k = 1.0 + qg_ref[0, 0:1, :], 1.0 + qg_ref[0, 1:2, :]
    g5q, g5k = 1.0 + qg_ref[1, 0:1, :], 1.0 + qg_ref[1, 1:2, :]
    for cp in early[:3]:
        cp.wait()

    def kv_tile(it, carry):
        t = N_TILE - 1 - it
        cos, sin = cos_sin(hi4_ref, lo4_ref, me * TOK + t * TILE, TILE)
        a = rms(x[rows_of(t), :].astype(F32), 1.0 + ng_ref[0, 0:1, :]).astype(BF16)
        win[rows_of(t + N_TILE), 0:HEAD] = head_rope(dot(a, wk[0]), g4k, cos, sin)
        win[rows_of(t + N_TILE), HEAD:2 * HEAD] = dot(a, wv[0]).astype(BF16)
        on(me < top, halo_copy(t), 'start')
        return carry

    lax.fori_loop(0, N_TILE, kv_tile, 0)
    own4 = win.at[pl.ds(WINDOW, TOK)]
    last_cps = [send(own4, last, last_send.at[n], last_recv, dev) for n, dev in enumerate((partner, xnb, ynb))]
    for cp in last_cps:
        on(is_last, cp, 'start')
    early[3].wait()
    for cp in ff4 + next_qkv:
        cp.wait()

    def hops(t):
        def hop(k, slot, rk, dev):
            return send(kv5.at[rows_of(t)], buf.at[slot, rows_of(t)], hop_send.at[k, t], hop_recv.at[rk, t], dev)
        return [(core == 0, hop(0, 0, 0, partner)),
                (chip == 0, hop(1, 1, 1, xnb)),
                (chip == 0, hop(2, 1, 1, ynb)),
                (chip == 1, hop(2, 1, 1, ynb)),
                (chip == 2, hop(1, 3, 2, xnb))]

    def early_pass(t):
        return send(buf.at[1, rows_of(t)], buf.at[3, rows_of(t)], hop_send.at[3, t], hop_recv.at[2, t], xnb)

    def first_in(t):
        send(kv5.at[rows_of(t)], buf.at[1, rows_of(t)], hop_send.at[0, t], hop_recv.at[1, t], partner).wait_recv()

    far = chip == 3

    n_key = WINDOW + TILE

    def layer_tile(it, carry):
        t = N_TILE - 1 - it
        rows = rows_of(t)
        cos, sin = cos_sin(hi4_ref, lo4_ref, me * TOK + t * TILE, TILE)
        a = rms(x[rows, :].astype(F32), 1.0 + ng_ref[0, 0:1, :]).astype(BF16)
        qs = [head_rope(dot(a, wq[0, h]), g4q, cos, sin) for h in range(4)]

        on(me > 0, halo_copy(t), 'wait_recv')
        start = pl.multiple_of(t * TILE, TILE)
        ks = win[pl.ds(start, n_key), 0:HEAD]
        vs = win[pl.ds(start, n_key), HEAD:2 * HEAD]
        col = lax.broadcasted_iota(jnp.int32, (1, n_key), 1)
        hidden = jnp.logical_and(me == 0, col + start < WINDOW)
        bias = jnp.where(hidden, NEG, -sigma if fast else 0.0)
        r = lax.broadcasted_iota(jnp.int32, (TILE, TILE), 0)
        c = lax.broadcasted_iota(jnp.int32, (TILE, TILE), 1)
        outs = []
        for h in range(4):
            s = dot_t(qs[h], ks) * COEF + bias
            s = jnp.concatenate([jnp.where(c > r, s[:, 0:TILE], NEG), s[:, TILE:WINDOW], jnp.where(c <= r, s[:, WINDOW:], NEG)], axis=1)
            if not fast:
                s = s - jnp.max(s, axis=1, keepdims=True)
            p = jnp.exp2(s)
            total = jnp.sum(p, axis=1, keepdims=True)
            outs.append((dot(p.astype(BF16), vs) / total).astype(BF16))
        h_mid = finish_rows(x[rows, :], jnp.concatenate(outs, axis=1), ng_ref[0], wo, wg, wu, wd)
        mid[rows, :] = h_mid
        cos, sin = cos_sin(hi5_ref, lo5_ref, me * TOK + t * TILE, TILE)
        a = rms(h_mid.astype(F32), 1.0 + ng_ref[1, 0:1, :]).astype(BF16)
        kv5[rows, 0:HEAD] = head_rope(dot(a, wk[1]), g5k, cos, sin)
        kv5[rows, HEAD:2 * HEAD] = dot(a, wv[1]).astype(BF16)
        for h in range(4):
            q[h, rows, :] = head_rope(dot(a, wq[1, h]), g5q, cos, sin)
        for cond, cp in hops(t):
            on(cond, cp, 'start')

        @pl.when(jnp.logical_and(far, it >= 1))
        def _():
            first_in(t + 1)
            early_pass(t + 1).start()
        return carry

    lax.fori_loop(0, N_TILE, layer_tile, 0)
    outs5 = [pltpu.make_async_copy(kv5.at[:, pl.ds(0, HEAD)], k_hbm, out_sem.at[0]), pltpu.make_async_copy(kv5.at[:, pl.ds(HEAD, HEAD)], v_hbm, out_sem.at[1])]
    for cp in outs5 + ff5:
        cp.start()

    def attend(ks, vs, rows, width, masked, first):
        n = rows.size
        if masked:
            r = lax.broadcasted_iota(jnp.int32, (n, n), 0)
            vis = lax.broadcasted_iota(jnp.int32, (n, n), 1) <= r
        for h in range(4):
            s = dot_t(q[h, rows, :], ks)
            t = s * COEF - sigma if fast else s * COEF
            if masked:
                tail = jnp.where(vis, t[:, width - n:], NEG)
                t = tail if width == n else jnp.concatenate([t[:, 0:width - n], tail], axis=1)
            if not fast:
                mx = jnp.broadcast_to(jnp.max(t, axis=1, keepdims=True), (n, 128))
                fresh = mx if first else jnp.maximum(m[h, rows, :], mx)
                if not first:
                    decay = jnp.exp2(m[h, rows, :] - fresh)
                    l[h, rows, :] = l[h, rows, :] * decay
                    acc[h, rows, :] = acc[h, rows, :] * decay[:, 0:1]
                m[h, rows, :] = fresh
                t = t - fresh[:, 0:1]
            p = jnp.exp2(t)
            lp = p[:, 0:128]
            for j in range(1, width // 128):
                lp = lp + p[:, j * 128:(j + 1) * 128]
            o = dot(p.astype(BF16), vs)
            if first:
                l[h, rows, :] = lp
                acc[h, rows, :] = o
            else:
                l[h, rows, :] += lp
                acc[h, rows, :] += o

    for i in range(N_TILE):
        width = (i + 1) * TILE
        attend(kv5[0:width, 0:HEAD], kv5[0:width, HEAD:2 * HEAD], pl.ds(i * TILE, TILE), width, True, True)

    def slot(s):
        ks = buf[s, :, 0:HEAD]
        vs = buf[s, :, HEAD:2 * HEAD]

        def q_rows(i, carry):
            attend(ks, vs, rows_of(i, QROWS), TOK, False, False)
            return carry

        lax.fori_loop(0, TOK // QROWS, q_rows, 0)

    def wide(s, dst, ssem, dev):
        return send(buf.at[s], buf.at[dst], ssem, wide_recv.at[dst], dev)

    def relay(s):
        odd = s % 2 == 1
        return [(odd, wide(s, jnp.minimum(s + 1, N_SLOT - 1), pass_send.at[s], partner)),
                (jnp.logical_and(jnp.logical_and(chip == 1, core == 0), s == 1), wide(s, 5, over_send, ynb)),
                (jnp.logical_and(jnp.logical_and(chip == 2, core == 1), s == 1), wide(s, 5, over_send, xnb))]

    def chunks_in(cond, slot_no, rk, n=N_TILE):
        @pl.when(cond)
        def _():
            def one(t, carry):
                send(kv5.at[rows_of(t)], buf.at[slot_no, rows_of(t)], hop_send.at[0, t], hop_recv.at[rk, t], partner).wait_recv()
                return carry
            lax.fori_loop(0, n, one, 0)

    gives = jnp.logical_or(me == 3, jnp.logical_or(me == 5, me == 1))
    spread = [(gives, send(last, last, last_send.at[0], last_recv, partner)), (me == 3, send(last, last, last_send.at[1], last_recv, xnb))]

    def pass_last(cond):
        @pl.when(cond)
        def _():
            send(last, last, last_send.at[2], last_recv, partner).wait_recv()
            for c, cp in spread:
                on(c, cp, 'start')

    pass_last(jnp.logical_and(gives, me > 1))

    def step(s, carry):
        chunks_in(jnp.logical_and(s == 0, core == 1), 0, 0)
        chunks_in(jnp.logical_and(s == 1, chip < 3), 1, 1)
        chunks_in(s == 3, 3, 2)

        @pl.when(jnp.logical_and(far, jnp.where(core == 1, s == 0, s == 1)))
        def _():
            first_in(0)
            early_pass(0).start()

        @pl.when(jnp.logical_or(jnp.logical_and(s > 0, s % 2 == 0), s == 5))
        def _():
            wide(s, s, pass_send.at[s], partner).wait_recv()

        for cond, cp in relay(s):
            on(cond, cp, 'start')

        @pl.when(jnp.logical_or(s >= 1, core == 1))
        def _():
            slot(s)

        return carry

    lax.fori_loop(0, 2 * chip + 1, step, 0)
    pass_last(me == 1)

    @pl.when(jnp.logical_and(jnp.logical_not(gives), jnp.logical_not(is_last)))
    def _():
        send(last, last, last_send.at[2], last_recv, partner).wait_recv()

    def put_last(src):
        return [pltpu.make_async_copy(src.at[:, pl.ds(0, HEAD)], kl_hbm, out_sem.at[2]), pltpu.make_async_copy(src.at[:, pl.ds(HEAD, HEAD)], vl_hbm, out_sem.at[3])]

    for cp in put_last(own4):
        on(is_last, cp, 'start')
    for cp in put_last(last):
        on(jnp.logical_not(is_last), cp, 'start')

    for cp in ff5:
        cp.wait()

    def out_copy(t):
        return pltpu.make_async_copy(xo.at[rows_of(t, FROWS)], out_hbm.at[rows_of(t, FROWS)], out_sem.at[4 + t])

    def finish_tile(t, carry):
        rows = rows_of(t, FROWS)
        attn = []
        for h in range(4):
            total = jnp.sum(l[h, rows, :], axis=1, keepdims=True)
            attn.append((acc[h, rows, :] / total).astype(BF16))
        xo[rows, :] = finish_rows(mid[rows, :], jnp.concatenate(attn, axis=1), ng_ref[1], wo, wg, wu, wd)
        out_copy(t).start()
        return carry

    lax.fori_loop(0, TOK // FROWS, finish_tile, 0)

    def drain_tile(t, carry):
        on(me < top, halo_copy(t), 'wait_send')
        on(far, early_pass(t), 'wait_send')
        for cond, cp in hops(t):
            on(cond, cp, 'wait_send')
        return carry

    lax.fori_loop(0, N_TILE, drain_tile, 0)

    def drain_step(s, carry):
        for cond, cp in relay(s):
            on(cond, cp, 'wait_send')
        return carry

    lax.fori_loop(1, 2 * chip + 1, drain_step, 0)
    for cp in last_cps:
        on(is_last, cp, 'wait_send')
    for cond, cp in spread:
        on(cond, cp, 'wait_send')
    for cp in outs5 + put_last(last):
        cp.wait()
    for t in range(TOK // FROWS):
        out_copy(t).wait()


def layers(fast, ng, qg, rope, x, wq, wk, wv, wo, wg, wu, wd):
    vm = pl.BlockSpec(memory_space=pltpu.VMEM)
    anyw = pl.BlockSpec(memory_space=pl.ANY)
    dma = pltpu.SemaphoreType.DMA
    kshape = jax.ShapeDtypeStruct((TOK, HEAD), BF16)
    return pl.pallas_call(
        functools.partial(layers_kernel, fast),
        in_specs=[vm] * 6 + [anyw] * 8,
        out_specs=[anyw] * 5 + [pl.BlockSpec(memory_space=pltpu.SMEM)],
        out_shape=[jax.ShapeDtypeStruct((TOK, D), BF16), kshape, kshape, kshape, kshape, jax.ShapeDtypeStruct((1,), F32)],
        scratch_shapes=[
            pltpu.VMEM((TOK, D), BF16), pltpu.VMEM((TOK, D), BF16), pltpu.VMEM((WINDOW + TOK, 2 * HEAD), BF16), pltpu.VMEM((TOK, 2 * HEAD), BF16),
            pltpu.VMEM((4, TOK, HEAD), BF16), pltpu.VMEM((N_SLOT, TOK, 2 * HEAD), BF16), pltpu.VMEM((4, TOK, HEAD), F32), pltpu.VMEM((4, TOK, 128), F32),
            pltpu.VMEM((8, 128) if fast else (4, TOK, 128), F32), pltpu.VMEM((TOK, 2 * HEAD), BF16), pltpu.VMEM((TOK, D), BF16),
            pltpu.VMEM((2, 4, D, HEAD), BF16), pltpu.VMEM((2, D, HEAD), BF16), pltpu.VMEM((2, D, HEAD), BF16),
            pltpu.VMEM((4 * HEAD, D), BF16), pltpu.VMEM((D, FF), BF16), pltpu.VMEM((D, FF), BF16), pltpu.VMEM((FF, D), BF16),
            dma((11,)), dma((4 + TOK // FROWS,)), dma((N_TILE,)), dma((N_TILE,)), dma((4, N_TILE)), dma((3, N_TILE)), dma((N_SLOT,)), dma, dma((N_SLOT,)),
            dma((3,)), dma],
        name="layers_fast" if fast else "layers_safe",
        compiler_params=pltpu.CompilerParams(vmem_limit_bytes=VLIM, collective_id=0 if fast else None, has_side_effects=True),
        cost_estimate=pl.CostEstimate(flops=60 * 10**9, bytes_accessed=30 << 20, transcendentals=0),
    )(ng, qg, *rope[0], *rope[1], x, wq, wk, wv, wo, wg, wu, wd)


def emit_kernel(*refs):
    ins, outs, mids, sem_in, sem_out = refs[0:5], refs[5:10], refs[10:15], refs[15], refs[16]
    loads = [pltpu.make_async_copy(i, m, sem_in.at[n]) for n, (i, m) in enumerate(zip(ins, mids))]
    stores = [pltpu.make_async_copy(m, o, sem_out.at[n]) for n, (m, o) in enumerate(zip(mids, outs))]
    for cp in loads:
        cp.start()
    for ld, st in zip(loads, stores):
        ld.wait()
        st.start()
    for st in stores:
        st.wait()


def emit(arrays):
    anyw = pl.BlockSpec(memory_space=pl.ANY)
    return pl.pallas_call(
        emit_kernel,
        in_specs=[anyw] * 5,
        out_specs=[anyw] * 5,
        out_shape=[jax.ShapeDtypeStruct(a.shape, a.dtype) for a in arrays],
        scratch_shapes=[pltpu.VMEM(a.shape, a.dtype) for a in arrays] + [pltpu.SemaphoreType.DMA((5,)), pltpu.SemaphoreType.DMA((5,))],
        name="emit",
    )(*arrays)


def solution(mesh):
    n_dev = mesh.shape['cp']
    rope = [rope_const(layer, TOK * n_dev) for layer in range(2)]

    def shard_body(x, ng, qg, w_q, w_k, w_v, w_o, w_gate, w_up, w_down):
        wq = w_q.transpose(0, 2, 1, 3)
        wk = w_k.reshape(2, D, HEAD)
        wv = w_v.reshape(2, D, HEAD)
        wo = w_o.reshape(2, 4 * HEAD, D)

        def run(fast):
            return tuple(layers(fast, ng, qg, rope, x, wq, wk, wv, wo, w_gate, w_up, w_down))

        *first, bound = run(True)
        _, rest = lax.while_loop(lambda c: c[0], lambda c: (jnp.zeros((), jnp.bool_), run(False)[:5]), (bound[0] > LIMIT, tuple(first)))
        out, k5, v5, kl, vl = emit(rest)
        return out, k5[:, None, :], v5[:, None, :], kl[:, None, :], vl[:, None, :]

    return jax.shard_map(shard_body, mesh=mesh, in_specs=(P('cp'), P(), P(), P(), P(), P(), P(), P(), P(), P()),
                         out_specs=(P('cp'), P('cp'), P('cp'), P(), P()), check_vma=False)
```

```python
import functools

import numpy as np
import jax
import jax.numpy as jnp
from jax import lax
from jax.experimental import pallas as pl
from jax.experimental.pallas import tpu as pltpu
from jax.sharding import PartitionSpec as P

WINDOW = 1024
EPS = 1e-6
BASES = (10000.0, 1000000.0)
SCALES = (1.0, 8.0)
HEAD = 256
TOK = 1024
D = 640
FF = 2048
TILE = 256
LO = 32
LOG2E = 1.4426950408889634
COEF = LOG2E / 16.0
TOP = 36.0
LIMIT = 56.0
NEG = -1e30
F32 = jnp.float32
BF16 = jnp.bfloat16
VLIM = 58 << 20


def rope_const(layer, seq_len):
    base, scale = BASES[layer], SCALES[layer]
    freq = base ** (-np.arange(HEAD // 2, dtype=np.float64) * 2.0 / HEAD)
    hi = (np.arange(seq_len // LO) * LO / scale)[:, None] * freq[None, :]
    lo = (np.arange(LO) / scale)[:, None] * freq[None, :]
    hi_tab = np.concatenate([np.cos(hi), np.sin(hi)], axis=1).astype(np.float32)
    lo_tab = np.concatenate([np.cos(lo), np.sin(lo)], axis=1).astype(np.float32)
    return hi_tab, lo_tab


def rms(x, gain):
    return x * lax.rsqrt(jnp.mean(x * x, axis=-1, keepdims=True) + EPS) * gain


def cos_sin(hi_ref, lo_ref, row0, rows):
    n_hi = rows // LO
    hi = hi_ref[pl.ds(pl.multiple_of(row0 // LO, 8), n_hi), :]
    lo = lo_ref[...]
    ch, sh = hi[:, None, 0:128], hi[:, None, 128:256]
    cl, sl = lo[None, :, 0:128], lo[None, :, 128:256]
    cos = (ch * cl - sh * sl).reshape(rows, 128)
    sin = (sh * cl + ch * sl).reshape(rows, 128)
    return cos, sin


def rotate(x, cos, sin):
    a, b = x[:, 0:128], x[:, 128:256]
    return jnp.concatenate([a * cos - b * sin, b * cos + a * sin], axis=1).astype(BF16)


def head_rope(proj, gain, cos, sin):
    return rotate(rms(proj.astype(BF16).astype(F32), gain), cos, sin)


def dot(a, b):
    return jnp.dot(a, b, preferred_element_type=F32)


def dot_t(a, b):
    return lax.dot_general(a, b, (((1,), (1,)), ((), ())), preferred_element_type=F32)


MESH = pl.DeviceIdType.MESH
N_SLOT = 8
OWN = 7
LENT = 256
N_TILE = TOK // TILE
QROWS = 512
FROWS = 512
FSTEP = 2048


def finish_rows(x, attn, ng, wo, wg, wu, wd):
    o = dot(attn, wo[...]).astype(BF16).astype(F32)
    h1 = (x.astype(F32) + rms(o, 1.0 + ng[1:2, :])).astype(BF16)
    b = rms(h1.astype(F32), 1.0 + ng[2:3, :]).astype(BF16)
    acc = None
    for f in range(0, FF, FSTEP):
        g = dot(b, wg[:, f:f + FSTEP])
        u = dot(b, wu[:, f:f + FSTEP])
        m = (jax.nn.gelu(g, approximate=True) * u).astype(BF16)
        part = dot(m, wd[f:f + FSTEP, :])
        acc = part if acc is None else acc + part
    o2 = acc.astype(BF16).astype(F32)
    return (h1.astype(F32) + rms(o2, 1.0 + ng[3:4, :])).astype(BF16)


def layers_kernel(fast, ng_ref, qg_ref, hi4_ref, lo4_ref, hi5_ref, lo5_ref, x_hbm, wq_hbm, wk_hbm, wv_hbm, wo_hbm, wg_hbm, wu_hbm, wd_hbm,
                  out_hbm, k_hbm, v_hbm, kl_hbm, vl_hbm, bound_ref,
                  x, mid, win, q, buf, acc, l, m, lent, last, xo, wq, wk, wv, wo, wg, wu, wd,
                  load_sem, out_sem, halo_send, halo_recv, hop_send, hop_recv, pass_send, over_send, wide_recv, last_send, last_recv, lend_sem):
    me = lax.axis_index('cp')
    core = me % 2
    chip = me // 2
    partner = me + 1 - 2 * core
    xnb = me + 2 - 4 * (chip % 2)
    ynb = me + 4 - 8 * (chip // 2)
    top = 7
    is_last = me == top
    kv5 = buf.at[OWN]
    near, helper, far = chip == 0, chip == 1, chip == 3
    borrowed = pl.ds(TOK, LENT)

    def load(src, dst, n):
        return pltpu.make_async_copy(src, dst, load_sem.at[n])

    early = [load(x_hbm, x, 0), load(wk_hbm.at[0], wk.at[0], 1), load(wv_hbm.at[0], wv.at[0], 2), load(wq_hbm.at[0], wq.at[0], 3)]
    ff4 = [load(wo_hbm.at[0], wo, 4), load(wg_hbm.at[0], wg, 5), load(wu_hbm.at[0], wu, 6), load(wd_hbm.at[0], wd, 7)]
    next_qkv = [load(wk_hbm.at[1], wk.at[1], 8), load(wv_hbm.at[1], wv.at[1], 9), load(wq_hbm.at[1], wq.at[1], 10)]
    ff5 = [load(wo_hbm.at[1], wo, 4), load(wg_hbm.at[1], wg, 5), load(wu_hbm.at[1], wu, 6), load(wd_hbm.at[1], wd, 7)]
    for cp in early:
        cp.start()

    if fast:
        barrier = pltpu.get_barrier_semaphore()
        for other in (partner, xnb, ynb, (me + 1) % 8, (me + 7) % 8):
            pl.semaphore_signal(barrier, inc=1, device_id=(other,), device_id_type=MESH)
    for cp in ff4 + next_qkv:
        cp.start()

    @pl.when(me == 0)
    def _():
        win[0:WINDOW, :] = jnp.zeros((WINDOW, 2 * HEAD), BF16)

    if fast:
        pl.semaphore_wait(barrier, 5)

    def send(src, dst, ssem, rsem, dev):
        return pltpu.make_async_remote_copy(src_ref=src, dst_ref=dst, send_sem=ssem, recv_sem=rsem, device_id=(dev,), device_id_type=MESH)

    def on(cond, copy, act):
        @pl.when(cond)
        def _():
            getattr(copy, act)()

    def rows_of(t, n=TILE):
        return pl.ds(pl.multiple_of(t * n, n), n)

    def halo_copy(t):
        return send(win.at[rows_of(t + N_TILE)], win.at[rows_of(t)], halo_send.at[t], halo_recv.at[t], (me + 1) % 8)

    gains = jnp.abs(1.0 + qg_ref[...])
    pair = jnp.maximum(gains[:, :, 0:HEAD // 2], gains[:, :, HEAD // 2:])
    bound = 16.0 * 1.02 * jnp.max(pair[:, 0:1] * pair[:, 1:2])
    bound_ref[0] = bound
    sigma = jnp.maximum(bound - TOP, 0.0) * LOG2E
    g4q, g4k = 1.0 + qg_ref[0, 0:1, :], 1.0 + qg_ref[0, 1:2, :]
    g5q, g5k = 1.0 + qg_ref[1, 0:1, :], 1.0 + qg_ref[1, 1:2, :]
    for cp in early[:3]:
        cp.wait()

    def kv_tile(it, carry):
        t = N_TILE - 1 - it
        cos, sin = cos_sin(hi4_ref, lo4_ref, me * TOK + t * TILE, TILE)
        a = rms(x[rows_of(t), :].astype(F32), 1.0 + ng_ref[0, 0:1, :]).astype(BF16)
        win[rows_of(t + N_TILE), 0:HEAD] = head_rope(dot(a, wk[0]), g4k, cos, sin)
        win[rows_of(t + N_TILE), HEAD:2 * HEAD] = dot(a, wv[0]).astype(BF16)
        on(me < top, halo_copy(t), 'start')
        return carry

    lax.fori_loop(0, N_TILE, kv_tile, 0)
    own4 = win.at[pl.ds(WINDOW, TOK)]
    last_cps = [send(own4, last, last_send.at[n], last_recv, dev) for n, dev in enumerate((partner, xnb, ynb))]
    for cp in last_cps:
        on(is_last, cp, 'start')
    early[3].wait()
    for cp in ff4 + next_qkv:
        cp.wait()

    def hops(t):
        def hop(k, slot, rk, dev):
            return send(kv5.at[rows_of(t)], buf.at[slot, rows_of(t)], hop_send.at[k, t], hop_recv.at[rk, t], dev)
        return [(jnp.logical_or(core == 0, helper), hop(0, 0, 0, partner)),
                (chip == 0, hop(1, 1, 1, xnb)),
                (chip == 0, hop(2, 1, 1, ynb)),
                (chip == 1, hop(2, 1, 1, ynb)),
                (chip == 2, hop(1, 3, 2, xnb)),
                (me == 5, hop(2, 3, 2, ynb)),
                (me == 6, hop(2, 5, 3, ynb)),
                (jnp.logical_and(me == 7, t == 0), hop(2, 6, 3, ynb))]

    def early_pass(t):
        return send(buf.at[1, rows_of(t)], buf.at[3, rows_of(t)], hop_send.at[3, t], hop_recv.at[2, t], xnb)

    def first_in(t):
        send(kv5.at[rows_of(t)], buf.at[1, rows_of(t)], hop_send.at[0, t], hop_recv.at[1, t], partner).wait_recv()

    def third_in(t):
        send(kv5.at[rows_of(t)], buf.at[3, rows_of(t)], hop_send.at[0, t], hop_recv.at[2, t], partner).wait_recv()

    def over_pass(k, t, dev):
        return send(buf.at[3, rows_of(t)], buf.at[3, rows_of(t)], hop_send.at[k, t], hop_recv.at[2, t], dev)

    lend = send(q.at[:, pl.ds(0, LENT), :], q.at[:, borrowed, :], lend_sem.at[0], lend_sem.at[1], ynb)
    give_back = send(lent, lent, lend_sem.at[2], lend_sem.at[3], ynb)

    n_key = WINDOW + TILE

    def nth(it):
        return jnp.where(it < 2, N_TILE - 1 - it, it - 2)

    def layer_tile(it, carry):
        t = nth(it)
        before = nth(jnp.maximum(it - 1, 0))
        rows = rows_of(t)
        cos, sin = cos_sin(hi4_ref, lo4_ref, me * TOK + t * TILE, TILE)
        a = rms(x[rows, :].astype(F32), 1.0 + ng_ref[0, 0:1, :]).astype(BF16)
        qs = [head_rope(dot(a, wq[0, h]), g4q, cos, sin) for h in range(4)]

        on(jnp.logical_and(me > 0, it < 2), halo_copy(t), 'wait_recv')
        for n in (1, 0):
            on(jnp.logical_and(me > 0, it == 2), halo_copy(n), 'wait_recv')
        start = pl.multiple_of(t * TILE, TILE)
        ks = win[pl.ds(start, n_key), 0:HEAD]
        vs = win[pl.ds(start, n_key), HEAD:2 * HEAD]
        col = lax.broadcasted_iota(jnp.int32, (1, n_key), 1)
        hidden = jnp.logical_and(me == 0, col + start < WINDOW)
        bias = jnp.where(hidden, NEG, -sigma if fast else 0.0)
        r = lax.broadcasted_iota(jnp.int32, (TILE, TILE), 0)
        c = lax.broadcasted_iota(jnp.int32, (TILE, TILE), 1)
        outs = []
        for h in range(4):
            s = dot_t(qs[h], ks) * COEF + bias
            s = jnp.concatenate([jnp.where(c > r, s[:, 0:TILE], NEG), s[:, TILE:WINDOW], jnp.where(c <= r, s[:, WINDOW:], NEG)], axis=1)
            if not fast:
                s = s - jnp.max(s, axis=1, keepdims=True)
            p = jnp.exp2(s)
            total = jnp.sum(p, axis=1, keepdims=True)
            outs.append((dot(p.astype(BF16), vs) / total).astype(BF16))
        h_mid = finish_rows(x[rows, :], jnp.concatenate(outs, axis=1), ng_ref[0], wo, wg, wu, wd)
        mid[rows, :] = h_mid
        cos, sin = cos_sin(hi5_ref, lo5_ref, me * TOK + t * TILE, TILE)
        a = rms(h_mid.astype(F32), 1.0 + ng_ref[1, 0:1, :]).astype(BF16)
        kv5[rows, 0:HEAD] = head_rope(dot(a, wk[1]), g5k, cos, sin)
        kv5[rows, HEAD:2 * HEAD] = dot(a, wv[1]).astype(BF16)
        for h in range(4):
            q[h, rows, :] = head_rope(dot(a, wq[1, h]), g5q, cos, sin)
        for cond, cp in hops(t):
            on(cond, cp, 'start')
        on(jnp.logical_and(far, it == 2), lend, 'start')

        @pl.when(jnp.logical_and(far, it >= 1))
        def _():
            first_in(before)
            early_pass(before).start()

        @pl.when(jnp.logical_and(me == 6, it >= 1))
        def _():
            third_in(before)
            over_pass(1, before, ynb).start()
        return carry

    lax.fori_loop(0, N_TILE, layer_tile, 0)
    outs5 = [pltpu.make_async_copy(kv5.at[:, pl.ds(0, HEAD)], k_hbm, out_sem.at[0]), pltpu.make_async_copy(kv5.at[:, pl.ds(HEAD, HEAD)], v_hbm, out_sem.at[1])]
    for cp in outs5 + ff5:
        cp.start()

    def attend(ks, vs, rows, width, masked, first):
        n = rows.size
        if masked:
            r = lax.broadcasted_iota(jnp.int32, (n, n), 0)
            vis = lax.broadcasted_iota(jnp.int32, (n, n), 1) <= r
        for h in range(4):
            s = dot_t(q[h, rows, :], ks)
            t = s * COEF - sigma if fast else s * COEF
            if masked:
                tail = jnp.where(vis, t[:, width - n:], NEG)
                t = tail if width == n else jnp.concatenate([t[:, 0:width - n], tail], axis=1)
            if not fast:
                mx = jnp.broadcast_to(jnp.max(t, axis=1, keepdims=True), (n, 128))
                fresh = mx if first else jnp.maximum(m[h, rows, :], mx)
                if not first:
                    decay = jnp.exp2(m[h, rows, :] - fresh)
                    l[h, rows, :] = l[h, rows, :] * decay
                    acc[h, rows, :] = acc[h, rows, :] * decay[:, 0:1]
                m[h, rows, :] = fresh
                t = t - fresh[:, 0:1]
            p = jnp.exp2(t)
            lp = p[:, 0:128]
            for j in range(1, width // 128):
                lp = lp + p[:, j * 128:(j + 1) * 128]
            o = dot(p.astype(BF16), vs)
            if first:
                l[h, rows, :] = lp
                acc[h, rows, :] = o
            else:
                l[h, rows, :] += lp
                acc[h, rows, :] += o

    for i in range(N_TILE):
        width = (i + 1) * TILE

        @pl.when(jnp.logical_or(i > 0, jnp.logical_not(far)))
        def _(i=i, width=width):
            attend(kv5[0:width, 0:HEAD], kv5[0:width, HEAD:2 * HEAD], pl.ds(i * TILE, TILE), width, True, True)

    def slot(s):
        ks = buf[s, :, 0:HEAD]
        vs = buf[s, :, HEAD:2 * HEAD]

        def q_rows(n, base):
            def one(i, carry):
                attend(ks, vs, pl.ds(pl.multiple_of(base + i * n, 128), n), TOK, False, False)
                return carry
            lax.fori_loop(0, (TOK - base) // n, one, 0)

        @pl.when(far)
        def _():
            q_rows((TOK - LENT) // 2, LENT)

        @pl.when(jnp.logical_not(far))
        def _():
            q_rows(QROWS, 0)

    def wide(s, dst, ssem, dev):
        return send(buf.at[s], buf.at[dst], ssem, wide_recv.at[dst], dev)

    def relay(s):
        odd = s % 2 == 1
        return [(odd, wide(s, jnp.minimum(s + 1, N_SLOT - 1), pass_send.at[s], partner)),
                (jnp.logical_and(jnp.logical_and(chip == 1, core == 0), s == 1), wide(s, 5, over_send, ynb)),
                (jnp.logical_and(jnp.logical_and(chip == 2, core == 1), s == 1), wide(s, 5, over_send, xnb))]

    def chunks_in(cond, slot_no, rk, n=N_TILE):
        @pl.when(cond)
        def _():
            def one(t, carry):
                send(kv5.at[rows_of(t)], buf.at[slot_no, rows_of(t)], hop_send.at[0, t], hop_recv.at[rk, t], partner).wait_recv()
                return carry
            lax.fori_loop(0, n, one, 0)

    gives = jnp.logical_or(me == 3, jnp.logical_or(me == 5, me == 1))
    spread = [(gives, send(last, last, last_send.at[0], last_recv, partner)), (me == 3, send(last, last, last_send.at[1], last_recv, xnb))]

    def pass_last(cond):
        @pl.when(cond)
        def _():
            send(last, last, last_send.at[2], last_recv, partner).wait_recv()
            for c, cp in spread:
                on(c, cp, 'start')

    pass_last(jnp.logical_and(gives, me > 1))

    def step(s, carry):
        chunks_in(jnp.logical_and(s == 0, core == 1), 0, 0)
        chunks_in(jnp.logical_and(s == 1, chip < 3), 1, 1)
        chunks_in(jnp.logical_and(s == 3, me != 6), 3, 2)

        @pl.when(jnp.logical_and(far, jnp.where(core == 1, s == 0, s == 1)))
        def _():
            first_in(1)
            early_pass(1).start()

        @pl.when(jnp.logical_and(me == 6, s == 1))
        def _():
            third_in(1)
            over_pass(1, 1, ynb).start()

        @pl.when(jnp.logical_or(jnp.logical_and(s > 0, s % 2 == 0), s == 5))
        def _():
            wide(s, s, pass_send.at[s], partner).wait_recv()

        for cond, cp in relay(s):
            on(cond, cp, 'start')

        @pl.when(jnp.logical_or(s >= 1, core == 1))
        def _():
            slot(s)

        return carry

    @pl.when(me == 1)
    def _():
        def one(it, carry):
            t = nth(it)
            third_in(t)
            over_pass(3, t, xnb).start()
            return carry
        lax.fori_loop(0, N_TILE, one, 0)

    lax.fori_loop(0, 2 * chip + 1, step, 0)
    pass_last(me == 1)

    pass_six = send(buf.at[5], buf.at[5], pass_send.at[5], wide_recv.at[5], partner)
    pass_three = send(buf.at[3], buf.at[4], pass_send.at[3], wide_recv.at[4], partner)
    gets_six = jnp.logical_and(helper, core == 0)

    @pl.when(helper)
    def _():
        chunks_in(core == 0, 5, 3)
        chunks_in(core == 1, 6, 3, 1)
        on(core == 0, pass_six, 'start')
        chunks_in(core == 1, 3, 2)
        on(core == 1, pass_three, 'start')
        lend.wait_recv()
        attend(buf[5 + core, 0:LENT, 0:HEAD], buf[5 + core, 0:LENT, HEAD:2 * HEAD], borrowed, LENT, True, True)

        def block(k, carry):
            s = jnp.where(k == 0, OWN, jnp.where(k <= 4, k - 1, jnp.where(k == 5, 5, 4)))
            chunks_in(jnp.logical_and(k == 1, core == 0), 0, 0)
            chunks_in(jnp.logical_and(k == 4, core == 0), 3, 2)
            on(jnp.logical_and(k == 4, core == 0), pass_three, 'start')
            on(jnp.logical_and(k == 5, core == 1), pass_six, 'wait_recv')
            on(k == 6, pass_three, 'wait_recv')

            @pl.when(jnp.logical_or(k != 5, core == 1))
            def _():
                attend(buf[s, :, 0:HEAD], buf[s, :, HEAD:2 * HEAD], borrowed, TOK, False, False)
            return carry

        lax.fori_loop(0, 7, block, 0)
        for h in range(4):
            total = jnp.sum(l[h, borrowed, :], axis=1, keepdims=True)
            lent[h] = (acc[h, borrowed, :] / total).astype(BF16)
        give_back.start()

    @pl.when(jnp.logical_and(jnp.logical_not(gives), jnp.logical_not(is_last)))
    def _():
        send(last, last, last_send.at[2], last_recv, partner).wait_recv()

    def put_last(src):
        return [pltpu.make_async_copy(src.at[:, pl.ds(0, HEAD)], kl_hbm, out_sem.at[2]), pltpu.make_async_copy(src.at[:, pl.ds(HEAD, HEAD)], vl_hbm, out_sem.at[3])]

    for cp in put_last(own4):
        on(is_last, cp, 'start')
    for cp in put_last(last):
        on(jnp.logical_not(is_last), cp, 'start')

    for cp in ff5:
        cp.wait()

    def out_copy(t):
        return pltpu.make_async_copy(xo.at[rows_of(t, FROWS)], out_hbm.at[rows_of(t, FROWS)], out_sem.at[4 + t])

    def finish_tile(it, carry):
        t = (it + 1) % (TOK // FROWS)

        @pl.when(jnp.logical_and(far, t == 0))
        def _():
            give_back.wait_recv()
            for h in range(4):
                acc[h, 0:LENT, :] = lent[h].astype(F32)
                l[h, 0:LENT, :] = jnp.full((LENT, 128), 1.0 / 128.0, F32)

        rows = rows_of(t, FROWS)
        attn = []
        for h in range(4):
            total = jnp.sum(l[h, rows, :], axis=1, keepdims=True)
            attn.append((acc[h, rows, :] / total).astype(BF16))
        xo[rows, :] = finish_rows(mid[rows, :], jnp.concatenate(attn, axis=1), ng_ref[1], wo, wg, wu, wd)
        out_copy(t).start()
        return carry

    lax.fori_loop(0, TOK // FROWS, finish_tile, 0)

    def drain_tile(t, carry):
        on(me < top, halo_copy(t), 'wait_send')
        on(far, early_pass(t), 'wait_send')
        on(me == 1, over_pass(3, t, xnb), 'wait_send')
        on(me == 6, over_pass(1, t, ynb), 'wait_send')
        for cond, cp in hops(t):
            on(cond, cp, 'wait_send')
        return carry

    lax.fori_loop(0, N_TILE, drain_tile, 0)

    def drain_step(s, carry):
        for cond, cp in relay(s):
            on(cond, cp, 'wait_send')
        return carry

    lax.fori_loop(1, 2 * chip + 1, drain_step, 0)
    for cp in last_cps:
        on(is_last, cp, 'wait_send')
    on(far, lend, 'wait_send')
    on(helper, give_back, 'wait_send')
    on(helper, pass_three, 'wait_send')
    on(gets_six, pass_six, 'wait_send')
    for cond, cp in spread:
        on(cond, cp, 'wait_send')
    for cp in outs5 + put_last(last):
        cp.wait()
    for t in range(TOK // FROWS):
        out_copy(t).wait()


def layers(fast, ng, qg, rope, x, wq, wk, wv, wo, wg, wu, wd):
    vm = pl.BlockSpec(memory_space=pltpu.VMEM)
    anyw = pl.BlockSpec(memory_space=pl.ANY)
    dma = pltpu.SemaphoreType.DMA
    kshape = jax.ShapeDtypeStruct((TOK, HEAD), BF16)
    return pl.pallas_call(
        functools.partial(layers_kernel, fast),
        in_specs=[vm] * 6 + [anyw] * 8,
        out_specs=[anyw] * 5 + [pl.BlockSpec(memory_space=pltpu.SMEM)],
        out_shape=[jax.ShapeDtypeStruct((TOK, D), BF16), kshape, kshape, kshape, kshape, jax.ShapeDtypeStruct((1,), F32)],
        scratch_shapes=[
            pltpu.VMEM((TOK, D), BF16), pltpu.VMEM((TOK, D), BF16), pltpu.VMEM((WINDOW + TOK, 2 * HEAD), BF16),
            pltpu.VMEM((4, TOK + LENT, HEAD), BF16), pltpu.VMEM((N_SLOT, TOK, 2 * HEAD), BF16), pltpu.VMEM((4, TOK + LENT, HEAD), F32),
            pltpu.VMEM((4, TOK + LENT, 128), F32), pltpu.VMEM((8, 128) if fast else (4, TOK + LENT, 128), F32),
            pltpu.VMEM((4, LENT, HEAD), BF16), pltpu.VMEM((TOK, 2 * HEAD), BF16), pltpu.VMEM((TOK, D), BF16),
            pltpu.VMEM((2, 4, D, HEAD), BF16), pltpu.VMEM((2, D, HEAD), BF16), pltpu.VMEM((2, D, HEAD), BF16),
            pltpu.VMEM((4 * HEAD, D), BF16), pltpu.VMEM((D, FF), BF16), pltpu.VMEM((D, FF), BF16), pltpu.VMEM((FF, D), BF16),
            dma((11,)), dma((4 + TOK // FROWS,)), dma((N_TILE,)), dma((N_TILE,)), dma((4, N_TILE)), dma((4, N_TILE)), dma((N_SLOT,)), dma, dma((N_SLOT,)),
            dma((3,)), dma, dma((4,))],
        name="layers_fast" if fast else "layers_safe",
        compiler_params=pltpu.CompilerParams(vmem_limit_bytes=VLIM, collective_id=0 if fast else None, has_side_effects=True),
        cost_estimate=pl.CostEstimate(flops=60 * 10**9, bytes_accessed=30 << 20, transcendentals=0),
    )(ng, qg, *rope[0], *rope[1], x, wq, wk, wv, wo, wg, wu, wd)


def emit_kernel(*refs):
    ins, outs, mids, sem_in, sem_out = refs[0:5], refs[5:10], refs[10:15], refs[15], refs[16]
    loads = [pltpu.make_async_copy(i, m, sem_in.at[n]) for n, (i, m) in enumerate(zip(ins, mids))]
    stores = [pltpu.make_async_copy(m, o, sem_out.at[n]) for n, (m, o) in enumerate(zip(mids, outs))]
    for cp in loads:
        cp.start()
    for ld, st in zip(loads, stores):
        ld.wait()
        st.start()
    for st in stores:
        st.wait()


def emit(arrays):
    anyw = pl.BlockSpec(memory_space=pl.ANY)
    return pl.pallas_call(
        emit_kernel,
        in_specs=[anyw] * 5,
        out_specs=[anyw] * 5,
        out_shape=[jax.ShapeDtypeStruct(a.shape, a.dtype) for a in arrays],
        scratch_shapes=[pltpu.VMEM(a.shape, a.dtype) for a in arrays] + [pltpu.SemaphoreType.DMA((5,)), pltpu.SemaphoreType.DMA((5,))],
        name="emit",
    )(*arrays)


def solution(mesh):
    n_dev = mesh.shape['cp']
    rope = [rope_const(layer, TOK * n_dev) for layer in range(2)]

    def shard_body(x, ng, qg, w_q, w_k, w_v, w_o, w_gate, w_up, w_down):
        wq = w_q.transpose(0, 2, 1, 3)
        wk = w_k.reshape(2, D, HEAD)
        wv = w_v.reshape(2, D, HEAD)
        wo = w_o.reshape(2, 4 * HEAD, D)

        def run(fast):
            return tuple(layers(fast, ng, qg, rope, x, wq, wk, wv, wo, w_gate, w_up, w_down))

        *first, bound = run(True)
        _, rest = lax.while_loop(lambda c: c[0], lambda c: (jnp.zeros((), jnp.bool_), run(False)[:5]), (bound[0] > LIMIT, tuple(first)))
        out, k5, v5, kl, vl = emit(rest)
        return out, k5[:, None, :], v5[:, None, :], kl[:, None, :], vl[:, None, :]

    return jax.shard_map(shard_body, mesh=mesh, in_specs=(P('cp'), P(), P(), P(), P(), P(), P(), P(), P(), P()),
                         out_specs=(P('cp'), P('cp'), P('cp'), P(), P()), check_vma=False)
```

```python
import functools

import numpy as np
import jax
import jax.numpy as jnp
from jax import lax
from jax.experimental import pallas as pl
from jax.experimental.pallas import tpu as pltpu
from jax.sharding import PartitionSpec as P

WINDOW = 1024
EPS = 1e-6
BASES = (10000.0, 1000000.0)
SCALES = (1.0, 8.0)
HEAD = 256
TOK = 1024
D = 640
FF = 2048
TILE = 256
LO = 32
LOG2E = 1.4426950408889634
COEF = LOG2E / 16.0
TOP = 36.0
LIMIT = 56.0
NEG = -1e30
F32 = jnp.float32
BF16 = jnp.bfloat16
VLIM = 58 << 20


def rope_const(layer, seq_len):
    base, scale = BASES[layer], SCALES[layer]
    freq = base ** (-np.arange(HEAD // 2, dtype=np.float64) * 2.0 / HEAD)
    hi = (np.arange(seq_len // LO) * LO / scale)[:, None] * freq[None, :]
    lo = (np.arange(LO) / scale)[:, None] * freq[None, :]
    hi_tab = np.concatenate([np.cos(hi), np.sin(hi)], axis=1).astype(np.float32)
    lo_tab = np.concatenate([np.cos(lo), np.sin(lo)], axis=1).astype(np.float32)
    return hi_tab, lo_tab


def rms(x, gain):
    return x * lax.rsqrt(jnp.mean(x * x, axis=-1, keepdims=True) + EPS) * gain


def cos_sin(hi_ref, lo_ref, row0, rows):
    n_hi = rows // LO
    hi = hi_ref[pl.ds(pl.multiple_of(row0 // LO, 8), n_hi), :]
    lo = lo_ref[...]
    ch, sh = hi[:, None, 0:128], hi[:, None, 128:256]
    cl, sl = lo[None, :, 0:128], lo[None, :, 128:256]
    cos = (ch * cl - sh * sl).reshape(rows, 128)
    sin = (sh * cl + ch * sl).reshape(rows, 128)
    return cos, sin


def rotate(x, cos, sin):
    a, b = x[:, 0:128], x[:, 128:256]
    return jnp.concatenate([a * cos - b * sin, b * cos + a * sin], axis=1).astype(BF16)


def head_rope(proj, gain, cos, sin):
    return rotate(rms(proj.astype(BF16).astype(F32), gain), cos, sin)


def dot(a, b):
    return jnp.dot(a, b, preferred_element_type=F32)


def dot_t(a, b):
    return lax.dot_general(a, b, (((1,), (1,)), ((), ())), preferred_element_type=F32)


MESH = pl.DeviceIdType.MESH
N_SLOT = 8
OWN = 7
LENT = 256
N_TILE = TOK // TILE
QROWS = 512
FROWS = 512


def finish_rows(fast, x, attn, ng, wo, wg, wu, wd):
    o = dot(attn, wo[...]).astype(BF16).astype(F32)
    h1 = (x.astype(F32) + rms(o, 1.0 + ng[1:2, :])).astype(BF16)
    b = rms(h1.astype(F32), 1.0 + ng[2:3, :]).astype(BF16)

    def ff(cols):
        m = (jax.nn.gelu(dot(b, wg[:, cols]), approximate=True) * dot(b, wu[:, cols])).astype(BF16)
        return dot(m, wd[cols, :])

    if fast:
        acc = ff(slice(None))
    else:
        acc = lax.fori_loop(0, FF // 256, lambda f, part: part + ff(pl.ds(pl.multiple_of(f * 256, 256), 256)), jnp.zeros(h1.shape, F32))
    o2 = acc.astype(BF16).astype(F32)
    return (h1.astype(F32) + rms(o2, 1.0 + ng[3:4, :])).astype(BF16)


def layers_kernel(fast, ng_ref, qg_ref, hi4_ref, lo4_ref, hi5_ref, lo5_ref, x_hbm, wq_hbm, wk_hbm, wv_hbm, wo_hbm, wg_hbm, wu_hbm, wd_hbm,
                  out_hbm, k_hbm, v_hbm, kl_hbm, vl_hbm, bound_ref,
                  x, mid, win, q, buf, acc, l, m, lent, last, xo, wq, wk, wv, wo, wg, wu, wd,
                  load_sem, out_sem, halo_send, halo_recv, hop_send, hop_recv, pass_send, over_send, wide_recv, last_send, last_recv, lend_sem):
    me = lax.axis_index('cp')
    core = me % 2
    chip = me // 2
    partner = me + 1 - 2 * core
    xnb = me + 2 - 4 * (chip % 2)
    ynb = me + 4 - 8 * (chip // 2)
    top = 7
    is_last = me == top
    kv5 = buf.at[OWN]
    near, helper, far = chip == 0, chip == 1, chip == 3
    borrowed = pl.ds(TOK, LENT)

    def load(src, dst, n):
        return pltpu.make_async_copy(src, dst, load_sem.at[n])

    early = [load(x_hbm, x, 0), load(wk_hbm.at[0], wk.at[0], 1), load(wv_hbm.at[0], wv.at[0], 2), load(wq_hbm.at[0], wq.at[0], 3)]
    ff4 = [load(wo_hbm.at[0], wo, 4), load(wg_hbm.at[0], wg, 5), load(wu_hbm.at[0], wu, 6), load(wd_hbm.at[0], wd, 7)]
    next_qkv = [load(wk_hbm.at[1], wk.at[1], 8), load(wv_hbm.at[1], wv.at[1], 9), load(wq_hbm.at[1], wq.at[1], 10)]
    ff5 = [load(wo_hbm.at[1], wo, 4), load(wg_hbm.at[1], wg, 5), load(wu_hbm.at[1], wu, 6), load(wd_hbm.at[1], wd, 7)]
    for cp in early:
        cp.start()

    if fast:
        barrier = pltpu.get_barrier_semaphore()
        for other in (partner, xnb, ynb, (me + 1) % 8, (me + 7) % 8):
            pl.semaphore_signal(barrier, inc=1, device_id=(other,), device_id_type=MESH)
    for cp in ff4 + next_qkv:
        cp.start()

    @pl.when(me == 0)
    def _():
        win[0:WINDOW, :] = jnp.zeros((WINDOW, 2 * HEAD), BF16)

    if fast:
        pl.semaphore_wait(barrier, 5)

    def send(src, dst, ssem, rsem, dev):
        return pltpu.make_async_remote_copy(src_ref=src, dst_ref=dst, send_sem=ssem, recv_sem=rsem, device_id=(dev,), device_id_type=MESH)

    def heads(one):
        if fast:
            for h in range(4):
                one(h, 0)
        else:
            lax.fori_loop(0, 4, one, 0)

    def on(cond, copy, act):
        @pl.when(cond)
        def _():
            getattr(copy, act)()

    def rows_of(t, n=TILE):
        return pl.ds(pl.multiple_of(t * n, n), n)

    def halo_copy(t):
        return send(win.at[rows_of(t + N_TILE)], win.at[rows_of(t)], halo_send.at[t], halo_recv.at[t], (me + 1) % 8)

    gains = jnp.abs(1.0 + qg_ref[...])
    pair = jnp.maximum(gains[:, :, 0:HEAD // 2], gains[:, :, HEAD // 2:])
    bound = 16.0 * 1.02 * jnp.max(pair[:, 0:1] * pair[:, 1:2])
    bound_ref[0] = bound
    sigma = jnp.maximum(bound - TOP, 0.0) * LOG2E
    g4q, g4k = 1.0 + qg_ref[0, 0:1, :], 1.0 + qg_ref[0, 1:2, :]
    g5q, g5k = 1.0 + qg_ref[1, 0:1, :], 1.0 + qg_ref[1, 1:2, :]
    for cp in early[:3]:
        cp.wait()

    def kv_tile(it, carry):
        t = N_TILE - 1 - it
        cos, sin = cos_sin(hi4_ref, lo4_ref, me * TOK + t * TILE, TILE)
        a = rms(x[rows_of(t), :].astype(F32), 1.0 + ng_ref[0, 0:1, :]).astype(BF16)
        win[rows_of(t + N_TILE), 0:HEAD] = head_rope(dot(a, wk[0]), g4k, cos, sin)
        win[rows_of(t + N_TILE), HEAD:2 * HEAD] = dot(a, wv[0]).astype(BF16)
        on(me < top, halo_copy(t), 'start')
        return carry

    lax.fori_loop(0, N_TILE, kv_tile, 0)
    own4 = win.at[pl.ds(WINDOW, TOK)]
    last_cps = [send(own4, last, last_send.at[n], last_recv, dev) for n, dev in enumerate((partner, xnb, ynb))]
    for cp in last_cps:
        on(is_last, cp, 'start')
    early[3].wait()
    for cp in ff4 + next_qkv:
        cp.wait()

    def hops(t):
        def hop(k, slot, rk, dev):
            return send(kv5.at[rows_of(t)], buf.at[slot, rows_of(t)], hop_send.at[k, t], hop_recv.at[rk, t], dev)
        return [(jnp.logical_or(core == 0, helper), hop(0, 0, 0, partner)),
                (chip == 0, hop(1, 1, 1, xnb)),
                (chip == 0, hop(2, 1, 1, ynb)),
                (chip == 1, hop(2, 1, 1, ynb)),
                (chip == 2, hop(1, 3, 2, xnb)),
                (me == 5, hop(2, 3, 2, ynb)),
                (me == 6, hop(2, 5, 3, ynb)),
                (jnp.logical_and(me == 7, t == 0), hop(2, 6, 3, ynb))]

    def early_pass(t):
        return send(buf.at[1, rows_of(t)], buf.at[3, rows_of(t)], hop_send.at[3, t], hop_recv.at[2, t], xnb)

    def first_in(t):
        send(kv5.at[rows_of(t)], buf.at[1, rows_of(t)], hop_send.at[0, t], hop_recv.at[1, t], partner).wait_recv()

    def third_in(t):
        send(kv5.at[rows_of(t)], buf.at[3, rows_of(t)], hop_send.at[0, t], hop_recv.at[2, t], partner).wait_recv()

    def over_pass(k, t, dev):
        return send(buf.at[3, rows_of(t)], buf.at[3, rows_of(t)], hop_send.at[k, t], hop_recv.at[2, t], dev)

    lend = send(q.at[:, pl.ds(0, LENT), :], q.at[:, borrowed, :], lend_sem.at[0], lend_sem.at[1], ynb)
    give_back = send(lent, lent, lend_sem.at[2], lend_sem.at[3], ynb)

    n_key = WINDOW + TILE

    def nth(it):
        return jnp.where(it < 2, N_TILE - 1 - it, it - 2)

    def layer_tile(it, carry):
        t = nth(it)
        before = nth(jnp.maximum(it - 1, 0))
        rows = rows_of(t)
        cos, sin = cos_sin(hi4_ref, lo4_ref, me * TOK + t * TILE, TILE)
        a = rms(x[rows, :].astype(F32), 1.0 + ng_ref[0, 0:1, :]).astype(BF16)

        if fast:
            qs = [head_rope(dot(a, wq[0, h]), g4q, cos, sin) for h in range(4)]
        on(jnp.logical_and(me > 0, it < 2), halo_copy(t), 'wait_recv')
        for n in (1, 0):
            on(jnp.logical_and(me > 0, it == 2), halo_copy(n), 'wait_recv')
        start = pl.multiple_of(t * TILE, TILE)
        ks = win[pl.ds(start, n_key), 0:HEAD]
        vs = win[pl.ds(start, n_key), HEAD:2 * HEAD]
        col = lax.broadcasted_iota(jnp.int32, (1, n_key), 1)
        hidden = jnp.logical_and(me == 0, col + start < WINDOW)
        bias = jnp.where(hidden, NEG, -sigma if fast else 0.0)
        r = lax.broadcasted_iota(jnp.int32, (TILE, TILE), 0)
        c = lax.broadcasted_iota(jnp.int32, (TILE, TILE), 1)

        def local(h, q_h):
            s = dot_t(q_h, ks) * COEF + bias
            s = jnp.concatenate([jnp.where(c > r, s[:, 0:TILE], NEG), s[:, TILE:WINDOW], jnp.where(c <= r, s[:, WINDOW:], NEG)], axis=1)
            if not fast:
                s = s - jnp.max(s, axis=1, keepdims=True)
            p = jnp.exp2(s)
            total = jnp.sum(p, axis=1, keepdims=True)
            return dot(p.astype(BF16), vs) / total

        if fast:
            outs = [local(h, qs[h]).astype(BF16) for h in range(4)]
        else:
            def one(h, carry):
                acc[h, 0:TILE, :] = local(h, head_rope(dot(a, wq[0, h]), g4q, cos, sin))
                return carry
            heads(one)
            outs = [acc[h, 0:TILE, :].astype(BF16) for h in range(4)]
        h_mid = finish_rows(fast, x[rows, :], jnp.concatenate(outs, axis=1), ng_ref[0], wo, wg, wu, wd)
        mid[rows, :] = h_mid
        cos, sin = cos_sin(hi5_ref, lo5_ref, me * TOK + t * TILE, TILE)
        a = rms(h_mid.astype(F32), 1.0 + ng_ref[1, 0:1, :]).astype(BF16)
        kv5[rows, 0:HEAD] = head_rope(dot(a, wk[1]), g5k, cos, sin)
        kv5[rows, HEAD:2 * HEAD] = dot(a, wv[1]).astype(BF16)

        def project(h, carry):
            q[h, rows, :] = head_rope(dot(a, wq[1, h]), g5q, cos, sin)
            return carry

        heads(project)
        for cond, cp in hops(t):
            on(cond, cp, 'start')
        on(jnp.logical_and(far, it == 2), lend, 'start')

        @pl.when(jnp.logical_and(far, it >= 1))
        def _():
            first_in(before)
            early_pass(before).start()

        @pl.when(jnp.logical_and(me == 6, it >= 1))
        def _():
            third_in(before)
            over_pass(1, before, ynb).start()
        return carry

    lax.fori_loop(0, N_TILE, layer_tile, 0)
    outs5 = [pltpu.make_async_copy(kv5.at[:, pl.ds(0, HEAD)], k_hbm, out_sem.at[0]), pltpu.make_async_copy(kv5.at[:, pl.ds(HEAD, HEAD)], v_hbm, out_sem.at[1])]
    for cp in outs5 + ff5:
        cp.start()

    def attend(ks, vs, rows, width, masked, first, shift=None):
        n = rows.size
        if masked:
            r = lax.broadcasted_iota(jnp.int32, (n, n), 0)
            vis = lax.broadcasted_iota(jnp.int32, (n, n), 1) <= r
        if shift is not None:
            r = lax.broadcasted_iota(jnp.int32, (n, width), 0) + shift
            vis = lax.broadcasted_iota(jnp.int32, (n, width), 1) <= r
        def one(h, carry):
            s = dot_t(q[h, rows, :], ks)
            t = s * COEF - sigma if fast else s * COEF
            if shift is not None:
                t = jnp.where(vis, t, NEG)
            if masked:
                tail = jnp.where(vis, t[:, width - n:], NEG)
                t = tail if width == n else jnp.concatenate([t[:, 0:width - n], tail], axis=1)
            if not fast:
                mx = jnp.broadcast_to(jnp.max(t, axis=1, keepdims=True), (n, 128))
                fresh = mx if first else jnp.maximum(m[h, rows, :], mx)
                if not first:
                    decay = jnp.exp2(m[h, rows, :] - fresh)
                    l[h, rows, :] = l[h, rows, :] * decay
                    acc[h, rows, :] = acc[h, rows, :] * decay[:, 0:1]
                m[h, rows, :] = fresh
                t = t - fresh[:, 0:1]
            p = jnp.exp2(t)
            lp = p[:, 0:128]
            for j in range(1, width // 128):
                lp = lp + p[:, j * 128:(j + 1) * 128]
            o = dot(p.astype(BF16), vs)
            if first:
                l[h, rows, :] = lp
                acc[h, rows, :] = o
            else:
                l[h, rows, :] += lp
                acc[h, rows, :] += o
            return carry

        heads(one)

    base = jnp.where(far, LENT // TILE, 0)
    if not fast:
        def diag(i, carry):
            attend(kv5[:, 0:HEAD], kv5[:, HEAD:2 * HEAD], rows_of(i), TOK, False, True, i * TILE)
            return carry
        lax.fori_loop(base, N_TILE, diag, 0)
    for i in range(N_TILE if fast else 0):
        width = (i + 1) * TILE

        @pl.when(jnp.logical_or(i > 0, jnp.logical_not(far)))
        def _(i=i, width=width):
            attend(kv5[0:width, 0:HEAD], kv5[0:width, HEAD:2 * HEAD], pl.ds(i * TILE, TILE), width, True, True)

    def slot(s):
        ks = buf[s, :, 0:HEAD]
        vs = buf[s, :, HEAD:2 * HEAD]

        def q_rows(n, base):
            def one(i, carry):
                attend(ks, vs, pl.ds(pl.multiple_of(base + i * n, 128), n), TOK, False, False)
                return carry
            lax.fori_loop(0, (TOK - base) // n, one, 0)

        if not fast:
            def one(i, carry):
                attend(ks, vs, rows_of(i), TOK, False, False)
                return carry
            lax.fori_loop(base, N_TILE, one, 0)
            return

        @pl.when(far)
        def _():
            q_rows((TOK - LENT) // 2, LENT)

        @pl.when(jnp.logical_not(far))
        def _():
            q_rows(QROWS, 0)

    def wide(s, dst, ssem, dev):
        return send(buf.at[s], buf.at[dst], ssem, wide_recv.at[dst], dev)

    def relay(s):
        odd = s % 2 == 1
        return [(odd, wide(s, jnp.minimum(s + 1, N_SLOT - 1), pass_send.at[s], partner)),
                (jnp.logical_and(jnp.logical_and(chip == 1, core == 0), s == 1), wide(s, 5, over_send, ynb)),
                (jnp.logical_and(jnp.logical_and(chip == 2, core == 1), s == 1), wide(s, 5, over_send, xnb))]

    def chunks_in(cond, slot_no, rk, n=N_TILE):
        @pl.when(cond)
        def _():
            def one(t, carry):
                send(kv5.at[rows_of(t)], buf.at[slot_no, rows_of(t)], hop_send.at[0, t], hop_recv.at[rk, t], partner).wait_recv()
                return carry
            lax.fori_loop(0, n, one, 0)

    gives = jnp.logical_or(me == 3, jnp.logical_or(me == 5, me == 1))
    spread = [(gives, send(last, last, last_send.at[0], last_recv, partner)), (me == 3, send(last, last, last_send.at[1], last_recv, xnb))]

    def pass_last(cond):
        @pl.when(cond)
        def _():
            send(last, last, last_send.at[2], last_recv, partner).wait_recv()
            for c, cp in spread:
                on(c, cp, 'start')

    pass_last(jnp.logical_and(gives, me > 1))

    def step(s, carry):
        chunks_in(jnp.logical_and(s == 0, core == 1), 0, 0)
        chunks_in(jnp.logical_and(s == 1, chip < 3), 1, 1)
        chunks_in(jnp.logical_and(s == 3, me != 6), 3, 2)

        @pl.when(jnp.logical_and(far, jnp.where(core == 1, s == 0, s == 1)))
        def _():
            first_in(1)
            early_pass(1).start()

        @pl.when(jnp.logical_and(me == 6, s == 1))
        def _():
            third_in(1)
            over_pass(1, 1, ynb).start()

        @pl.when(jnp.logical_or(jnp.logical_and(s > 0, s % 2 == 0), s == 5))
        def _():
            wide(s, s, pass_send.at[s], partner).wait_recv()

        for cond, cp in relay(s):
            on(cond, cp, 'start')

        @pl.when(jnp.logical_or(s >= 1, core == 1))
        def _():
            slot(s)

        return carry

    @pl.when(me == 1)
    def _():
        def one(it, carry):
            t = nth(it)
            third_in(t)
            over_pass(3, t, xnb).start()
            return carry
        lax.fori_loop(0, N_TILE, one, 0)

    lax.fori_loop(0, 2 * chip + 1, step, 0)
    pass_last(me == 1)

    pass_six = send(buf.at[5], buf.at[5], pass_send.at[5], wide_recv.at[5], partner)
    pass_three = send(buf.at[3], buf.at[4], pass_send.at[3], wide_recv.at[4], partner)
    gets_six = jnp.logical_and(helper, core == 0)

    @pl.when(helper)
    def _():
        chunks_in(core == 0, 5, 3)
        chunks_in(core == 1, 6, 3, 1)
        on(core == 0, pass_six, 'start')
        chunks_in(core == 1, 3, 2)
        on(core == 1, pass_three, 'start')
        lend.wait_recv()
        attend(buf[5 + core, 0:LENT, 0:HEAD], buf[5 + core, 0:LENT, HEAD:2 * HEAD], borrowed, LENT, True, True)

        def block(k, carry):
            s = jnp.where(k == 0, OWN, jnp.where(k <= 4, k - 1, jnp.where(k == 5, 5, 4)))
            chunks_in(jnp.logical_and(k == 1, core == 0), 0, 0)
            chunks_in(jnp.logical_and(k == 4, core == 0), 3, 2)
            on(jnp.logical_and(k == 4, core == 0), pass_three, 'start')
            on(jnp.logical_and(k == 5, core == 1), pass_six, 'wait_recv')
            on(k == 6, pass_three, 'wait_recv')

            @pl.when(jnp.logical_or(k != 5, core == 1))
            def _():
                attend(buf[s, :, 0:HEAD], buf[s, :, HEAD:2 * HEAD], borrowed, TOK, False, False)
            return carry

        lax.fori_loop(0, 7, block, 0)
        for h in range(4):
            total = jnp.sum(l[h, borrowed, :], axis=1, keepdims=True)
            lent[h] = (acc[h, borrowed, :] / total).astype(BF16)
        give_back.start()

    @pl.when(jnp.logical_and(jnp.logical_not(gives), jnp.logical_not(is_last)))
    def _():
        send(last, last, last_send.at[2], last_recv, partner).wait_recv()

    def put_last(src):
        return [pltpu.make_async_copy(src.at[:, pl.ds(0, HEAD)], kl_hbm, out_sem.at[2]), pltpu.make_async_copy(src.at[:, pl.ds(HEAD, HEAD)], vl_hbm, out_sem.at[3])]

    for cp in put_last(own4):
        on(is_last, cp, 'start')
    for cp in put_last(last):
        on(jnp.logical_not(is_last), cp, 'start')

    for cp in ff5:
        cp.wait()

    def out_copy(t):
        return pltpu.make_async_copy(xo.at[rows_of(t, FROWS)], out_hbm.at[rows_of(t, FROWS)], out_sem.at[4 + t])

    def finish_tile(it, carry):
        t = (it + 1) % (TOK // FROWS)

        @pl.when(jnp.logical_and(far, t == 0))
        def _():
            give_back.wait_recv()
            for h in range(4):
                acc[h, 0:LENT, :] = lent[h].astype(F32)
                l[h, 0:LENT, :] = jnp.full((LENT, 128), 1.0 / 128.0, F32)

        rows = rows_of(t, FROWS)
        attn = []
        for h in range(4):
            total = jnp.sum(l[h, rows, :], axis=1, keepdims=True)
            attn.append((acc[h, rows, :] / total).astype(BF16))
        xo[rows, :] = finish_rows(fast, mid[rows, :], jnp.concatenate(attn, axis=1), ng_ref[1], wo, wg, wu, wd)
        out_copy(t).start()
        return carry

    lax.fori_loop(0, TOK // FROWS, finish_tile, 0)

    def drain_tile(t, carry):
        on(me < top, halo_copy(t), 'wait_send')
        on(far, early_pass(t), 'wait_send')
        on(me == 1, over_pass(3, t, xnb), 'wait_send')
        on(me == 6, over_pass(1, t, ynb), 'wait_send')
        for cond, cp in hops(t):
            on(cond, cp, 'wait_send')
        return carry

    lax.fori_loop(0, N_TILE, drain_tile, 0)

    def drain_step(s, carry):
        for cond, cp in relay(s):
            on(cond, cp, 'wait_send')
        return carry

    lax.fori_loop(1, 2 * chip + 1, drain_step, 0)
    for cp in last_cps:
        on(is_last, cp, 'wait_send')
    on(far, lend, 'wait_send')
    on(helper, give_back, 'wait_send')
    on(helper, pass_three, 'wait_send')
    on(gets_six, pass_six, 'wait_send')
    for cond, cp in spread:
        on(cond, cp, 'wait_send')
    for cp in outs5 + put_last(last):
        cp.wait()
    for t in range(TOK // FROWS):
        out_copy(t).wait()


def layers(fast, ng, qg, rope, x, wq, wk, wv, wo, wg, wu, wd):
    vm = pl.BlockSpec(memory_space=pltpu.VMEM)
    anyw = pl.BlockSpec(memory_space=pl.ANY)
    dma = pltpu.SemaphoreType.DMA
    kshape = jax.ShapeDtypeStruct((TOK, HEAD), BF16)
    return pl.pallas_call(
        functools.partial(layers_kernel, fast),
        in_specs=[vm] * 6 + [anyw] * 8,
        out_specs=[anyw] * 5 + [pl.BlockSpec(memory_space=pltpu.SMEM)],
        out_shape=[jax.ShapeDtypeStruct((TOK, D), BF16), kshape, kshape, kshape, kshape, jax.ShapeDtypeStruct((1,), F32)],
        scratch_shapes=[
            pltpu.VMEM((TOK, D), BF16), pltpu.VMEM((TOK, D), BF16), pltpu.VMEM((WINDOW + TOK, 2 * HEAD), BF16),
            pltpu.VMEM((4, TOK + LENT, HEAD), BF16), pltpu.VMEM((N_SLOT, TOK, 2 * HEAD), BF16), pltpu.VMEM((4, TOK + LENT, HEAD), F32),
            pltpu.VMEM((4, TOK + LENT, 128), F32), pltpu.VMEM((8, 128) if fast else (4, TOK + LENT, 128), F32),
            pltpu.VMEM((4, LENT, HEAD), BF16), pltpu.VMEM((TOK, 2 * HEAD), BF16), pltpu.VMEM((TOK, D), BF16),
            pltpu.VMEM((2, 4, D, HEAD), BF16), pltpu.VMEM((2, D, HEAD), BF16), pltpu.VMEM((2, D, HEAD), BF16),
            pltpu.VMEM((4 * HEAD, D), BF16), pltpu.VMEM((D, FF), BF16), pltpu.VMEM((D, FF), BF16), pltpu.VMEM((FF, D), BF16),
            dma((11,)), dma((4 + TOK // FROWS,)), dma((N_TILE,)), dma((N_TILE,)), dma((4, N_TILE)), dma((4, N_TILE)), dma((N_SLOT,)), dma, dma((N_SLOT,)),
            dma((3,)), dma, dma((4,))],
        name="layers_fast" if fast else "layers_safe",
        compiler_params=pltpu.CompilerParams(vmem_limit_bytes=VLIM, collective_id=0 if fast else None, has_side_effects=True),
        cost_estimate=pl.CostEstimate(flops=60 * 10**9, bytes_accessed=30 << 20, transcendentals=0),
    )(ng, qg, *rope[0], *rope[1], x, wq, wk, wv, wo, wg, wu, wd)


def emit_kernel(*refs):
    ins, outs, mids, sem_in, sem_out = refs[0:5], refs[5:10], refs[10:15], refs[15], refs[16]
    loads = [pltpu.make_async_copy(i, m, sem_in.at[n]) for n, (i, m) in enumerate(zip(ins, mids))]
    stores = [pltpu.make_async_copy(m, o, sem_out.at[n]) for n, (m, o) in enumerate(zip(mids, outs))]
    for cp in loads:
        cp.start()
    for ld, st in zip(loads, stores):
        ld.wait()
        st.start()
    for st in stores:
        st.wait()


def emit(arrays):
    anyw = pl.BlockSpec(memory_space=pl.ANY)
    return pl.pallas_call(
        emit_kernel,
        in_specs=[anyw] * 5,
        out_specs=[anyw] * 5,
        out_shape=[jax.ShapeDtypeStruct(a.shape, a.dtype) for a in arrays],
        scratch_shapes=[pltpu.VMEM(a.shape, a.dtype) for a in arrays] + [pltpu.SemaphoreType.DMA((5,)), pltpu.SemaphoreType.DMA((5,))],
        name="emit",
    )(*arrays)


def solution(mesh):
    n_dev = mesh.shape['cp']
    rope = [rope_const(layer, TOK * n_dev) for layer in range(2)]

    def shard_body(x, ng, qg, w_q, w_k, w_v, w_o, w_gate, w_up, w_down):
        wq = w_q.transpose(0, 2, 1, 3)
        wk = w_k.reshape(2, D, HEAD)
        wv = w_v.reshape(2, D, HEAD)
        wo = w_o.reshape(2, 4 * HEAD, D)

        def run(fast):
            return tuple(layers(fast, ng, qg, rope, x, wq, wk, wv, wo, w_gate, w_up, w_down))

        *first, bound = run(True)
        _, rest = lax.while_loop(lambda c: c[0], lambda c: (jnp.zeros((), jnp.bool_), run(False)[:5]), (bound[0] > LIMIT, tuple(first)))
        out, k5, v5, kl, vl = emit(rest)
        return out, k5[:, None, :], v5[:, None, :], kl[:, None, :], vl[:, None, :]

    return jax.shard_map(shard_body, mesh=mesh, in_specs=(P('cp'), P(), P(), P(), P(), P(), P(), P(), P(), P()),
                         out_specs=(P('cp'), P('cp'), P('cp'), P(), P()), check_vma=False)
```

```python
import functools

import numpy as np
import jax
import jax.numpy as jnp
from jax import lax
from jax.experimental import pallas as pl
from jax.experimental.pallas import tpu as pltpu
from jax.sharding import PartitionSpec as P

WINDOW = 1024
EPS = 1e-6
BASES = (10000.0, 1000000.0)
SCALES = (1.0, 8.0)
HEAD = 256
TOK = 1024
D = 640
FF = 2048
TILE = 256
LO = 32
LOG2E = 1.4426950408889634
COEF = LOG2E / 16.0
TOP = 36.0
LIMIT = 56.0
NEG = -1e30
F32 = jnp.float32
BF16 = jnp.bfloat16
VLIM = 58 << 20


def rope_const(layer, seq_len):
    base, scale = BASES[layer], SCALES[layer]
    freq = base ** (-np.arange(HEAD // 2, dtype=np.float64) * 2.0 / HEAD)
    hi = (np.arange(seq_len // LO) * LO / scale)[:, None] * freq[None, :]
    lo = (np.arange(LO) / scale)[:, None] * freq[None, :]
    hi_tab = np.concatenate([np.cos(hi), np.sin(hi)], axis=1).astype(np.float32)
    lo_tab = np.concatenate([np.cos(lo), np.sin(lo)], axis=1).astype(np.float32)
    return hi_tab, lo_tab


def rms(x, gain):
    return x * lax.rsqrt(jnp.mean(x * x, axis=-1, keepdims=True) + EPS) * gain


def cos_sin(hi_ref, lo_ref, row0, rows):
    n_hi = rows // LO
    hi = hi_ref[pl.ds(pl.multiple_of(row0 // LO, 8), n_hi), :]
    lo = lo_ref[...]
    ch, sh = hi[:, None, 0:128], hi[:, None, 128:256]
    cl, sl = lo[None, :, 0:128], lo[None, :, 128:256]
    cos = (ch * cl - sh * sl).reshape(rows, 128)
    sin = (sh * cl + ch * sl).reshape(rows, 128)
    return cos, sin


def rotate(x, cos, sin):
    a, b = x[:, 0:128], x[:, 128:256]
    return jnp.concatenate([a * cos - b * sin, b * cos + a * sin], axis=1).astype(BF16)


def head_rope(proj, gain, cos, sin):
    return rotate(rms(proj.astype(BF16).astype(F32), gain), cos, sin)


def dot(a, b):
    return jnp.dot(a, b, preferred_element_type=F32)


def dot_t(a, b):
    return lax.dot_general(a, b, (((1,), (1,)), ((), ())), preferred_element_type=F32)


MESH = pl.DeviceIdType.MESH
N_SLOT = 8
OWN = 7
LENT = 256
N_TILE = TOK // TILE
QROWS = 512
FROWS = 512
PARTS = 2


def finish_rows(fast, x, attn, ng, wo, wg, wu, wd):
    n = PARTS if fast else 1
    size = x.shape[0] // n
    groups = [slice(i * size, (i + 1) * size) for i in range(n)]

    def ff(b, cols):
        m = (jax.nn.gelu(dot(b, wg[:, cols]), approximate=True) * dot(b, wu[:, cols])).astype(BF16)
        return m if fast else dot(m, wd[cols, :])

    o = [dot(attn[g], wo[...]).astype(BF16).astype(F32) for g in groups]
    h1, b = [], []
    for g, o_g in zip(groups, o):
        h1.append((x[g].astype(F32) + rms(o_g, 1.0 + ng[1:2, :])).astype(BF16))
        b.append(rms(h1[-1].astype(F32), 1.0 + ng[2:3, :]).astype(BF16))
    if fast:
        m = [ff(b_g, slice(None)) for b_g in b]
        y = [dot(m_g, wd[...]) for m_g in m]
    else:
        y = [lax.fori_loop(0, FF // 256, lambda f, part: part + ff(b[0], pl.ds(pl.multiple_of(f * 256, 256), 256)), jnp.zeros(x.shape, F32))]
    return [(h_g.astype(F32) + rms(y_g.astype(BF16).astype(F32), 1.0 + ng[3:4, :])).astype(BF16) for h_g, y_g in zip(h1, y)]


def layers_kernel(fast, ng_hbm, qg_hbm, hi4_hbm, lo4_hbm, hi5_hbm, lo5_hbm, x_hbm, wq_hbm, wk_hbm, wv_hbm, wo_hbm, wg_hbm, wu_hbm, wd_hbm,
                  out_hbm, k_hbm, v_hbm, kl_hbm, vl_hbm, bound_ref,
                  ng_ref, qg_ref, hi4_ref, lo4_ref, hi5_ref, lo5_ref, x, mid, win, q, buf, acc, l, m, lent, last, xo, wq, wk, wv, wo, wg, wu, wd,
                  load_sem, out_sem, halo_send, halo_recv, hop_send, hop_recv, pass_send, over_send, wide_recv, last_send, last_recv, lend_sem):
    me = lax.axis_index('cp')
    core = me % 2
    chip = me // 2
    partner = me + 1 - 2 * core
    xnb = me + 2 - 4 * (chip % 2)
    ynb = me + 4 - 8 * (chip // 2)
    top = 7
    is_last = me == top
    kv5 = buf.at[OWN]
    near, helper, far = chip == 0, chip == 1, chip == 3
    borrowed = pl.ds(TOK, LENT)

    def load(src, dst, n):
        return pltpu.make_async_copy(src, dst, load_sem.at[n])

    turns = pl.ds(pl.multiple_of(me * (TOK // LO), TOK // LO), TOK // LO)
    small = [load(ng_hbm, ng_ref, 11), load(qg_hbm, qg_ref, 12), load(hi4_hbm.at[turns], hi4_ref, 13), load(lo4_hbm, lo4_ref, 14),
             load(hi5_hbm.at[turns], hi5_ref, 15), load(lo5_hbm, lo5_ref, 16)]
    early = [load(x_hbm, x, 0), load(wk_hbm.at[0], wk.at[0], 1), load(wv_hbm.at[0], wv.at[0], 2), load(wq_hbm.at[0], wq.at[0], 3)]
    ff4 = [load(wo_hbm.at[0], wo, 4), load(wg_hbm.at[0], wg, 5), load(wu_hbm.at[0], wu, 6), load(wd_hbm.at[0], wd, 7)]
    next_qkv = [load(wk_hbm.at[1], wk.at[1], 8), load(wv_hbm.at[1], wv.at[1], 9), load(wq_hbm.at[1], wq.at[1], 10)]
    ff5 = [load(wo_hbm.at[1], wo, 4), load(wg_hbm.at[1], wg, 5), load(wu_hbm.at[1], wu, 6), load(wd_hbm.at[1], wd, 7)]
    for cp in small + early:
        cp.start()

    if fast:
        barrier = pltpu.get_barrier_semaphore()
        for other in (partner, xnb, ynb, (me + 1) % 8, (me + 7) % 8):
            pl.semaphore_signal(barrier, inc=1, device_id=(other,), device_id_type=MESH)
    for cp in ff4 + next_qkv:
        cp.start()

    @pl.when(me == 0)
    def _():
        win[0:WINDOW, :] = jnp.zeros((WINDOW, 2 * HEAD), BF16)


    def send(src, dst, ssem, rsem, dev):
        return pltpu.make_async_remote_copy(src_ref=src, dst_ref=dst, send_sem=ssem, recv_sem=rsem, device_id=(dev,), device_id_type=MESH)

    def heads(one):
        if fast:
            for h in range(4):
                one(h, 0)
        else:
            lax.fori_loop(0, 4, one, 0)

    def on(cond, copy, act):
        @pl.when(cond)
        def _():
            getattr(copy, act)()

    def rows_of(t, n=TILE):
        return pl.ds(pl.multiple_of(t * n, n), n)

    def halo_copy(t):
        return send(win.at[rows_of(t + N_TILE)], win.at[rows_of(t)], halo_send.at[t], halo_recv.at[t], (me + 1) % 8)

    for cp in small + early[:3]:
        cp.wait()
    gains = jnp.abs(1.0 + qg_ref[...])
    pair = jnp.maximum(gains[:, :, 0:HEAD // 2], gains[:, :, HEAD // 2:])
    bound = 16.0 * 1.02 * jnp.max(pair[:, 0:1] * pair[:, 1:2])
    bound_ref[0] = bound
    sigma = jnp.maximum(bound - TOP, 0.0) * LOG2E
    g4q, g4k = 1.0 + qg_ref[0, 0:1, :], 1.0 + qg_ref[0, 1:2, :]
    g5q, g5k = 1.0 + qg_ref[1, 0:1, :], 1.0 + qg_ref[1, 1:2, :]
    def kv_tile(it, carry):
        t = N_TILE - 1 - it
        cos, sin = cos_sin(hi4_ref, lo4_ref, t * TILE, TILE)
        a = rms(x[rows_of(t), :].astype(F32), 1.0 + ng_ref[0, 0:1, :]).astype(BF16)
        mid[rows_of(t), :] = a
        win[rows_of(t + N_TILE), 0:HEAD] = head_rope(dot(a, wk[0]), g4k, cos, sin)
        win[rows_of(t + N_TILE), HEAD:2 * HEAD] = dot(a, wv[0]).astype(BF16)
        if fast:
            @pl.when(it == 0)
            def _():
                pl.semaphore_wait(barrier, 5)
        on(me < top, halo_copy(t), 'start')
        return carry

    lax.fori_loop(0, N_TILE, kv_tile, 0)
    own4 = win.at[pl.ds(WINDOW, TOK)]
    last_cps = [send(own4, last, last_send.at[n], last_recv, dev) for n, dev in enumerate((partner, xnb, ynb))]
    for cp in last_cps:
        on(is_last, cp, 'start')
    early[3].wait()
    for cp in ff4 + next_qkv:
        cp.wait()

    def hops(t):
        def hop(k, slot, rk, dev):
            return send(kv5.at[rows_of(t)], buf.at[slot, rows_of(t)], hop_send.at[k, t], hop_recv.at[rk, t], dev)
        return [(jnp.logical_or(core == 0, helper), hop(0, 0, 0, partner)),
                (chip == 0, hop(1, 1, 1, xnb)),
                (chip == 0, hop(2, 1, 1, ynb)),
                (chip == 1, hop(2, 1, 1, ynb)),
                (chip == 2, hop(1, 3, 2, xnb)),
                (me == 5, hop(2, 3, 2, ynb)),
                (me == 6, hop(2, 5, 3, ynb)),
                (jnp.logical_and(me == 7, t == 0), hop(2, 6, 3, ynb))]

    def early_pass(t):
        return send(buf.at[1, rows_of(t)], buf.at[3, rows_of(t)], hop_send.at[3, t], hop_recv.at[2, t], xnb)

    def first_in(t):
        send(kv5.at[rows_of(t)], buf.at[1, rows_of(t)], hop_send.at[0, t], hop_recv.at[1, t], partner).wait_recv()

    def third_in(t):
        send(kv5.at[rows_of(t)], buf.at[3, rows_of(t)], hop_send.at[0, t], hop_recv.at[2, t], partner).wait_recv()

    def over_pass(k, t, dev):
        return send(buf.at[3, rows_of(t)], buf.at[3, rows_of(t)], hop_send.at[k, t], hop_recv.at[2, t], dev)

    lend = send(q.at[:, pl.ds(0, LENT), :], q.at[:, borrowed, :], lend_sem.at[0], lend_sem.at[1], ynb)
    give_back = send(lent, lent, lend_sem.at[2], lend_sem.at[3], ynb)

    n_key = WINDOW + TILE

    def nth(it):
        return jnp.where(it < 2, N_TILE - 1 - it, it - 2)

    def layer_tile(it, carry):
        t = nth(it)
        before = nth(jnp.maximum(it - 1, 0))
        rows = rows_of(t)
        cos, sin = cos_sin(hi4_ref, lo4_ref, t * TILE, TILE)
        a = mid[rows, :]

        if fast:
            qs = [head_rope(dot(a, wq[0, h]), g4q, cos, sin) for h in range(4)]
        on(jnp.logical_and(me > 0, it < 2), halo_copy(t), 'wait_recv')
        for n in (1, 0):
            on(jnp.logical_and(me > 0, it == 2), halo_copy(n), 'wait_recv')
        start = pl.multiple_of(t * TILE, TILE)
        ks = win[pl.ds(start, n_key), 0:HEAD]
        vs = win[pl.ds(start, n_key), HEAD:2 * HEAD]
        col = lax.broadcasted_iota(jnp.int32, (1, n_key), 1)
        hidden = jnp.logical_and(me == 0, col + start < WINDOW)
        bias = jnp.where(hidden, NEG, -sigma if fast else 0.0)
        r = lax.broadcasted_iota(jnp.int32, (TILE, TILE), 0)
        c = lax.broadcasted_iota(jnp.int32, (TILE, TILE), 1)

        def local(h, q_h):
            s = dot_t(q_h, ks) * COEF + bias
            s = jnp.concatenate([jnp.where(c > r, s[:, 0:TILE], NEG), s[:, TILE:WINDOW], jnp.where(c <= r, s[:, WINDOW:], NEG)], axis=1)
            if not fast:
                s = s - jnp.max(s, axis=1, keepdims=True)
            p = jnp.exp2(s)
            total = jnp.sum(p, axis=1, keepdims=True)
            return dot(p.astype(BF16), vs) / total

        if fast:
            outs = [local(h, qs[h]).astype(BF16) for h in range(4)]
        else:
            def one(h, carry):
                acc[h, 0:TILE, :] = local(h, head_rope(dot(a, wq[0, h]), g4q, cos, sin))
                return carry
            heads(one)
            outs = [acc[h, 0:TILE, :].astype(BF16) for h in range(4)]
        h_mid = finish_rows(fast, x[rows, :], jnp.concatenate(outs, axis=1), ng_ref[0], wo, wg, wu, wd)
        cos, sin = cos_sin(hi5_ref, lo5_ref, t * TILE, TILE)
        size = TILE // len(h_mid)
        parts = []
        for i, h_g in enumerate(h_mid):
            here = pl.ds(pl.multiple_of(t * TILE + i * size, size), size)
            mid[here, :] = h_g
            parts.append((here, rms(h_g.astype(F32), 1.0 + ng_ref[1, 0:1, :]).astype(BF16), cos[i * size:(i + 1) * size], sin[i * size:(i + 1) * size]))
        for here, a_g, cos_g, sin_g in parts:
            kv5[here, 0:HEAD] = head_rope(dot(a_g, wk[1]), g5k, cos_g, sin_g)
            kv5[here, HEAD:2 * HEAD] = dot(a_g, wv[1]).astype(BF16)

        def project(h, carry):
            for here, a_g, cos_g, sin_g in parts:
                q[h, here, :] = head_rope(dot(a_g, wq[1, h]), g5q, cos_g, sin_g)
            return carry

        heads(project)
        for cond, cp in hops(t):
            on(cond, cp, 'start')
        on(jnp.logical_and(far, it == 2), lend, 'start')

        @pl.when(jnp.logical_and(far, it >= 1))
        def _():
            first_in(before)
            early_pass(before).start()

        @pl.when(jnp.logical_and(me == 6, it >= 1))
        def _():
            third_in(before)
            over_pass(1, before, ynb).start()
        return carry

    lax.fori_loop(0, N_TILE, layer_tile, 0)
    outs5 = [pltpu.make_async_copy(kv5.at[:, pl.ds(0, HEAD)], k_hbm, out_sem.at[0]), pltpu.make_async_copy(kv5.at[:, pl.ds(HEAD, HEAD)], v_hbm, out_sem.at[1])]
    for cp in outs5 + ff5:
        cp.start()

    def attend(ks, vs, rows, width, masked, first, shift=None):
        n = rows.size
        if masked:
            r = lax.broadcasted_iota(jnp.int32, (n, n), 0)
            vis = lax.broadcasted_iota(jnp.int32, (n, n), 1) <= r
        if shift is not None:
            r = lax.broadcasted_iota(jnp.int32, (n, width), 0) + shift
            vis = lax.broadcasted_iota(jnp.int32, (n, width), 1) <= r
        def one(h, carry):
            s = dot_t(q[h, rows, :], ks)
            t = s * COEF - sigma if fast else s * COEF
            if shift is not None:
                t = jnp.where(vis, t, NEG)
            if masked:
                tail = jnp.where(vis, t[:, width - n:], NEG)
                t = tail if width == n else jnp.concatenate([t[:, 0:width - n], tail], axis=1)
            if not fast:
                mx = jnp.broadcast_to(jnp.max(t, axis=1, keepdims=True), (n, 128))
                fresh = mx if first else jnp.maximum(m[h, rows, :], mx)
                if not first:
                    decay = jnp.exp2(m[h, rows, :] - fresh)
                    l[h, rows, :] = l[h, rows, :] * decay
                    acc[h, rows, :] = acc[h, rows, :] * decay[:, 0:1]
                m[h, rows, :] = fresh
                t = t - fresh[:, 0:1]
            p = jnp.exp2(t)
            lp = p[:, 0:128]
            for j in range(1, width // 128):
                lp = lp + p[:, j * 128:(j + 1) * 128]
            o = dot(p.astype(BF16), vs)
            if first:
                l[h, rows, :] = lp
                acc[h, rows, :] = o
            else:
                l[h, rows, :] += lp
                acc[h, rows, :] += o
            return carry

        heads(one)

    base = jnp.where(far, LENT // TILE, 0)
    if not fast:
        def diag(i, carry):
            attend(kv5[:, 0:HEAD], kv5[:, HEAD:2 * HEAD], rows_of(i), TOK, False, True, i * TILE)
            return carry
        lax.fori_loop(base, N_TILE, diag, 0)
    for i in range(N_TILE if fast else 0):
        width = (i + 1) * TILE

        @pl.when(jnp.logical_or(i > 0, jnp.logical_not(far)))
        def _(i=i, width=width):
            attend(kv5[0:width, 0:HEAD], kv5[0:width, HEAD:2 * HEAD], pl.ds(i * TILE, TILE), width, True, True)

    def slot(s):
        ks = buf[s, :, 0:HEAD]
        vs = buf[s, :, HEAD:2 * HEAD]

        def q_rows(n, base):
            def one(i, carry):
                attend(ks, vs, pl.ds(pl.multiple_of(base + i * n, 128), n), TOK, False, False)
                return carry
            lax.fori_loop(0, (TOK - base) // n, one, 0)

        if not fast:
            def one(i, carry):
                attend(ks, vs, rows_of(i), TOK, False, False)
                return carry
            lax.fori_loop(base, N_TILE, one, 0)
            return

        @pl.when(far)
        def _():
            q_rows(TOK - LENT, LENT)

        @pl.when(jnp.logical_not(far))
        def _():
            q_rows(QROWS, 0)

    def wide(s, dst, ssem, dev):
        return send(buf.at[s], buf.at[dst], ssem, wide_recv.at[dst], dev)

    def relay(s):
        odd = s % 2 == 1
        return [(odd, wide(s, jnp.minimum(s + 1, N_SLOT - 1), pass_send.at[s], partner)),
                (jnp.logical_and(jnp.logical_and(chip == 1, core == 0), s == 1), wide(s, 5, over_send, ynb)),
                (jnp.logical_and(jnp.logical_and(chip == 2, core == 1), s == 1), wide(s, 5, over_send, xnb))]

    def chunks_in(cond, slot_no, rk, n=N_TILE):
        @pl.when(cond)
        def _():
            def one(t, carry):
                send(kv5.at[rows_of(t)], buf.at[slot_no, rows_of(t)], hop_send.at[0, t], hop_recv.at[rk, t], partner).wait_recv()
                return carry
            lax.fori_loop(0, n, one, 0)

    gives = jnp.logical_or(me == 3, jnp.logical_or(me == 5, me == 1))
    spread = [(gives, send(last, last, last_send.at[0], last_recv, partner)), (me == 3, send(last, last, last_send.at[1], last_recv, xnb))]

    def pass_last(cond):
        @pl.when(cond)
        def _():
            send(last, last, last_send.at[2], last_recv, partner).wait_recv()
            for c, cp in spread:
                on(c, cp, 'start')

    pass_last(jnp.logical_and(gives, me > 1))

    def step(s, carry):
        chunks_in(jnp.logical_and(s == 0, core == 1), 0, 0)
        chunks_in(jnp.logical_and(s == 1, chip < 3), 1, 1)
        chunks_in(jnp.logical_and(s == 3, me != 6), 3, 2)

        @pl.when(jnp.logical_and(far, jnp.where(core == 1, s == 0, s == 1)))
        def _():
            first_in(1)
            early_pass(1).start()

        @pl.when(jnp.logical_and(me == 6, s == 1))
        def _():
            third_in(1)
            over_pass(1, 1, ynb).start()

        @pl.when(jnp.logical_or(jnp.logical_and(s > 0, s % 2 == 0), s == 5))
        def _():
            wide(s, s, pass_send.at[s], partner).wait_recv()

        for cond, cp in relay(s):
            on(cond, cp, 'start')

        @pl.when(jnp.logical_or(s >= 1, core == 1))
        def _():
            slot(s)

        return carry

    @pl.when(me == 1)
    def _():
        def one(it, carry):
            t = nth(it)
            third_in(t)
            over_pass(3, t, xnb).start()
            return carry
        lax.fori_loop(0, N_TILE, one, 0)

    lax.fori_loop(0, 2 * chip + 1, step, 0)
    pass_last(me == 1)

    pass_six = send(buf.at[5], buf.at[5], pass_send.at[5], wide_recv.at[5], partner)
    pass_three = send(buf.at[3], buf.at[4], pass_send.at[3], wide_recv.at[4], partner)
    gets_six = jnp.logical_and(helper, core == 0)

    @pl.when(helper)
    def _():
        chunks_in(core == 0, 5, 3)
        chunks_in(core == 1, 6, 3, 1)
        on(core == 0, pass_six, 'start')
        chunks_in(core == 1, 3, 2)
        on(core == 1, pass_three, 'start')
        lend.wait_recv()
        attend(buf[5 + core, 0:LENT, 0:HEAD], buf[5 + core, 0:LENT, HEAD:2 * HEAD], borrowed, LENT, True, True)

        def block(k, carry):
            s = jnp.where(k == 0, OWN, jnp.where(k <= 4, k - 1, jnp.where(k == 5, 5, 4)))
            chunks_in(jnp.logical_and(k == 1, core == 0), 0, 0)
            chunks_in(jnp.logical_and(k == 4, core == 0), 3, 2)
            on(jnp.logical_and(k == 4, core == 0), pass_three, 'start')
            on(jnp.logical_and(k == 5, core == 1), pass_six, 'wait_recv')
            on(k == 6, pass_three, 'wait_recv')

            @pl.when(jnp.logical_or(k != 5, core == 1))
            def _():
                attend(buf[s, :, 0:HEAD], buf[s, :, HEAD:2 * HEAD], borrowed, TOK, False, False)
            return carry

        lax.fori_loop(0, 7, block, 0)
        for h in range(4):
            total = jnp.sum(l[h, borrowed, :], axis=1, keepdims=True)
            lent[h] = (acc[h, borrowed, :] / total).astype(BF16)
        give_back.start()

    @pl.when(jnp.logical_and(jnp.logical_not(gives), jnp.logical_not(is_last)))
    def _():
        send(last, last, last_send.at[2], last_recv, partner).wait_recv()

    def put_last(src):
        return [pltpu.make_async_copy(src.at[:, pl.ds(0, HEAD)], kl_hbm, out_sem.at[2]), pltpu.make_async_copy(src.at[:, pl.ds(HEAD, HEAD)], vl_hbm, out_sem.at[3])]

    for cp in put_last(own4):
        on(is_last, cp, 'start')
    for cp in put_last(last):
        on(jnp.logical_not(is_last), cp, 'start')

    for cp in ff5:
        cp.wait()

    def out_copy(t):
        return pltpu.make_async_copy(xo.at[rows_of(t, FROWS)], out_hbm.at[rows_of(t, FROWS)], out_sem.at[4 + t])

    def finish_tile(it, carry):
        t = (it + 1) % (TOK // FROWS)

        @pl.when(jnp.logical_and(far, t == 0))
        def _():
            give_back.wait_recv()
            for h in range(4):
                acc[h, 0:LENT, :] = lent[h].astype(F32)
                l[h, 0:LENT, :] = jnp.full((LENT, 128), 1.0 / 128.0, F32)

        rows = rows_of(t, FROWS)
        attn = []
        for h in range(4):
            total = jnp.sum(l[h, rows, :], axis=1, keepdims=True)
            attn.append((acc[h, rows, :] / total).astype(BF16))
        xo[rows, :] = jnp.concatenate(finish_rows(fast, mid[rows, :], jnp.concatenate(attn, axis=1), ng_ref[1], wo, wg, wu, wd), axis=0)
        out_copy(t).start()
        return carry

    lax.fori_loop(0, TOK // FROWS, finish_tile, 0)

    def drain_tile(t, carry):
        on(me < top, halo_copy(t), 'wait_send')
        on(far, early_pass(t), 'wait_send')
        on(me == 1, over_pass(3, t, xnb), 'wait_send')
        on(me == 6, over_pass(1, t, ynb), 'wait_send')
        for cond, cp in hops(t):
            on(cond, cp, 'wait_send')
        return carry

    lax.fori_loop(0, N_TILE, drain_tile, 0)

    def drain_step(s, carry):
        for cond, cp in relay(s):
            on(cond, cp, 'wait_send')
        return carry

    lax.fori_loop(1, 2 * chip + 1, drain_step, 0)
    for cp in last_cps:
        on(is_last, cp, 'wait_send')
    on(far, lend, 'wait_send')
    on(helper, give_back, 'wait_send')
    on(helper, pass_three, 'wait_send')
    on(gets_six, pass_six, 'wait_send')
    for cond, cp in spread:
        on(cond, cp, 'wait_send')
    for cp in outs5 + put_last(last):
        cp.wait()
    for t in range(TOK // FROWS):
        out_copy(t).wait()


def layers(fast, ng, qg, rope, x, wq, wk, wv, wo, wg, wu, wd):
    anyw = pl.BlockSpec(memory_space=pl.ANY)
    dma = pltpu.SemaphoreType.DMA
    kshape = jax.ShapeDtypeStruct((TOK, HEAD), BF16)
    return pl.pallas_call(
        functools.partial(layers_kernel, fast),
        in_specs=[anyw] * 14,
        out_specs=[anyw] * 5 + [pl.BlockSpec(memory_space=pltpu.SMEM)],
        out_shape=[jax.ShapeDtypeStruct((TOK, D), BF16), kshape, kshape, kshape, kshape, jax.ShapeDtypeStruct((1,), F32)],
        scratch_shapes=[
            pltpu.VMEM((2, 4, D), F32), pltpu.VMEM((2, 2, HEAD), F32), pltpu.VMEM((TOK // LO, HEAD), F32), pltpu.VMEM((LO, HEAD), F32),
            pltpu.VMEM((TOK // LO, HEAD), F32), pltpu.VMEM((LO, HEAD), F32), pltpu.VMEM((TOK, D), BF16), pltpu.VMEM((TOK, D), BF16), pltpu.VMEM((WINDOW + TOK, 2 * HEAD), BF16),
            pltpu.VMEM((4, TOK + LENT, HEAD), BF16), pltpu.VMEM((N_SLOT, TOK, 2 * HEAD), BF16), pltpu.VMEM((4, TOK + LENT, HEAD), F32),
            pltpu.VMEM((4, TOK + LENT, 128), F32), pltpu.VMEM((8, 128) if fast else (4, TOK + LENT, 128), F32),
            pltpu.VMEM((4, LENT, HEAD), BF16), pltpu.VMEM((TOK, 2 * HEAD), BF16), pltpu.VMEM((TOK, D), BF16),
            pltpu.VMEM((2, 4, D, HEAD), BF16), pltpu.VMEM((2, D, HEAD), BF16), pltpu.VMEM((2, D, HEAD), BF16),
            pltpu.VMEM((4 * HEAD, D), BF16), pltpu.VMEM((D, FF), BF16), pltpu.VMEM((D, FF), BF16), pltpu.VMEM((FF, D), BF16),
            dma((17,)), dma((4 + TOK // FROWS,)), dma((N_TILE,)), dma((N_TILE,)), dma((4, N_TILE)), dma((4, N_TILE)), dma((N_SLOT,)), dma, dma((N_SLOT,)),
            dma((3,)), dma, dma((4,))],
        name="layers_fast" if fast else "layers_safe",
        compiler_params=pltpu.CompilerParams(vmem_limit_bytes=VLIM, collective_id=0 if fast else None, has_side_effects=True),
        cost_estimate=pl.CostEstimate(flops=60 * 10**9, bytes_accessed=30 << 20, transcendentals=0),
    )(ng, qg, *rope[0], *rope[1], x, wq, wk, wv, wo, wg, wu, wd)


def emit_kernel(*refs):
    ins, outs, mids, sem_in, sem_out = refs[0:5], refs[5:10], refs[10:15], refs[15], refs[16]
    loads = [pltpu.make_async_copy(i, m, sem_in.at[n]) for n, (i, m) in enumerate(zip(ins, mids))]
    stores = [pltpu.make_async_copy(m, o, sem_out.at[n]) for n, (m, o) in enumerate(zip(mids, outs))]
    for cp in loads:
        cp.start()
    for ld, st in zip(loads, stores):
        ld.wait()
        st.start()
    for st in stores:
        st.wait()


def emit(arrays):
    anyw = pl.BlockSpec(memory_space=pl.ANY)
    return pl.pallas_call(
        emit_kernel,
        in_specs=[anyw] * 5,
        out_specs=[anyw] * 5,
        out_shape=[jax.ShapeDtypeStruct(a.shape, a.dtype) for a in arrays],
        scratch_shapes=[pltpu.VMEM(a.shape, a.dtype) for a in arrays] + [pltpu.SemaphoreType.DMA((5,)), pltpu.SemaphoreType.DMA((5,))],
        name="emit",
    )(*arrays)


def solution(mesh):
    n_dev = mesh.shape['cp']
    rope = [rope_const(layer, TOK * n_dev) for layer in range(2)]

    def shard_body(x, ng, qg, w_q, w_k, w_v, w_o, w_gate, w_up, w_down):
        wq = w_q.transpose(0, 2, 1, 3)
        wk = w_k.reshape(2, D, HEAD)
        wv = w_v.reshape(2, D, HEAD)
        wo = w_o.reshape(2, 4 * HEAD, D)

        def run(fast):
            return tuple(layers(fast, ng, qg, rope, x, wq, wk, wv, wo, w_gate, w_up, w_down))

        *first, bound = run(True)
        _, rest = lax.while_loop(lambda c: c[0], lambda c: (jnp.zeros((), jnp.bool_), run(False)[:5]), (bound[0] > LIMIT, tuple(first)))
        out, k5, v5, kl, vl = emit(rest)
        return out, k5[:, None, :], v5[:, None, :], kl[:, None, :], vl[:, None, :]

    return jax.shard_map(shard_body, mesh=mesh, in_specs=(P('cp'), P(), P(), P(), P(), P(), P(), P(), P(), P()),
                         out_specs=(P('cp'), P('cp'), P('cp'), P(), P()), check_vma=False)
```

```python
import functools

import numpy as np
import jax
import jax.numpy as jnp
from jax import lax
from jax.experimental import pallas as pl
from jax.experimental.pallas import tpu as pltpu
from jax.sharding import PartitionSpec as P

WINDOW = 1024
EPS = 1e-6
BASES = (10000.0, 1000000.0)
SCALES = (1.0, 8.0)
HEAD = 256
TOK = 1024
D = 640
FF = 2048
TILE = 256
LO = 32
LOG2E = 1.4426950408889634
COEF = LOG2E / 16.0
TOP = 36.0
LIMIT = 56.0
NEG = -1e30
F32 = jnp.float32
BF16 = jnp.bfloat16
VLIM = 58 << 20


def rope_const(layer, seq_len):
    base, scale = BASES[layer], SCALES[layer]
    freq = base ** (-np.arange(HEAD // 2, dtype=np.float64) * 2.0 / HEAD)
    hi = (np.arange(seq_len // LO) * LO / scale)[:, None] * freq[None, :]
    lo = (np.arange(LO) / scale)[:, None] * freq[None, :]
    hi_tab = np.concatenate([np.cos(hi), np.sin(hi)], axis=1).astype(np.float32)
    lo_tab = np.concatenate([np.cos(lo), np.sin(lo)], axis=1).astype(np.float32)
    return hi_tab, lo_tab


def rms(x, gain):
    return x * lax.rsqrt(jnp.mean(x * x, axis=-1, keepdims=True) + EPS) * gain


def cos_sin(hi_ref, lo_ref, row0, rows):
    n_hi = rows // LO
    hi = hi_ref[pl.ds(pl.multiple_of(row0 // LO, 8), n_hi), :]
    lo = lo_ref[...]
    ch, sh = hi[:, None, 0:128], hi[:, None, 128:256]
    cl, sl = lo[None, :, 0:128], lo[None, :, 128:256]
    cos = (ch * cl - sh * sl).reshape(rows, 128)
    sin = (sh * cl + ch * sl).reshape(rows, 128)
    return cos, sin


def rotate(x, cos, sin):
    a, b = x[:, 0:128], x[:, 128:256]
    return jnp.concatenate([a * cos - b * sin, b * cos + a * sin], axis=1).astype(BF16)


def head_rope(proj, gain, cos, sin):
    return rotate(rms(proj.astype(BF16).astype(F32), gain), cos, sin)


def dot(a, b):
    return jnp.dot(a, b, preferred_element_type=F32)


def dot_t(a, b):
    return lax.dot_general(a, b, (((1,), (1,)), ((), ())), preferred_element_type=F32)


MESH = pl.DeviceIdType.MESH
N_SLOT = 8
OWN = 7
LENT = 256
N_TILE = TOK // TILE
QROWS = 512
FROWS = 512
PARTS = 2


def finish_rows(fast, x, attn, ng, wo, wg, wu, wd):
    n = PARTS if fast else 1
    size = x.shape[0] // n
    groups = [slice(i * size, (i + 1) * size) for i in range(n)]

    def ff(b, cols):
        m = (jax.nn.gelu(dot(b, wg[:, cols]), approximate=True) * dot(b, wu[:, cols])).astype(BF16)
        return m if fast else dot(m, wd[cols, :])

    o = [dot(attn[g], wo[...]).astype(BF16).astype(F32) for g in groups]
    h1, b = [], []
    for g, o_g in zip(groups, o):
        h1.append((x[g].astype(F32) + rms(o_g, 1.0 + ng[1:2, :])).astype(BF16))
        b.append(rms(h1[-1].astype(F32), 1.0 + ng[2:3, :]).astype(BF16))
    if fast:
        m = [ff(b_g, slice(None)) for b_g in b]
        y = [dot(m_g, wd[...]) for m_g in m]
    else:
        y = [lax.fori_loop(0, FF // 256, lambda f, part: part + ff(b[0], pl.ds(pl.multiple_of(f * 256, 256), 256)), jnp.zeros(x.shape, F32))]
    return [(h_g.astype(F32) + rms(y_g.astype(BF16).astype(F32), 1.0 + ng[3:4, :])).astype(BF16) for h_g, y_g in zip(h1, y)]


def layers_kernel(fast, ng_hbm, qg_hbm, hi4_hbm, lo4_hbm, hi5_hbm, lo5_hbm, x_hbm, wq_hbm, wk_hbm, wv_hbm, wo_hbm, wg_hbm, wu_hbm, wd_hbm,
                  out_hbm, k_hbm, v_hbm, kl_hbm, vl_hbm, bound_ref,
                  ng_ref, qg_ref, hi4_ref, lo4_ref, hi5_ref, lo5_ref, x, mid, win, q, buf, acc, l, m, lent, last, xo, wq, wk, wv, wo, wg, wu, wd,
                  load_sem, out_sem, halo_send, halo_recv, hop_send, hop_recv, pass_send, over_send, wide_recv, last_send, last_recv, lend_sem):
    me = lax.axis_index('cp')
    core = me % 2
    chip = me // 2
    partner = me + 1 - 2 * core
    xnb = me + 2 - 4 * (chip % 2)
    ynb = me + 4 - 8 * (chip // 2)
    top = 7
    is_last = me == top
    kv5 = buf.at[OWN]
    near, helper, far = chip == 0, chip == 1, chip == 3
    borrowed = pl.ds(TOK, LENT)

    def load(src, dst, n):
        return pltpu.make_async_copy(src, dst, load_sem.at[n])

    turns = pl.ds(pl.multiple_of(me * (TOK // LO), TOK // LO), TOK // LO)
    small = [load(ng_hbm, ng_ref, 11), load(qg_hbm, qg_ref, 12), load(hi4_hbm.at[turns], hi4_ref, 13), load(lo4_hbm, lo4_ref, 14),
             load(hi5_hbm.at[turns], hi5_ref, 15), load(lo5_hbm, lo5_ref, 16)]
    early = [load(x_hbm, x, 0), load(wk_hbm.at[0], wk.at[0], 1), load(wv_hbm.at[0], wv.at[0], 2), load(wq_hbm.at[0], wq.at[0], 3)]
    ff4 = [load(wo_hbm.at[0], wo, 4), load(wg_hbm.at[0], wg, 5), load(wu_hbm.at[0], wu, 6), load(wd_hbm.at[0], wd, 7)]
    next_qkv = [load(wk_hbm.at[1], wk.at[1], 8), load(wv_hbm.at[1], wv.at[1], 9), load(wq_hbm.at[1], wq.at[1], 10)]
    ff5 = [load(wo_hbm.at[1], wo, 4), load(wg_hbm.at[1], wg, 5), load(wu_hbm.at[1], wu, 6), load(wd_hbm.at[1], wd, 7)]
    for cp in small + early:
        cp.start()

    if fast:
        barrier = pltpu.get_barrier_semaphore()
        for other in (partner, xnb, ynb, (me + 1) % 8, (me + 7) % 8):
            pl.semaphore_signal(barrier, inc=1, device_id=(other,), device_id_type=MESH)
    for cp in ff4 + next_qkv:
        cp.start()

    @pl.when(me == 0)
    def _():
        win[0:WINDOW, :] = jnp.zeros((WINDOW, 2 * HEAD), BF16)


    def send(src, dst, ssem, rsem, dev):
        return pltpu.make_async_remote_copy(src_ref=src, dst_ref=dst, send_sem=ssem, recv_sem=rsem, device_id=(dev,), device_id_type=MESH)

    def heads(one):
        if fast:
            for h in range(4):
                one(h, 0)
        else:
            lax.fori_loop(0, 4, one, 0)

    def on(cond, copy, act):
        @pl.when(cond)
        def _():
            getattr(copy, act)()

    def rows_of(t, n=TILE):
        return pl.ds(pl.multiple_of(t * n, n), n)

    def halo_copy(t):
        return send(win.at[rows_of(t + N_TILE)], win.at[rows_of(t)], halo_send.at[t], halo_recv.at[t], (me + 1) % 8)

    for cp in small + early[:3]:
        cp.wait()
    gains = jnp.abs(1.0 + qg_ref[...])
    pair = jnp.maximum(gains[:, :, 0:HEAD // 2], gains[:, :, HEAD // 2:])
    bound = 16.0 * 1.02 * jnp.max(pair[:, 0:1] * pair[:, 1:2])
    bound_ref[0] = bound
    sigma = jnp.maximum(bound - TOP, 0.0) * LOG2E
    g4q, g4k = 1.0 + qg_ref[0, 0:1, :], 1.0 + qg_ref[0, 1:2, :]
    g5q, g5k = 1.0 + qg_ref[1, 0:1, :], 1.0 + qg_ref[1, 1:2, :]
    def kv_tile(it, carry):
        t = N_TILE - 1 - it
        cos, sin = cos_sin(hi4_ref, lo4_ref, t * TILE, TILE)
        a = rms(x[rows_of(t), :].astype(F32), 1.0 + ng_ref[0, 0:1, :]).astype(BF16)
        mid[rows_of(t), :] = a
        win[rows_of(t + N_TILE), 0:HEAD] = head_rope(dot(a, wk[0]), g4k, cos, sin)
        win[rows_of(t + N_TILE), HEAD:2 * HEAD] = dot(a, wv[0]).astype(BF16)
        if fast:
            @pl.when(it == 0)
            def _():
                pl.semaphore_wait(barrier, 5)
        on(me < top, halo_copy(t), 'start')
        return carry

    lax.fori_loop(0, N_TILE, kv_tile, 0)
    own4 = win.at[pl.ds(WINDOW, TOK)]
    last_cps = [send(own4, last, last_send.at[n], last_recv, dev) for n, dev in enumerate((partner, xnb, ynb))]
    for cp in last_cps:
        on(is_last, cp, 'start')
    early[3].wait()
    for cp in ff4 + next_qkv:
        cp.wait()

    def hops(t):
        def hop(k, slot, rk, dev):
            return send(kv5.at[rows_of(t)], buf.at[slot, rows_of(t)], hop_send.at[k, t], hop_recv.at[rk, t], dev)
        return [(jnp.logical_or(core == 0, helper), hop(0, 0, 0, partner)),
                (chip == 0, hop(1, 1, 1, xnb)),
                (chip == 0, hop(2, 1, 1, ynb)),
                (chip == 1, hop(2, 1, 1, ynb)),
                (chip == 2, hop(1, 3, 2, xnb)),
                (me == 5, hop(2, 3, 2, ynb)),
                (me == 6, hop(2, 5, 3, ynb)),
                (jnp.logical_and(me == 7, t == 0), hop(2, 6, 3, ynb))]

    def early_pass(t):
        return send(buf.at[1, rows_of(t)], buf.at[3, rows_of(t)], hop_send.at[3, t], hop_recv.at[2, t], xnb)

    def first_in(t):
        send(kv5.at[rows_of(t)], buf.at[1, rows_of(t)], hop_send.at[0, t], hop_recv.at[1, t], partner).wait_recv()

    def third_in(t):
        send(kv5.at[rows_of(t)], buf.at[3, rows_of(t)], hop_send.at[0, t], hop_recv.at[2, t], partner).wait_recv()

    def over_pass(k, t, dev):
        return send(buf.at[3, rows_of(t)], buf.at[3, rows_of(t)], hop_send.at[k, t], hop_recv.at[2, t], dev)

    lend = send(q.at[:, pl.ds(0, LENT), :], q.at[:, borrowed, :], lend_sem.at[0], lend_sem.at[1], ynb)
    give_back = send(lent, lent, lend_sem.at[2], lend_sem.at[3], ynb)

    n_key = WINDOW + TILE

    def nth(it):
        return jnp.where(it < 2, N_TILE - 1 - it, it - 2)

    def layer_tile(it, carry):
        t = nth(it)
        before = nth(jnp.maximum(it - 1, 0))
        rows = rows_of(t)
        cos, sin = cos_sin(hi4_ref, lo4_ref, t * TILE, TILE)
        a = mid[rows, :]

        if fast:
            qs = [head_rope(dot(a, wq[0, h]), g4q, cos, sin) for h in range(4)]
        on(jnp.logical_and(me > 0, it < 2), halo_copy(t), 'wait_recv')
        for n in (1, 0):
            on(jnp.logical_and(me > 0, it == 2), halo_copy(n), 'wait_recv')
        start = pl.multiple_of(t * TILE, TILE)
        ks = win[pl.ds(start, n_key), 0:HEAD]
        vs = win[pl.ds(start, n_key), HEAD:2 * HEAD]
        col = lax.broadcasted_iota(jnp.int32, (1, n_key), 1)
        hidden = jnp.logical_and(me == 0, col + start < WINDOW)
        bias = jnp.where(hidden, NEG, -sigma if fast else 0.0)
        r = lax.broadcasted_iota(jnp.int32, (TILE, TILE), 0)
        c = lax.broadcasted_iota(jnp.int32, (TILE, TILE), 1)

        def local(h, q_h):
            s = dot_t(q_h, ks) * COEF + bias
            s = jnp.concatenate([jnp.where(c > r, s[:, 0:TILE], NEG), s[:, TILE:WINDOW], jnp.where(c <= r, s[:, WINDOW:], NEG)], axis=1)
            if not fast:
                s = s - jnp.max(s, axis=1, keepdims=True)
            p = jnp.exp2(s)
            total = jnp.sum(p, axis=1, keepdims=True)
            return dot(p.astype(BF16), vs) / total

        if fast:
            outs = [local(h, qs[h]).astype(BF16) for h in range(4)]
        else:
            def one(h, carry):
                acc[h, 0:TILE, :] = local(h, head_rope(dot(a, wq[0, h]), g4q, cos, sin))
                return carry
            heads(one)
            outs = [acc[h, 0:TILE, :].astype(BF16) for h in range(4)]
        h_mid = finish_rows(fast, x[rows, :], jnp.concatenate(outs, axis=1), ng_ref[0], wo, wg, wu, wd)
        cos, sin = cos_sin(hi5_ref, lo5_ref, t * TILE, TILE)
        size = TILE // len(h_mid)
        parts = []
        for i, h_g in enumerate(h_mid):
            here = pl.ds(pl.multiple_of(t * TILE + i * size, size), size)
            mid[here, :] = h_g
            parts.append((here, rms(h_g.astype(F32), 1.0 + ng_ref[1, 0:1, :]).astype(BF16), cos[i * size:(i + 1) * size], sin[i * size:(i + 1) * size]))
        for here, a_g, cos_g, sin_g in parts:
            kv5[here, 0:HEAD] = head_rope(dot(a_g, wk[1]), g5k, cos_g, sin_g)
            kv5[here, HEAD:2 * HEAD] = dot(a_g, wv[1]).astype(BF16)

        def project(h, carry):
            for here, a_g, cos_g, sin_g in parts:
                q[h, here, :] = head_rope(dot(a_g, wq[1, h]), g5q, cos_g, sin_g)
            return carry

        heads(project)
        for cond, cp in hops(t):
            on(cond, cp, 'start')
        on(jnp.logical_and(far, it == 2), lend, 'start')

        @pl.when(jnp.logical_and(far, it >= 1))
        def _():
            first_in(before)
            early_pass(before).start()

        @pl.when(jnp.logical_and(me == 6, it >= 1))
        def _():
            third_in(before)
            over_pass(1, before, ynb).start()
        return carry

    lax.fori_loop(0, N_TILE, layer_tile, 0)
    outs5 = [pltpu.make_async_copy(kv5.at[:, pl.ds(0, HEAD)], k_hbm, out_sem.at[0]), pltpu.make_async_copy(kv5.at[:, pl.ds(HEAD, HEAD)], v_hbm, out_sem.at[1])]
    for cp in outs5 + ff5:
        cp.start()

    def attend(ks, vs, rows, width, masked, first, shift=None):
        n = rows.size
        if masked:
            r = lax.broadcasted_iota(jnp.int32, (n, n), 0)
            vis = lax.broadcasted_iota(jnp.int32, (n, n), 1) <= r
        if shift is not None:
            r = lax.broadcasted_iota(jnp.int32, (n, width), 0) + shift
            vis = lax.broadcasted_iota(jnp.int32, (n, width), 1) <= r
        def one(h, carry):
            s = dot_t(q[h, rows, :], ks)
            t = s * COEF - sigma if fast else s * COEF
            if shift is not None:
                t = jnp.where(vis, t, NEG)
            if masked:
                tail = jnp.where(vis, t[:, width - n:], NEG)
                t = tail if width == n else jnp.concatenate([t[:, 0:width - n], tail], axis=1)
            if not fast:
                mx = jnp.broadcast_to(jnp.max(t, axis=1, keepdims=True), (n, 128))
                fresh = mx if first else jnp.maximum(m[h, rows, :], mx)
                if not first:
                    decay = jnp.exp2(m[h, rows, :] - fresh)
                    l[h, rows, :] = l[h, rows, :] * decay
                    acc[h, rows, :] = acc[h, rows, :] * decay[:, 0:1]
                m[h, rows, :] = fresh
                t = t - fresh[:, 0:1]
            p = jnp.exp2(t)
            lp = p[:, 0:128]
            for j in range(1, width // 128):
                lp = lp + p[:, j * 128:(j + 1) * 128]
            o = dot(p.astype(BF16), vs)
            if first:
                l[h, rows, :] = lp
                acc[h, rows, :] = o
            else:
                l[h, rows, :] += lp
                acc[h, rows, :] += o
            return carry

        heads(one)

    base = jnp.where(far, LENT // TILE, 0)
    if not fast:
        def diag(i, carry):
            attend(kv5[:, 0:HEAD], kv5[:, HEAD:2 * HEAD], rows_of(i), TOK, False, True, i * TILE)
            return carry
        lax.fori_loop(base, N_TILE, diag, 0)
    for i in range(N_TILE if fast else 0):
        width = (i + 1) * TILE

        @pl.when(jnp.logical_or(i > 0, jnp.logical_not(far)))
        def _(i=i, width=width):
            attend(kv5[0:width, 0:HEAD], kv5[0:width, HEAD:2 * HEAD], pl.ds(i * TILE, TILE), width, True, True)

    def slot(s):
        ks = buf[s, :, 0:HEAD]
        vs = buf[s, :, HEAD:2 * HEAD]

        def q_rows(n, base):
            def one(i, carry):
                attend(ks, vs, pl.ds(pl.multiple_of(base + i * n, 128), n), TOK, False, False)
                return carry
            lax.fori_loop(0, (TOK - base) // n, one, 0)

        if not fast:
            def one(i, carry):
                attend(ks, vs, rows_of(i), TOK, False, False)
                return carry
            lax.fori_loop(base, N_TILE, one, 0)
            return

        @pl.when(far)
        def _():
            q_rows(TOK - LENT, LENT)

        @pl.when(jnp.logical_not(far))
        def _():
            q_rows(QROWS, 0)

    def wide(s, dst, ssem, dev):
        return send(buf.at[s], buf.at[dst], ssem, wide_recv.at[dst], dev)

    def relay(s):
        odd = s % 2 == 1
        return [(odd, wide(s, jnp.minimum(s + 1, N_SLOT - 1), pass_send.at[s], partner)),
                (jnp.logical_and(jnp.logical_and(chip == 1, core == 0), s == 1), wide(s, 5, over_send, ynb)),
                (jnp.logical_and(jnp.logical_and(chip == 2, core == 1), s == 1), wide(s, 5, over_send, xnb))]

    def chunks_in(cond, slot_no, rk, start=0, stop=N_TILE):
        @pl.when(cond)
        def _():
            def one(t, carry):
                send(kv5.at[rows_of(t)], buf.at[slot_no, rows_of(t)], hop_send.at[0, t], hop_recv.at[rk, t], partner).wait_recv()
                return carry
            lax.fori_loop(start, stop, one, 0)

    gives = jnp.logical_or(me == 3, jnp.logical_or(me == 5, me == 1))
    spread = [(gives, send(last, last, last_send.at[0], last_recv, partner)), (me == 3, send(last, last, last_send.at[1], last_recv, xnb))]

    def pass_last(cond):
        @pl.when(cond)
        def _():
            send(last, last, last_send.at[2], last_recv, partner).wait_recv()
            for c, cp in spread:
                on(c, cp, 'start')

    pass_last(jnp.logical_and(gives, me > 1))

    pass_six = send(buf.at[5], buf.at[5], pass_send.at[5], wide_recv.at[5], partner)
    pass_three = send(buf.at[3], buf.at[4], pass_send.at[3], wide_recv.at[4], partner)
    gets_six = jnp.logical_and(helper, core == 0)

    def attend_lent():
        chunks_in(True, 5 + core, 3, 0, 1)
        lend.wait_recv()
        attend(buf[5 + core, 0:LENT, 0:HEAD], buf[5 + core, 0:LENT, HEAD:2 * HEAD], borrowed, LENT, True, True)

        def block(k, carry):
            s = jnp.where(k == 0, OWN, jnp.where(k <= 4, k - 1, jnp.where(k == 5, 5, 4)))
            chunks_in(jnp.logical_and(k == 1, core == 0), 0, 0)
            early = jnp.logical_and(k == 3, core == 0)
            chunks_in(early, 5, 3, 1)
            on(early, pass_six, 'start')
            turn = k == 4
            chunks_in(turn, 3, 2)
            on(turn, pass_three, 'start')
            on(jnp.logical_and(k == 5, core == 1), pass_six, 'wait_recv')
            on(k == 6, pass_three, 'wait_recv')

            @pl.when(jnp.logical_or(k != 5, core == 1))
            def _():
                attend(buf[s, :, 0:HEAD], buf[s, :, HEAD:2 * HEAD], borrowed, TOK, False, False)
            return carry

        lax.fori_loop(0, 7, block, 0)
        for h in range(4):
            total = jnp.sum(l[h, borrowed, :], axis=1, keepdims=True)
            lent[h] = (acc[h, borrowed, :] / total).astype(BF16)
        give_back.start()

    def step(s, carry):
        chunks_in(jnp.logical_and(s == 0, core == 1), 0, 0)
        chunks_in(jnp.logical_and(s == 1, chip < 3), 1, 1)
        chunks_in(jnp.logical_and(s == 3, me != 6), 3, 2)

        @pl.when(jnp.logical_and(far, jnp.where(core == 1, s == 0, s == 1)))
        def _():
            first_in(1)
            early_pass(1).start()

        @pl.when(jnp.logical_and(me == 6, s == 1))
        def _():
            third_in(1)
            over_pass(1, 1, ynb).start()

        @pl.when(jnp.logical_or(jnp.logical_and(s > 0, s % 2 == 0), s == 5))
        def _():
            wide(s, s, pass_send.at[s], partner).wait_recv()

        for cond, cp in relay(s):
            on(cond, cp, 'start')

        @pl.when(jnp.logical_and(helper, s == 2))
        def _():
            attend_lent()

        @pl.when(jnp.logical_or(s >= 1, core == 1))
        def _():
            slot(s)

        return carry

    @pl.when(me == 1)
    def _():
        def one(it, carry):
            t = nth(it)
            third_in(t)
            over_pass(3, t, xnb).start()
            return carry
        lax.fori_loop(0, N_TILE, one, 0)

    lax.fori_loop(0, 2 * chip + 1, step, 0)
    pass_last(me == 1)


    @pl.when(jnp.logical_and(jnp.logical_not(gives), jnp.logical_not(is_last)))
    def _():
        send(last, last, last_send.at[2], last_recv, partner).wait_recv()

    def put_last(src):
        return [pltpu.make_async_copy(src.at[:, pl.ds(0, HEAD)], kl_hbm, out_sem.at[2]), pltpu.make_async_copy(src.at[:, pl.ds(HEAD, HEAD)], vl_hbm, out_sem.at[3])]

    for cp in put_last(own4):
        on(is_last, cp, 'start')
    for cp in put_last(last):
        on(jnp.logical_not(is_last), cp, 'start')

    for cp in ff5:
        cp.wait()

    def out_copy(t):
        return pltpu.make_async_copy(xo.at[rows_of(t, FROWS)], out_hbm.at[rows_of(t, FROWS)], out_sem.at[4 + t])

    def finish_tile(it, carry):
        t = (it + 1) % (TOK // FROWS)

        @pl.when(jnp.logical_and(far, t == 0))
        def _():
            give_back.wait_recv()
            for h in range(4):
                acc[h, 0:LENT, :] = lent[h].astype(F32)
                l[h, 0:LENT, :] = jnp.full((LENT, 128), 1.0 / 128.0, F32)

        rows = rows_of(t, FROWS)
        attn = []
        for h in range(4):
            total = jnp.sum(l[h, rows, :], axis=1, keepdims=True)
            attn.append((acc[h, rows, :] / total).astype(BF16))
        xo[rows, :] = jnp.concatenate(finish_rows(fast, mid[rows, :], jnp.concatenate(attn, axis=1), ng_ref[1], wo, wg, wu, wd), axis=0)
        out_copy(t).start()
        return carry

    lax.fori_loop(0, TOK // FROWS, finish_tile, 0)

    def drain_tile(t, carry):
        on(me < top, halo_copy(t), 'wait_send')
        on(far, early_pass(t), 'wait_send')
        on(me == 1, over_pass(3, t, xnb), 'wait_send')
        on(me == 6, over_pass(1, t, ynb), 'wait_send')
        for cond, cp in hops(t):
            on(cond, cp, 'wait_send')
        return carry

    lax.fori_loop(0, N_TILE, drain_tile, 0)

    def drain_step(s, carry):
        for cond, cp in relay(s):
            on(cond, cp, 'wait_send')
        return carry

    lax.fori_loop(1, 2 * chip + 1, drain_step, 0)
    for cp in last_cps:
        on(is_last, cp, 'wait_send')
    on(far, lend, 'wait_send')
    on(helper, give_back, 'wait_send')
    on(helper, pass_three, 'wait_send')
    on(gets_six, pass_six, 'wait_send')
    for cond, cp in spread:
        on(cond, cp, 'wait_send')
    for cp in outs5 + put_last(last):
        cp.wait()
    for t in range(TOK // FROWS):
        out_copy(t).wait()


def layers(fast, ng, qg, rope, x, wq, wk, wv, wo, wg, wu, wd):
    anyw = pl.BlockSpec(memory_space=pl.ANY)
    dma = pltpu.SemaphoreType.DMA
    kshape = jax.ShapeDtypeStruct((TOK, HEAD), BF16)
    return pl.pallas_call(
        functools.partial(layers_kernel, fast),
        in_specs=[anyw] * 14,
        out_specs=[anyw] * 5 + [pl.BlockSpec(memory_space=pltpu.SMEM)],
        out_shape=[jax.ShapeDtypeStruct((TOK, D), BF16), kshape, kshape, kshape, kshape, jax.ShapeDtypeStruct((1,), F32)],
        scratch_shapes=[
            pltpu.VMEM((2, 4, D), F32), pltpu.VMEM((2, 2, HEAD), F32), pltpu.VMEM((TOK // LO, HEAD), F32), pltpu.VMEM((LO, HEAD), F32),
            pltpu.VMEM((TOK // LO, HEAD), F32), pltpu.VMEM((LO, HEAD), F32), pltpu.VMEM((TOK, D), BF16), pltpu.VMEM((TOK, D), BF16), pltpu.VMEM((WINDOW + TOK, 2 * HEAD), BF16),
            pltpu.VMEM((4, TOK + LENT, HEAD), BF16), pltpu.VMEM((N_SLOT, TOK, 2 * HEAD), BF16), pltpu.VMEM((4, TOK + LENT, HEAD), F32),
            pltpu.VMEM((4, TOK + LENT, 128), F32), pltpu.VMEM((8, 128) if fast else (4, TOK + LENT, 128), F32),
            pltpu.VMEM((4, LENT, HEAD), BF16), pltpu.VMEM((TOK, 2 * HEAD), BF16), pltpu.VMEM((TOK, D), BF16),
            pltpu.VMEM((2, 4, D, HEAD), BF16), pltpu.VMEM((2, D, HEAD), BF16), pltpu.VMEM((2, D, HEAD), BF16),
            pltpu.VMEM((4 * HEAD, D), BF16), pltpu.VMEM((D, FF), BF16), pltpu.VMEM((D, FF), BF16), pltpu.VMEM((FF, D), BF16),
            dma((17,)), dma((4 + TOK // FROWS,)), dma((N_TILE,)), dma((N_TILE,)), dma((4, N_TILE)), dma((4, N_TILE)), dma((N_SLOT,)), dma, dma((N_SLOT,)),
            dma((3,)), dma, dma((4,))],
        name="layers_fast" if fast else "layers_safe",
        compiler_params=pltpu.CompilerParams(vmem_limit_bytes=VLIM, collective_id=0 if fast else None, has_side_effects=True),
        cost_estimate=pl.CostEstimate(flops=60 * 10**9, bytes_accessed=30 << 20, transcendentals=0),
    )(ng, qg, *rope[0], *rope[1], x, wq, wk, wv, wo, wg, wu, wd)


def emit_kernel(*refs):
    ins, outs, mids, sem_in, sem_out = refs[0:5], refs[5:10], refs[10:15], refs[15], refs[16]
    loads = [pltpu.make_async_copy(i, m, sem_in.at[n]) for n, (i, m) in enumerate(zip(ins, mids))]
    stores = [pltpu.make_async_copy(m, o, sem_out.at[n]) for n, (m, o) in enumerate(zip(mids, outs))]
    for cp in loads:
        cp.start()
    for ld, st in zip(loads, stores):
        ld.wait()
        st.start()
    for st in stores:
        st.wait()


def emit(arrays):
    anyw = pl.BlockSpec(memory_space=pl.ANY)
    return pl.pallas_call(
        emit_kernel,
        in_specs=[anyw] * 5,
        out_specs=[anyw] * 5,
        out_shape=[jax.ShapeDtypeStruct(a.shape, a.dtype) for a in arrays],
        scratch_shapes=[pltpu.VMEM(a.shape, a.dtype) for a in arrays] + [pltpu.SemaphoreType.DMA((5,)), pltpu.SemaphoreType.DMA((5,))],
        name="emit",
    )(*arrays)


def solution(mesh):
    n_dev = mesh.shape['cp']
    rope = [rope_const(layer, TOK * n_dev) for layer in range(2)]

    def shard_body(x, ng, qg, w_q, w_k, w_v, w_o, w_gate, w_up, w_down):
        wq = w_q.transpose(0, 2, 1, 3)
        wk = w_k.reshape(2, D, HEAD)
        wv = w_v.reshape(2, D, HEAD)
        wo = w_o.reshape(2, 4 * HEAD, D)

        def run(fast):
            return tuple(layers(fast, ng, qg, rope, x, wq, wk, wv, wo, w_gate, w_up, w_down))

        *first, bound = run(True)
        _, rest = lax.while_loop(lambda c: c[0], lambda c: (jnp.zeros((), jnp.bool_), run(False)[:5]), (bound[0] > LIMIT, tuple(first)))
        out, k5, v5, kl, vl = emit(rest)
        return out, k5[:, None, :], v5[:, None, :], kl[:, None, :], vl[:, None, :]

    return jax.shard_map(shard_body, mesh=mesh, in_specs=(P('cp'), P(), P(), P(), P(), P(), P(), P(), P(), P()),
                         out_specs=(P('cp'), P('cp'), P('cp'), P(), P()), check_vma=False)
```

```python
import functools

import numpy as np
import jax
import jax.numpy as jnp
from jax import lax
from jax.experimental import pallas as pl
from jax.experimental.pallas import tpu as pltpu
from jax.sharding import PartitionSpec as P

WINDOW = 1024
EPS = 1e-6
BASES = (10000.0, 1000000.0)
SCALES = (1.0, 8.0)
HEAD = 256
TOK = 1024
D = 640
FF = 2048
TILE = 256
LO = 32
LOG2E = 1.4426950408889634
COEF = LOG2E / 16.0
TOP = 36.0
LIMIT = 56.0
NEG = -1e30
F32 = jnp.float32
BF16 = jnp.bfloat16
VLIM = 58 << 20


def rope_const(layer, seq_len):
    base, scale = BASES[layer], SCALES[layer]
    freq = base ** (-np.arange(HEAD // 2, dtype=np.float64) * 2.0 / HEAD)
    hi = (np.arange(seq_len // LO) * LO / scale)[:, None] * freq[None, :]
    lo = (np.arange(LO) / scale)[:, None] * freq[None, :]
    hi_tab = np.concatenate([np.cos(hi), np.sin(hi)], axis=1).astype(np.float32)
    lo_tab = np.concatenate([np.cos(lo), np.sin(lo)], axis=1).astype(np.float32)
    return hi_tab, lo_tab


def rms(x, gain):
    return x * lax.rsqrt(jnp.mean(x * x, axis=-1, keepdims=True) + EPS) * gain


def cos_sin(hi_ref, lo_ref, row0, rows):
    n_hi = rows // LO
    hi = hi_ref[pl.ds(pl.multiple_of(row0 // LO, 8), n_hi), :]
    lo = lo_ref[...]
    ch, sh = hi[:, None, 0:128], hi[:, None, 128:256]
    cl, sl = lo[None, :, 0:128], lo[None, :, 128:256]
    cos = (ch * cl - sh * sl).reshape(rows, 128)
    sin = (sh * cl + ch * sl).reshape(rows, 128)
    return cos, sin


def rotate(x, cos, sin):
    a, b = x[:, 0:128], x[:, 128:256]
    return jnp.concatenate([a * cos - b * sin, b * cos + a * sin], axis=1).astype(BF16)


def head_rope(proj, gain, cos, sin):
    return rotate(rms(proj.astype(BF16).astype(F32), gain), cos, sin)


def dot(a, b):
    return jnp.dot(a, b, preferred_element_type=F32)


def dot_t(a, b):
    return lax.dot_general(a, b, (((1,), (1,)), ((), ())), preferred_element_type=F32)


MESH = pl.DeviceIdType.MESH
N_SLOT = 8
OWN = 7
LENT = 256
N_TILE = TOK // TILE
QROWS = 1024
FROWS = 256
PARTS = 2


def finish_rows(fast, x, attn, ng, wo, wg, wu, wd):
    n = PARTS if fast else 1
    size = x.shape[0] // n
    groups = [slice(i * size, (i + 1) * size) for i in range(n)]

    def ff(b, cols):
        m = (jax.nn.gelu(dot(b, wg[:, cols]), approximate=True) * dot(b, wu[:, cols])).astype(BF16)
        return m if fast else dot(m, wd[cols, :])

    o = [dot(attn[g], wo[...]).astype(BF16).astype(F32) for g in groups]
    h1, b = [], []
    for g, o_g in zip(groups, o):
        h1.append((x[g].astype(F32) + rms(o_g, 1.0 + ng[1:2, :])).astype(BF16))
        b.append(rms(h1[-1].astype(F32), 1.0 + ng[2:3, :]).astype(BF16))
    if fast:
        m = [ff(b_g, slice(None)) for b_g in b]
        y = [dot(m_g, wd[...]) for m_g in m]
    else:
        y = [lax.fori_loop(0, FF // 256, lambda f, part: part + ff(b[0], pl.ds(pl.multiple_of(f * 256, 256), 256)), jnp.zeros(x.shape, F32))]
    return [(h_g.astype(F32) + rms(y_g.astype(BF16).astype(F32), 1.0 + ng[3:4, :])).astype(BF16) for h_g, y_g in zip(h1, y)]


def layers_kernel(fast, ng_hbm, qg_hbm, hi4_hbm, lo4_hbm, hi5_hbm, lo5_hbm, x_hbm, wq_hbm, wk_hbm, wv_hbm, wo_hbm, wg_hbm, wu_hbm, wd_hbm,
                  out_hbm, k_hbm, v_hbm, kl_hbm, vl_hbm, bound_ref,
                  ng_ref, qg_ref, hi4_ref, lo4_ref, hi5_ref, lo5_ref, x, mid, win, q, buf, acc, l, m, lent, last, xo, wq, wk, wv, wo, wg, wu, wd,
                  load_sem, out_sem, halo_send, halo_recv, hop_send, hop_recv, pass_send, over_send, wide_recv, last_send, last_recv, lend_sem):
    me = lax.axis_index('cp')
    core = me % 2
    chip = me // 2
    partner = me + 1 - 2 * core
    xnb = me + 2 - 4 * (chip % 2)
    ynb = me + 4 - 8 * (chip // 2)
    top = 7
    is_last = me == top
    kv5 = buf.at[OWN]
    near, helper, far = chip == 0, chip == 1, chip == 3
    borrowed = pl.ds(TOK, LENT)

    def load(src, dst, n):
        return pltpu.make_async_copy(src, dst, load_sem.at[n])

    turns = pl.ds(pl.multiple_of(me * (TOK // LO), TOK // LO), TOK // LO)
    small = [load(ng_hbm, ng_ref, 11), load(qg_hbm, qg_ref, 12), load(hi4_hbm.at[turns], hi4_ref, 13), load(lo4_hbm, lo4_ref, 14),
             load(hi5_hbm.at[turns], hi5_ref, 15), load(lo5_hbm, lo5_ref, 16)]
    early = [load(x_hbm, x, 0), load(wk_hbm.at[0], wk.at[0], 1), load(wv_hbm.at[0], wv.at[0], 2), load(wq_hbm.at[0], wq.at[0], 3)]
    ff4 = [load(wo_hbm.at[0], wo, 4), load(wg_hbm.at[0], wg, 5), load(wu_hbm.at[0], wu, 6), load(wd_hbm.at[0], wd, 7)]
    next_qkv = [load(wk_hbm.at[1], wk.at[1], 8), load(wv_hbm.at[1], wv.at[1], 9), load(wq_hbm.at[1], wq.at[1], 10)]
    ff5 = [load(wo_hbm.at[1], wo, 4), load(wg_hbm.at[1], wg, 5), load(wu_hbm.at[1], wu, 6), load(wd_hbm.at[1], wd, 7)]
    for cp in small + early:
        cp.start()

    if fast:
        barrier = pltpu.get_barrier_semaphore()
        for other in (partner, xnb, ynb, (me + 1) % 8, (me + 7) % 8):
            pl.semaphore_signal(barrier, inc=1, device_id=(other,), device_id_type=MESH)
    for cp in ff4 + next_qkv:
        cp.start()

    @pl.when(me == 0)
    def _():
        win[0:WINDOW, :] = jnp.zeros((WINDOW, 2 * HEAD), BF16)


    def send(src, dst, ssem, rsem, dev):
        return pltpu.make_async_remote_copy(src_ref=src, dst_ref=dst, send_sem=ssem, recv_sem=rsem, device_id=(dev,), device_id_type=MESH)

    def heads(one):
        if fast:
            for h in range(4):
                one(h, 0)
        else:
            lax.fori_loop(0, 4, one, 0)

    def on(cond, copy, act):
        @pl.when(cond)
        def _():
            getattr(copy, act)()

    def rows_of(t, n=TILE):
        return pl.ds(pl.multiple_of(t * n, n), n)

    def halo_copy(t):
        return send(win.at[rows_of(t + N_TILE)], win.at[rows_of(t)], halo_send.at[t], halo_recv.at[t], (me + 1) % 8)

    for cp in small + early[:3]:
        cp.wait()
    gains = jnp.abs(1.0 + qg_ref[...])
    pair = jnp.maximum(gains[:, :, 0:HEAD // 2], gains[:, :, HEAD // 2:])
    bound = 16.0 * 1.02 * jnp.max(pair[:, 0:1] * pair[:, 1:2])
    bound_ref[0] = bound
    sigma = jnp.maximum(bound - TOP, 0.0) * LOG2E
    g4q, g4k = 1.0 + qg_ref[0, 0:1, :], 1.0 + qg_ref[0, 1:2, :]
    g5q, g5k = 1.0 + qg_ref[1, 0:1, :], 1.0 + qg_ref[1, 1:2, :]
    def kv_tile(it, carry):
        t = N_TILE - 1 - it
        cos, sin = cos_sin(hi4_ref, lo4_ref, t * TILE, TILE)
        a = rms(x[rows_of(t), :].astype(F32), 1.0 + ng_ref[0, 0:1, :]).astype(BF16)
        mid[rows_of(t), :] = a
        win[rows_of(t + N_TILE), 0:HEAD] = head_rope(dot(a, wk[0]), g4k, cos, sin)
        win[rows_of(t + N_TILE), HEAD:2 * HEAD] = dot(a, wv[0]).astype(BF16)
        if fast:
            @pl.when(it == 0)
            def _():
                pl.semaphore_wait(barrier, 5)
        on(me < top, halo_copy(t), 'start')
        return carry

    lax.fori_loop(0, N_TILE, kv_tile, 0)
    own4 = win.at[pl.ds(WINDOW, TOK)]
    last_cps = [send(own4, last, last_send.at[n], last_recv, dev) for n, dev in enumerate((partner, xnb, ynb))]
    for cp in last_cps:
        on(is_last, cp, 'start')
    early[3].wait()
    for cp in ff4 + next_qkv:
        cp.wait()

    def hops(t):
        def hop(k, slot, rk, dev):
            return send(kv5.at[rows_of(t)], buf.at[slot, rows_of(t)], hop_send.at[k, t], hop_recv.at[rk, t], dev)
        return [(jnp.logical_or(core == 0, helper), hop(0, 0, 0, partner)),
                (chip == 0, hop(1, 1, 1, xnb)),
                (chip == 0, hop(2, 1, 1, ynb)),
                (chip == 1, hop(2, 1, 1, ynb)),
                (chip == 2, hop(1, 3, 2, xnb)),
                (me == 5, hop(2, 3, 2, ynb)),
                (me == 6, hop(2, 5, 3, ynb)),
                (jnp.logical_and(me == 7, t == 0), hop(2, 6, 3, ynb))]

    def early_pass(t):
        return send(buf.at[1, rows_of(t)], buf.at[3, rows_of(t)], hop_send.at[3, t], hop_recv.at[2, t], xnb)

    def first_in(t):
        send(kv5.at[rows_of(t)], buf.at[1, rows_of(t)], hop_send.at[0, t], hop_recv.at[1, t], partner).wait_recv()

    def third_in(t):
        send(kv5.at[rows_of(t)], buf.at[3, rows_of(t)], hop_send.at[0, t], hop_recv.at[2, t], partner).wait_recv()

    def over_pass(k, t, dev):
        return send(buf.at[3, rows_of(t)], buf.at[3, rows_of(t)], hop_send.at[k, t], hop_recv.at[2, t], dev)

    lend = send(q.at[:, pl.ds(0, LENT), :], q.at[:, borrowed, :], lend_sem.at[0], lend_sem.at[1], ynb)
    give_back = send(lent, lent, lend_sem.at[2], lend_sem.at[3], ynb)

    n_key = WINDOW + TILE

    def nth(it):
        return jnp.where(it < 2, N_TILE - 1 - it, it - 2)

    def layer_tile(it, carry):
        t = nth(it)
        before = nth(jnp.maximum(it - 1, 0))
        rows = rows_of(t)
        cos, sin = cos_sin(hi4_ref, lo4_ref, t * TILE, TILE)
        a = mid[rows, :]

        if fast:
            qs = [head_rope(dot(a, wq[0, h]), g4q, cos, sin) for h in range(4)]
        on(jnp.logical_and(me > 0, it < 2), halo_copy(t), 'wait_recv')
        for n in (1, 0):
            on(jnp.logical_and(me > 0, it == 2), halo_copy(n), 'wait_recv')
        start = pl.multiple_of(t * TILE, TILE)
        ks = win[pl.ds(start, n_key), 0:HEAD]
        vs = win[pl.ds(start, n_key), HEAD:2 * HEAD]
        col = lax.broadcasted_iota(jnp.int32, (1, n_key), 1)
        hidden = jnp.logical_and(me == 0, col + start < WINDOW)
        bias = jnp.where(hidden, NEG, -sigma if fast else 0.0)
        r = lax.broadcasted_iota(jnp.int32, (TILE, TILE), 0)
        c = lax.broadcasted_iota(jnp.int32, (TILE, TILE), 1)

        def local(h, q_h):
            s = dot_t(q_h, ks) * COEF + bias
            s = jnp.concatenate([jnp.where(c > r, s[:, 0:TILE], NEG), s[:, TILE:WINDOW], jnp.where(c <= r, s[:, WINDOW:], NEG)], axis=1)
            if not fast:
                s = s - jnp.max(s, axis=1, keepdims=True)
            p = jnp.exp2(s)
            total = jnp.sum(p, axis=1, keepdims=True)
            return dot(p.astype(BF16), vs) / total

        if fast:
            outs = [local(h, qs[h]).astype(BF16) for h in range(4)]
        else:
            def one(h, carry):
                acc[h, 0:TILE, :] = local(h, head_rope(dot(a, wq[0, h]), g4q, cos, sin))
                return carry
            heads(one)
            outs = [acc[h, 0:TILE, :].astype(BF16) for h in range(4)]
        h_mid = finish_rows(fast, x[rows, :], jnp.concatenate(outs, axis=1), ng_ref[0], wo, wg, wu, wd)
        cos, sin = cos_sin(hi5_ref, lo5_ref, t * TILE, TILE)
        size = TILE // len(h_mid)
        parts = []
        for i, h_g in enumerate(h_mid):
            here = pl.ds(pl.multiple_of(t * TILE + i * size, size), size)
            mid[here, :] = h_g
            parts.append((here, rms(h_g.astype(F32), 1.0 + ng_ref[1, 0:1, :]).astype(BF16), cos[i * size:(i + 1) * size], sin[i * size:(i + 1) * size]))
        for here, a_g, cos_g, sin_g in parts:
            kv5[here, 0:HEAD] = head_rope(dot(a_g, wk[1]), g5k, cos_g, sin_g)
            kv5[here, HEAD:2 * HEAD] = dot(a_g, wv[1]).astype(BF16)

        def project(h, carry):
            for here, a_g, cos_g, sin_g in parts:
                q[h, here, :] = head_rope(dot(a_g, wq[1, h]), g5q, cos_g, sin_g)
            return carry

        heads(project)
        for cond, cp in hops(t):
            on(cond, cp, 'start')
        on(jnp.logical_and(far, it == 2), lend, 'start')

        @pl.when(jnp.logical_and(far, it >= 1))
        def _():
            first_in(before)
            early_pass(before).start()

        @pl.when(jnp.logical_and(me == 6, it >= 1))
        def _():
            third_in(before)
            over_pass(1, before, ynb).start()
        return carry

    lax.fori_loop(0, N_TILE, layer_tile, 0)
    outs5 = [pltpu.make_async_copy(kv5.at[:, pl.ds(0, HEAD)], k_hbm, out_sem.at[0]), pltpu.make_async_copy(kv5.at[:, pl.ds(HEAD, HEAD)], v_hbm, out_sem.at[1])]
    for cp in outs5 + ff5:
        cp.start()

    def attend(ks, vs, rows, width, masked, first, shift=None):
        n = rows.size
        if masked:
            r = lax.broadcasted_iota(jnp.int32, (n, n), 0)
            vis = lax.broadcasted_iota(jnp.int32, (n, n), 1) <= r
        if shift is not None:
            r = lax.broadcasted_iota(jnp.int32, (n, width), 0) + shift
            vis = lax.broadcasted_iota(jnp.int32, (n, width), 1) <= r
        def one(h, carry):
            s = dot_t(q[h, rows, :], ks)
            t = s * COEF - sigma if fast else s * COEF
            if shift is not None:
                t = jnp.where(vis, t, NEG)
            if masked:
                tail = jnp.where(vis, t[:, width - n:], NEG)
                t = tail if width == n else jnp.concatenate([t[:, 0:width - n], tail], axis=1)
            if not fast:
                mx = jnp.broadcast_to(jnp.max(t, axis=1, keepdims=True), (n, 128))
                fresh = mx if first else jnp.maximum(m[h, rows, :], mx)
                if not first:
                    decay = jnp.exp2(m[h, rows, :] - fresh)
                    l[h, rows, :] = l[h, rows, :] * decay
                    acc[h, rows, :] = acc[h, rows, :] * decay[:, 0:1]
                m[h, rows, :] = fresh
                t = t - fresh[:, 0:1]
            p = jnp.exp2(t)
            lp = p[:, 0:128]
            for j in range(1, width // 128):
                lp = lp + p[:, j * 128:(j + 1) * 128]
            o = dot(p.astype(BF16), vs)
            if first:
                l[h, rows, :] = lp
                acc[h, rows, :] = o
            else:
                l[h, rows, :] += lp
                acc[h, rows, :] += o
            return carry

        heads(one)

    base = jnp.where(far, LENT // TILE, 0)
    if not fast:
        def diag(i, carry):
            attend(kv5[:, 0:HEAD], kv5[:, HEAD:2 * HEAD], rows_of(i), TOK, False, True, i * TILE)
            return carry
        lax.fori_loop(base, N_TILE, diag, 0)
    for i in range(N_TILE if fast else 0):
        width = (i + 1) * TILE

        @pl.when(jnp.logical_or(i > 0, jnp.logical_not(far)))
        def _(i=i, width=width):
            attend(kv5[0:width, 0:HEAD], kv5[0:width, HEAD:2 * HEAD], pl.ds(i * TILE, TILE), width, True, True)

    def slot(s):
        ks = buf[s, :, 0:HEAD]
        vs = buf[s, :, HEAD:2 * HEAD]

        def q_rows(n, base):
            def one(i, carry):
                attend(ks, vs, pl.ds(pl.multiple_of(base + i * n, 128), n), TOK, False, False)
                return carry
            lax.fori_loop(0, (TOK - base) // n, one, 0)

        if not fast:
            def one(i, carry):
                attend(ks, vs, rows_of(i), TOK, False, False)
                return carry
            lax.fori_loop(base, N_TILE, one, 0)
            return

        @pl.when(far)
        def _():
            q_rows(TOK - LENT, LENT)

        @pl.when(jnp.logical_not(far))
        def _():
            q_rows(QROWS, 0)

    def wide(s, dst, ssem, dev):
        return send(buf.at[s], buf.at[dst], ssem, wide_recv.at[dst], dev)

    def relay(s):
        odd = s % 2 == 1
        return [(odd, wide(s, jnp.minimum(s + 1, N_SLOT - 1), pass_send.at[s], partner)),
                (jnp.logical_and(jnp.logical_and(chip == 1, core == 0), s == 1), wide(s, 5, over_send, ynb)),
                (jnp.logical_and(jnp.logical_and(chip == 2, core == 1), s == 1), wide(s, 5, over_send, xnb))]

    def chunks_in(cond, slot_no, rk, start=0, stop=N_TILE):
        @pl.when(cond)
        def _():
            def one(t, carry):
                send(kv5.at[rows_of(t)], buf.at[slot_no, rows_of(t)], hop_send.at[0, t], hop_recv.at[rk, t], partner).wait_recv()
                return carry
            lax.fori_loop(start, stop, one, 0)

    gives = jnp.logical_or(me == 3, jnp.logical_or(me == 5, me == 1))
    spread = [(gives, send(last, last, last_send.at[0], last_recv, partner)), (me == 3, send(last, last, last_send.at[1], last_recv, xnb))]

    def pass_last(cond):
        @pl.when(cond)
        def _():
            send(last, last, last_send.at[2], last_recv, partner).wait_recv()
            for c, cp in spread:
                on(c, cp, 'start')

    pass_last(jnp.logical_and(gives, me > 1))

    pass_six = send(buf.at[5], buf.at[5], pass_send.at[5], wide_recv.at[5], partner)
    pass_three = send(buf.at[3], buf.at[4], pass_send.at[3], wide_recv.at[4], partner)
    gets_six = jnp.logical_and(helper, core == 0)

    def attend_lent():
        chunks_in(True, 5 + core, 3, 0, 1)
        lend.wait_recv()
        attend(buf[5 + core, 0:LENT, 0:HEAD], buf[5 + core, 0:LENT, HEAD:2 * HEAD], borrowed, LENT, True, True)

        def block(k, carry):
            s = jnp.where(k == 0, OWN, jnp.where(k <= 4, k - 1, jnp.where(k == 5, 5, 4)))
            chunks_in(jnp.logical_and(k == 1, core == 0), 0, 0)
            early = jnp.logical_and(k == 3, core == 0)
            chunks_in(early, 5, 3, 1)
            on(early, pass_six, 'start')
            turn = k == 4
            chunks_in(turn, 3, 2)
            on(turn, pass_three, 'start')
            on(jnp.logical_and(k == 5, core == 1), pass_six, 'wait_recv')
            on(k == 6, pass_three, 'wait_recv')

            @pl.when(jnp.logical_or(k != 5, core == 1))
            def _():
                attend(buf[s, :, 0:HEAD], buf[s, :, HEAD:2 * HEAD], borrowed, TOK, False, False)
            return carry

        lax.fori_loop(0, 7, block, 0)
        for h in range(4):
            total = jnp.sum(l[h, borrowed, :], axis=1, keepdims=True)
            lent[h] = (acc[h, borrowed, :] / total).astype(BF16)
        give_back.start()

    def step(s, carry):
        chunks_in(jnp.logical_and(s == 0, core == 1), 0, 0)
        chunks_in(jnp.logical_and(s == 1, chip < 3), 1, 1)
        chunks_in(jnp.logical_and(s == 3, me != 6), 3, 2)

        @pl.when(jnp.logical_and(far, jnp.where(core == 1, s == 0, s == 1)))
        def _():
            first_in(1)
            early_pass(1).start()

        @pl.when(jnp.logical_and(me == 6, s == 1))
        def _():
            third_in(1)
            over_pass(1, 1, ynb).start()

        @pl.when(jnp.logical_or(jnp.logical_and(s > 0, s % 2 == 0), s == 5))
        def _():
            wide(s, s, pass_send.at[s], partner).wait_recv()

        for cond, cp in relay(s):
            on(cond, cp, 'start')

        @pl.when(jnp.logical_and(helper, s == 2))
        def _():
            attend_lent()

        @pl.when(jnp.logical_or(s >= 1, core == 1))
        def _():
            slot(s)

        return carry

    @pl.when(me == 1)
    def _():
        def one(it, carry):
            t = nth(it)
            third_in(t)
            over_pass(3, t, xnb).start()
            return carry
        lax.fori_loop(0, N_TILE, one, 0)

    lax.fori_loop(0, 2 * chip + 1, step, 0)
    pass_last(me == 1)


    @pl.when(jnp.logical_and(jnp.logical_not(gives), jnp.logical_not(is_last)))
    def _():
        send(last, last, last_send.at[2], last_recv, partner).wait_recv()

    def put_last(src):
        return [pltpu.make_async_copy(src.at[:, pl.ds(0, HEAD)], kl_hbm, out_sem.at[2]), pltpu.make_async_copy(src.at[:, pl.ds(HEAD, HEAD)], vl_hbm, out_sem.at[3])]

    for cp in put_last(own4):
        on(is_last, cp, 'start')
    for cp in put_last(last):
        on(jnp.logical_not(is_last), cp, 'start')

    for cp in ff5:
        cp.wait()

    def out_copy(t):
        return pltpu.make_async_copy(xo.at[rows_of(t, FROWS)], out_hbm.at[rows_of(t, FROWS)], out_sem.at[4 + t])

    def finish_tile(it, carry):
        t = (it + 1) % (TOK // FROWS)

        @pl.when(jnp.logical_and(far, t == 0))
        def _():
            give_back.wait_recv()
            for h in range(4):
                acc[h, 0:LENT, :] = lent[h].astype(F32)
                l[h, 0:LENT, :] = jnp.full((LENT, 128), 1.0 / 128.0, F32)

        rows = rows_of(t, FROWS)
        attn = []
        for h in range(4):
            total = jnp.sum(l[h, rows, :], axis=1, keepdims=True)
            attn.append((acc[h, rows, :] / total).astype(BF16))
        xo[rows, :] = jnp.concatenate(finish_rows(fast, mid[rows, :], jnp.concatenate(attn, axis=1), ng_ref[1], wo, wg, wu, wd), axis=0)
        out_copy(t).start()
        return carry

    lax.fori_loop(0, TOK // FROWS, finish_tile, 0)

    def drain_tile(t, carry):
        on(me < top, halo_copy(t), 'wait_send')
        on(far, early_pass(t), 'wait_send')
        on(me == 1, over_pass(3, t, xnb), 'wait_send')
        on(me == 6, over_pass(1, t, ynb), 'wait_send')
        for cond, cp in hops(t):
            on(cond, cp, 'wait_send')
        return carry

    lax.fori_loop(0, N_TILE, drain_tile, 0)

    def drain_step(s, carry):
        for cond, cp in relay(s):
            on(cond, cp, 'wait_send')
        return carry

    lax.fori_loop(1, 2 * chip + 1, drain_step, 0)
    for cp in last_cps:
        on(is_last, cp, 'wait_send')
    on(far, lend, 'wait_send')
    on(helper, give_back, 'wait_send')
    on(helper, pass_three, 'wait_send')
    on(gets_six, pass_six, 'wait_send')
    for cond, cp in spread:
        on(cond, cp, 'wait_send')
    for cp in outs5 + put_last(last):
        cp.wait()
    for t in range(TOK // FROWS):
        out_copy(t).wait()


def layers(fast, ng, qg, rope, x, wq, wk, wv, wo, wg, wu, wd):
    anyw = pl.BlockSpec(memory_space=pl.ANY)
    dma = pltpu.SemaphoreType.DMA
    kshape = jax.ShapeDtypeStruct((TOK, HEAD), BF16)
    return pl.pallas_call(
        functools.partial(layers_kernel, fast),
        in_specs=[anyw] * 14,
        out_specs=[anyw] * 5 + [pl.BlockSpec(memory_space=pltpu.SMEM)],
        out_shape=[jax.ShapeDtypeStruct((TOK, D), BF16), kshape, kshape, kshape, kshape, jax.ShapeDtypeStruct((1,), F32)],
        scratch_shapes=[
            pltpu.VMEM((2, 4, D), F32), pltpu.VMEM((2, 2, HEAD), F32), pltpu.VMEM((TOK // LO, HEAD), F32), pltpu.VMEM((LO, HEAD), F32),
            pltpu.VMEM((TOK // LO, HEAD), F32), pltpu.VMEM((LO, HEAD), F32), pltpu.VMEM((TOK, D), BF16), pltpu.VMEM((TOK, D), BF16), pltpu.VMEM((WINDOW + TOK, 2 * HEAD), BF16),
            pltpu.VMEM((4, TOK + LENT, HEAD), BF16), pltpu.VMEM((N_SLOT, TOK, 2 * HEAD), BF16), pltpu.VMEM((4, TOK + LENT, HEAD), F32),
            pltpu.VMEM((4, TOK + LENT, 128), F32), pltpu.VMEM((8, 128) if fast else (4, TOK + LENT, 128), F32),
            pltpu.VMEM((4, LENT, HEAD), BF16), pltpu.VMEM((TOK, 2 * HEAD), BF16), pltpu.VMEM((TOK, D), BF16),
            pltpu.VMEM((2, 4, D, HEAD), BF16), pltpu.VMEM((2, D, HEAD), BF16), pltpu.VMEM((2, D, HEAD), BF16),
            pltpu.VMEM((4 * HEAD, D), BF16), pltpu.VMEM((D, FF), BF16), pltpu.VMEM((D, FF), BF16), pltpu.VMEM((FF, D), BF16),
            dma((17,)), dma((4 + TOK // FROWS,)), dma((N_TILE,)), dma((N_TILE,)), dma((4, N_TILE)), dma((4, N_TILE)), dma((N_SLOT,)), dma, dma((N_SLOT,)),
            dma((3,)), dma, dma((4,))],
        name="layers_fast" if fast else "layers_safe",
        compiler_params=pltpu.CompilerParams(vmem_limit_bytes=VLIM, collective_id=0 if fast else None, has_side_effects=True),
        cost_estimate=pl.CostEstimate(flops=60 * 10**9, bytes_accessed=30 << 20, transcendentals=0),
    )(ng, qg, *rope[0], *rope[1], x, wq, wk, wv, wo, wg, wu, wd)


def emit_kernel(*refs):
    ins, outs, mids, sem_in, sem_out = refs[0:5], refs[5:10], refs[10:15], refs[15], refs[16]
    loads = [pltpu.make_async_copy(i, m, sem_in.at[n]) for n, (i, m) in enumerate(zip(ins, mids))]
    stores = [pltpu.make_async_copy(m, o, sem_out.at[n]) for n, (m, o) in enumerate(zip(mids, outs))]
    for cp in loads:
        cp.start()
    for ld, st in zip(loads, stores):
        ld.wait()
        st.start()
    for st in stores:
        st.wait()


def emit(arrays):
    anyw = pl.BlockSpec(memory_space=pl.ANY)
    return pl.pallas_call(
        emit_kernel,
        in_specs=[anyw] * 5,
        out_specs=[anyw] * 5,
        out_shape=[jax.ShapeDtypeStruct(a.shape, a.dtype) for a in arrays],
        scratch_shapes=[pltpu.VMEM(a.shape, a.dtype) for a in arrays] + [pltpu.SemaphoreType.DMA((5,)), pltpu.SemaphoreType.DMA((5,))],
        name="emit",
    )(*arrays)


def solution(mesh):
    n_dev = mesh.shape['cp']
    rope = [rope_const(layer, TOK * n_dev) for layer in range(2)]

    def shard_body(x, ng, qg, w_q, w_k, w_v, w_o, w_gate, w_up, w_down):
        wq = w_q.transpose(0, 2, 1, 3)
        wk = w_k.reshape(2, D, HEAD)
        wv = w_v.reshape(2, D, HEAD)
        wo = w_o.reshape(2, 4 * HEAD, D)

        def run(fast):
            return tuple(layers(fast, ng, qg, rope, x, wq, wk, wv, wo, w_gate, w_up, w_down))

        *first, bound = run(True)
        _, rest = lax.while_loop(lambda c: c[0], lambda c: (jnp.zeros((), jnp.bool_), run(False)[:5]), (bound[0] > LIMIT, tuple(first)))
        out, k5, v5, kl, vl = emit(rest)
        return out, k5[:, None, :], v5[:, None, :], kl[:, None, :], vl[:, None, :]

    return jax.shard_map(shard_body, mesh=mesh, in_specs=(P('cp'), P(), P(), P(), P(), P(), P(), P(), P(), P()),
                         out_specs=(P('cp'), P('cp'), P('cp'), P(), P()), check_vma=False)
```
